32 devices in a mesh: tp: 32 (over z, y, x, core).
Axes of the slice: x: 2, y: 2, z: 4, core: 2. Of those that a mesh axis runs over, the one named last changes fastest.
Arguments:
- x_in: bfloat16 [16, 256, 4096], P(None, 'tp')
- grad_y: bfloat16 [16, 256, 4096], P(None, 'tp')
- ln_gain: float32 [4096], replicated
- w_query: bfloat16 [4096, 32, 128], P(None, 'tp')
- w_key: bfloat16 [4096, 128], replicated
- w_value: bfloat16 [4096, 128], replicated
- w_out: bfloat16 [32, 128, 4096], P('tp')
- w_gate: bfloat16 [4096, 16384], P(None, 'tp')
- w_up: bfloat16 [4096, 16384], P(None, 'tp')
- w_down: bfloat16 [16384, 4096], P('tp')
Outputs:
- output 1: bfloat16 [16, 256, 4096], P(None, 'tp')
- output 2: bfloat16 [16, 256, 4096], P(None, 'tp')
- output 3: float32 [4096], replicated
- output 4: bfloat16 [4096, 32, 128], P(None, 'tp')
- output 5: bfloat16 [4096, 128], replicated
- output 6: bfloat16 [4096, 128], replicated
- output 7: bfloat16 [32, 128, 4096], P('tp')
- output 8: bfloat16 [4096, 16384], P(None, 'tp')
- output 9: bfloat16 [4096, 16384], P(None, 'tp')
- output 10: bfloat16 [16384, 4096], P('tp')
All inputs are finite; a program needn't handle non-finite values.
Results may differ from the reference program's by a relative error of at most 0.0189316.
Values are sent between devices in bfloat16 or wider.
A program may use at most 1 GiB of HBM per device.

```python
import jax
import jax.numpy as jnp
from jax import lax

BATCH_SIZE = 16
SEQ_LEN = 256
MODEL_DIM = 4096
NUM_HEADS = 32
HEAD_DIM = 128
FFN_DIM = 16384

LN_EPS = 1e-6
ROPE_BASE = 10000.0


def setup_inputs(seed: int = 0) -> dict:
    keys = jax.random.split(jax.random.key(seed), 12)
    act_shape = (BATCH_SIZE, SEQ_LEN, MODEL_DIM)
    mean_vec = jax.random.normal(keys[0], (MODEL_DIM,), jnp.float32)
    tok_scale = jnp.exp(jax.random.uniform(keys[1], (BATCH_SIZE, SEQ_LEN, 1), jnp.float32, -0.7, 0.7))
    x_in = (jax.random.normal(keys[2], act_shape, jnp.float32) + mean_vec) * tok_scale
    grad_y = jax.random.normal(keys[3], act_shape, jnp.float32)
    ln_gain = jax.random.uniform(keys[4], (MODEL_DIM,), jnp.float32, 0.2, 2.0)
    in_scale = MODEL_DIM ** -0.5
    w_query = jax.random.normal(keys[5], (MODEL_DIM, NUM_HEADS, HEAD_DIM), jnp.float32) * in_scale
    w_key = jax.random.normal(keys[6], (MODEL_DIM, HEAD_DIM), jnp.float32) * in_scale
    w_value = jax.random.normal(keys[7], (MODEL_DIM, HEAD_DIM), jnp.float32) * in_scale
    w_out = jax.random.normal(keys[8], (NUM_HEADS, HEAD_DIM, MODEL_DIM), jnp.float32) * (NUM_HEADS * HEAD_DIM) ** -0.5
    w_gate = jax.random.normal(keys[9], (MODEL_DIM, FFN_DIM), jnp.float32) * in_scale
    w_up = jax.random.normal(keys[10], (MODEL_DIM, FFN_DIM), jnp.float32) * in_scale
    w_down = jax.random.normal(keys[11], (FFN_DIM, MODEL_DIM), jnp.float32) * FFN_DIM ** -0.5
    return {
        "x_in": x_in.astype(jnp.bfloat16),
        "grad_y": grad_y.astype(jnp.bfloat16),
        "ln_gain": ln_gain,
        "w_query": w_query.astype(jnp.bfloat16),
        "w_key": w_key.astype(jnp.bfloat16),
        "w_value": w_value.astype(jnp.bfloat16),
        "w_out": w_out.astype(jnp.bfloat16),
        "w_gate": w_gate.astype(jnp.bfloat16),
        "w_up": w_up.astype(jnp.bfloat16),
        "w_down": w_down.astype(jnp.bfloat16),
    }


def as_bf16(value):
    return value + lax.stop_gradient(value.astype(jnp.bfloat16).astype(jnp.float32) - value)


def rope_tables(seq_len, head_dim):
    half_dim = head_dim // 2
    inv_freq = ROPE_BASE ** (-jnp.arange(half_dim, dtype=jnp.float32) * 2.0 / head_dim)
    angles = jnp.arange(seq_len, dtype=jnp.float32)[:, None] * inv_freq[None, :]
    return jnp.cos(angles), jnp.sin(angles)


def rotate_half(values, cos_tab, sin_tab):
    half_dim = values.shape[-1] // 2
    first_half = values[..., :half_dim]
    second_half = values[..., half_dim:]
    return jnp.concatenate([first_half * cos_tab - second_half * sin_tab, second_half * cos_tab + first_half * sin_tab], axis=-1)


def layer_forward(x_in, ln_gain, w_query, w_key, w_value, w_out, w_gate, w_up, w_down):
    residual = x_in.astype(jnp.float32)
    centered = residual - jnp.mean(residual, axis=-1, keepdims=True)
    inv_std = lax.rsqrt(jnp.mean(centered * centered, axis=-1, keepdims=True) + LN_EPS)
    normed = as_bf16(ln_gain * centered * inv_std)
    cos_tab, sin_tab = rope_tables(SEQ_LEN, HEAD_DIM)
    q_raw = jnp.einsum("bld,dnk->blnk", normed, w_query.astype(jnp.float32))
    k_raw = jnp.einsum("bld,dk->blk", normed, w_key.astype(jnp.float32))
    values = as_bf16(jnp.einsum("bld,dk->blk", normed, w_value.astype(jnp.float32)))
    q_rot = as_bf16(rotate_half(q_raw, cos_tab[:, None, :], sin_tab[:, None, :]))
    k_rot = as_bf16(rotate_half(k_raw, cos_tab, sin_tab))
    scores = jnp.einsum("bqnk,bsk->bnqs", q_rot, k_rot) * HEAD_DIM ** -0.5
    positions = jnp.arange(SEQ_LEN)
    causal = positions[:, None] >= positions[None, :]
    attn_probs = as_bf16(jax.nn.softmax(jnp.where(causal, scores, -1e30), axis=-1))
    attn_heads = as_bf16(jnp.einsum("bnqs,bsk->bqnk", attn_probs, values))
    attn_out = jnp.einsum("bqnk,nkd->bqd", attn_heads, w_out.astype(jnp.float32))
    gate_pre = jnp.einsum("bld,df->blf", normed, w_gate.astype(jnp.float32))
    up_pre = jnp.einsum("bld,df->blf", normed, w_up.astype(jnp.float32))
    hidden = as_bf16(jax.nn.silu(gate_pre) * up_pre)
    mlp_out = jnp.einsum("blf,fd->bld", hidden, w_down.astype(jnp.float32))
    return residual + attn_out + mlp_out


def reference(x_in, grad_y, ln_gain, w_query, w_key, w_value, w_out, w_gate, w_up, w_down):
    out_f32, pullback = jax.vjp(layer_forward, x_in, ln_gain, w_query, w_key, w_value, w_out, w_gate, w_up, w_down)
    gradients = pullback(grad_y.astype(jnp.float32))
    return (
        out_f32.astype(jnp.bfloat16),
        gradients[0].astype(jnp.bfloat16),
        gradients[1].astype(jnp.float32),
        gradients[2].astype(jnp.bfloat16),
        gradients[3].astype(jnp.bfloat16),
        gradients[4].astype(jnp.bfloat16),
        gradients[5].astype(jnp.bfloat16),
        gradients[6].astype(jnp.bfloat16),
        gradients[7].astype(jnp.bfloat16),
        gradients[8].astype(jnp.bfloat16),
    )
```

```python
import functools

import jax
import jax.numpy as jnp
from jax import lax
from jax.experimental import pallas as pl
from jax.experimental.pallas import tpu as pltpu
from jax.sharding import PartitionSpec as P

LN_EPS = 1e-6
ROPE_BASE = 10000.0
MESH = pl.DeviceIdType.MESH
F32 = jnp.float32
BF16 = jnp.bfloat16

GROUP = 8
SEQ = 256
DIM = 4096
HALF = DIM // 2
HEAD = 128
FFN = 512
OWN = 2 * FFN + HEAD
KEY = 2 * OWN
NCAT = 2 * OWN + 2 * HEAD
NZO = 2 * (FFN + HEAD)
QCOL = (2 * FFN, OWN + 2 * FFN)
OCOL = (2 * FFN, 2 * FFN + HEAD)


def dims():
    i = lax.axis_index("tp")
    return lax.div(i, 8), lax.rem(lax.div(i, 4), 2), lax.rem(lax.div(i, 2), 2), lax.rem(i, 2)


def index(z, y, x, core):
    return ((z * 2 + y) * 2 + x) * 2 + core


def rows8(start, size):
    return pl.ds(pl.multiple_of(start, 8), size)


def rows16(start, size):
    return pl.ds(pl.multiple_of(start, 16), size)


def lanes(start, size):
    return pl.ds(pl.multiple_of(start, 128), size)


def remote(src, dst, send, recv, target):
    return pltpu.make_async_remote_copy(src, dst, send, recv, device_id=(target,), device_id_type=MESH)


def entry_barrier(partners):
    barrier = pltpu.get_barrier_semaphore()
    for partner in partners:
        pl.semaphore_signal(barrier, inc=1, device_id=(partner,), device_id_type=MESH)
    pl.semaphore_wait(barrier, len(partners))


def dot_nt(a, b):
    return lax.dot_general(a, b, (((1,), (1,)), ((), ())), preferred_element_type=F32)


def dot_tn(a, b):
    return lax.dot_general(a, b, (((0,), (0,)), ((), ())), preferred_element_type=F32)


def dot_nn(a, b):
    return jnp.dot(a, b, preferred_element_type=F32)


def row_position(r):
    return ((r // 16) % 4) * 64 + (r // 128) * 32 + ((r // 64) % 2) * 16 + r % 16


def gather_kernel(
    h_loc, dy_loc, w1, w3, wq, wk, wv, w2, wo, cos_t, sin_t,
    h_all, dy_all, h_sib, dy_sib, y_part, dh_part, g_all, zo_all, g_sib, zo_sib,
    wcat, w2o, hv, dyv, proj, zo, g, yo, dho, probs, qs, stage,
    s1, r1, s2, r2, s3, r3, sx, rx, sw, rw, ss, rs, sg, rg, lsem, wsem, osem, gsem,
):
    z, y, x, core = dims()
    sib = index(z, y, x, 1 - core)
    xn = index(z, y, 1 - x, core)
    yn = index(z, 1 - y, x, core)
    zn = [index(lax.rem(z + k, 4), y, x, core) for k in (1, 2, 3)]
    entry_barrier([sib, xn, yn] + zn)
    row0 = (y * 2 + x) * 64 + z * 16
    full = ((h_loc, h_all, h_sib), (dy_loc, dy_all, dy_sib))

    swaps = []
    for s, (loc, out, _) in enumerate(full):
        swaps.append(remote(loc.at[rows8(8 * (1 - core), 8)], out.at[:, rows8(row0 + 8 * core, 8), :], sx.at[s], rx.at[s], sib))
    for c in swaps:
        c.start()
    takes = [pltpu.make_async_copy(loc.at[rows8(8 * core, 8)], stage.at[s], lsem.at[s]) for s, (loc, _, _) in enumerate(full)]
    for c in takes:
        c.start()
    puts = []
    for s, (_, out, _) in enumerate(full):
        takes[s].wait()
        c = pltpu.make_async_copy(stage.at[s], out.at[:, rows8(row0 + 8 * core, 8), :], lsem.at[s])
        c.start()
        puts.append(c)
    for c in puts:
        c.wait()
    for c in swaps:
        c.wait_recv()

    def p1(b, s):
        out = full[s][1]
        block = out.at[b, rows16(row0, 16), :]
        return [remote(block, block, s1.at[b, s, k], r1.at[b, s, k], zn[k]) for k in range(3)]

    def p2(b, s):
        out = full[s][1]
        rows = rows16((y * 2 + x) * 64, 64)
        left = out.at[b, rows, 0:HALF]
        right = out.at[b, rows, HALF:DIM]
        return [remote(left, left, s2.at[b, s, 0], r2.at[b, s, 0], yn), remote(right, right, s2.at[b, s, 1], r2.at[b, s, 1], xn)]

    def p3(b, s):
        out = full[s][1]
        copies = []
        for k in range(2):
            left = out.at[b, rows16((k * 2 + x) * 64, 64), 0:HALF]
            copies.append(remote(left, left, s3.at[b, s, k], r3.at[b, s, k], xn))
        right = out.at[b, rows16(y * 128, 128), HALF:DIM]
        copies.append(remote(right, right, s3.at[b, s, 2], r3.at[b, s, 2], yn))
        return copies

    def start(copies):
        for c in copies:
            c.start()

    def wait_recv(copies):
        for c in copies:
            c.wait_recv()

    def step2(b, s):
        wait_recv(p1(b, s))
        start(p2(b, s))

    def step3(b, s):
        wait_recv(p2(b, s))
        start(p3(b, s))

    for b in range(2):
        for s in range(2):
            start(p1(b, s))

    pieces = ((w1, 0, FFN), (w3, FFN, FFN), (wq, 2 * FFN, HEAD))
    local = []
    for k, (w, col, width) in enumerate(pieces):
        local.append(pltpu.make_async_copy(w, wcat.at[:, col : col + width], wsem.at[k]))
    local.append(pltpu.make_async_copy(wk, wcat.at[:, KEY : KEY + HEAD], wsem.at[3]))
    local.append(pltpu.make_async_copy(wv, wcat.at[:, KEY + HEAD : NCAT], wsem.at[4]))
    local.append(pltpu.make_async_copy(w2, w2o.at[0:FFN], wsem.at[5]))
    local.append(pltpu.make_async_copy(wo, w2o.at[2 * FFN : 2 * FFN + HEAD], wsem.at[6]))
    far = []
    for k, (w, col, width) in enumerate(pieces):
        far.append(remote(w, wcat.at[:, OWN + col : OWN + col + width], sw.at[k], rw.at[k], sib))
    far.append(remote(w2, w2o.at[FFN : 2 * FFN], sw.at[3], rw.at[3], sib))
    far.append(remote(wo, w2o.at[2 * FFN + HEAD : NZO], sw.at[4], rw.at[4], sib))
    start(local)
    start(far)

    for b in range(2):
        for s in range(2):
            start(p1(b + 2, s))
            step2(b, s)
            if b == 0:
                step3(b, s)
    for c in local:
        c.wait()
    wait_recv(far)

    def sib_copies(b):
        copies = [remote(out.at[b], far_out.at[b], ss.at[b, s], rs.at[b, s], sib) for s, (_, out, far_out) in enumerate(full)]
        return copies

    def gz_copies(b):
        return [
            remote(g.at[:, OWN : 2 * OWN], g_sib.at[b], sg.at[b, 0], rg.at[b, 0], sib),
            remote(zo.at[:, FFN : 2 * FFN], zo_sib.at[b, :, 0:FFN], sg.at[b, 1], rg.at[b, 1], sib),
            remote(zo.at[:, OCOL[1] : NZO], zo_sib.at[b, :, FFN : FFN + HEAD], sg.at[b, 2], rg.at[b, 2], sib),
        ]

    def gz_local(b):
        return [pltpu.make_async_copy(g, g_all.at[b], gsem.at[0]), pltpu.make_async_copy(zo, zo_all.at[b], gsem.at[1])]

    y_out = lambda b: pltpu.make_async_copy(yo, y_part.at[b], osem.at[0])
    dh_out = lambda b: pltpu.make_async_copy(dho, dh_part.at[b], osem.at[1])
    scale = HEAD ** -0.5

    def rotate(v, sign):
        return v * cos_t[...] + sign * (pltpu.roll(v, HEAD // 2, 1) * sin_t[...])

    def batch_step(b, carry):
        wait_recv(p3(b, 0))
        load_h = pltpu.make_async_copy(h_all.at[b], hv, lsem.at[0])
        load_h.start()

        @pl.when(b < GROUP - 1)
        def _():
            step3(b + 1, 0)

        @pl.when(b < GROUP - 2)
        def _():
            step2(b + 2, 0)

        wait_recv(p3(b, 1))
        load_dy = pltpu.make_async_copy(dy_all.at[b], dyv, lsem.at[1])
        load_dy.start()
        start(sib_copies(b))
        load_h.wait()

        def proj_tile(t, c):
            proj[:, lanes(t * 512, 512)] = dot_nn(hv[...], wcat[:, lanes(t * 512, 512)])
            return c

        lax.fori_loop(0, NCAT // 512, proj_tile, 0)

        @pl.when(b < GROUP - 1)
        def _():
            step3(b + 1, 1)

        @pl.when(b < GROUP - 2)
        def _():
            step2(b + 2, 1)

        @pl.when(b < GROUP - 4)
        def _():
            for s in range(2):
                start(p1(b + 4, s))

        @pl.when(b > 0)
        def _():
            for c in gz_local(b - 1):
                c.wait()
            for c in gz_copies(b - 1):
                c.wait_send()
            y_out(b - 1).wait()
            dh_out(b - 1).wait()

        def hidden_tile(t, c):
            at = t * 256 + lax.div(t, 2) * (OWN - FFN)
            gate = proj[:, lanes(at, 256)]
            up = proj[:, lanes(at + FFN, 256)]
            zo[:, lanes(t * 256, 256)] = (gate * jax.nn.sigmoid(gate) * up).astype(BF16)
            return c

        lax.fori_loop(0, 4, hidden_tile, 0)

        keys = rotate(proj[:, KEY : KEY + HEAD], 1.0).astype(BF16)
        vals = proj[:, KEY + HEAD : NCAT].astype(BF16)
        qs[2] = keys
        qs[3] = vals
        q_pos = row_position(lax.broadcasted_iota(jnp.int32, (SEQ, SEQ), 0))
        k_pos = row_position(lax.broadcasted_iota(jnp.int32, (SEQ, SEQ), 1))
        causal = q_pos >= k_pos
        for hd in range(2):
            query = rotate(proj[:, QCOL[hd] : QCOL[hd] + HEAD], 1.0).astype(BF16)
            qs[hd] = query
            scores = jnp.where(causal, dot_nt(query, keys) * scale, -1e30)
            e = jnp.exp(scores - jnp.max(scores, axis=-1, keepdims=True))
            p = e / jnp.sum(e, axis=-1, keepdims=True)
            probs[hd] = p
            zo[:, OCOL[hd] : OCOL[hd] + HEAD] = dot_nn(p.astype(BF16), vals).astype(BF16)

        def y_tile(n, c):
            yo[:, lanes(n * 512, 512)] = dot_nn(zo[...], w2o[:, lanes(n * 512, 512)]).astype(BF16)
            return c

        lax.fori_loop(0, DIM // 512, y_tile, 0)
        y_out(b).start()
        load_dy.wait()

        def dz_tile(t, c):
            dz = dot_nt(dyv[...], w2o[rows16(t * 256, 256), :])
            at = t * 256 + lax.div(t, 2) * (OWN - FFN)
            gate = proj[:, lanes(at, 256)]
            up = proj[:, lanes(at + FFN, 256)]
            sig = jax.nn.sigmoid(gate)
            g[:, lanes(at, 256)] = (dz * up * sig * (1.0 + gate * (1.0 - sig))).astype(BF16)
            g[:, lanes(at + FFN, 256)] = (dz * (gate * sig)).astype(BF16)
            return c

        lax.fori_loop(0, 4, dz_tile, 0)
        d_heads = dot_nt(dyv[...], w2o[2 * FFN : NZO, :]).astype(BF16)
        d_keys = jnp.zeros((SEQ, HEAD), F32)
        d_vals = jnp.zeros((SEQ, HEAD), F32)
        for hd in range(2):
            d_out = d_heads[:, hd * HEAD : (hd + 1) * HEAD]
            p = probs[hd]
            d_probs = dot_nt(d_out, qs[3])
            d_vals = d_vals + dot_tn(p.astype(BF16), d_out)
            row_dot = jnp.sum(p * d_probs, axis=-1, keepdims=True)
            d_scores = (p * (d_probs - row_dot) * scale).astype(BF16)
            g[:, QCOL[hd] : QCOL[hd] + HEAD] = rotate(dot_nn(d_scores, qs[2]), -1.0).astype(BF16)
            d_keys = d_keys + dot_tn(d_scores, qs[hd])
        g[:, KEY : KEY + HEAD] = rotate(d_keys, -1.0).astype(BF16)
        g[:, KEY + HEAD : NCAT] = d_vals.astype(BF16)

        def dh_tile(n, c):
            dho[:, lanes(n * 512, 512)] = dot_nt(g[...], wcat[rows16(n * 512, 512), :]).astype(BF16)
            return c

        lax.fori_loop(0, DIM // 512, dh_tile, 0)
        dh_out(b).start()
        start(gz_local(b))
        start(gz_copies(b))
        return carry

    lax.fori_loop(0, GROUP, batch_step, 0)

    last = GROUP - 1
    for c in gz_local(last):
        c.wait()
    y_out(last).wait()
    dh_out(last).wait()
    for c in gz_copies(last):
        c.wait_send()

    def finish(b, carry):
        for s in range(2):
            for c in p1(b, s) + p2(b, s) + p3(b, s):
                c.wait_send()
        for c in sib_copies(b):
            c.wait()
        wait_recv(gz_copies(b))
        return carry

    lax.fori_loop(0, GROUP, finish, 0)
    for c in swaps:
        c.wait_send()
    for c in far:
        c.wait_send()


def gather_call(h_loc, dy_loc, w1, w3, wq, wk, wv, w2, wo, cos_t, sin_t):
    any_spec = pl.BlockSpec(memory_space=pl.ANY)
    vmem_spec = pl.BlockSpec(memory_space=pltpu.VMEM)
    dma = pltpu.SemaphoreType.DMA
    shapes = [(GROUP, SEQ, DIM)] * 6 + [(GROUP, SEQ, NCAT), (GROUP, SEQ, NZO), (GROUP, SEQ, OWN), (GROUP, SEQ, FFN + HEAD)]
    return pl.pallas_call(
        gather_kernel,
        out_shape=[jax.ShapeDtypeStruct(s, BF16) for s in shapes],
        in_specs=[any_spec] * 9 + [vmem_spec] * 2,
        out_specs=[any_spec] * len(shapes),
        scratch_shapes=[
            pltpu.VMEM((DIM, NCAT), BF16),
            pltpu.VMEM((NZO, DIM), BF16),
            pltpu.VMEM((SEQ, DIM), BF16),
            pltpu.VMEM((SEQ, DIM), BF16),
            pltpu.VMEM((SEQ, NCAT), F32),
            pltpu.VMEM((SEQ, NZO), BF16),
            pltpu.VMEM((SEQ, NCAT), BF16),
            pltpu.VMEM((SEQ, DIM), BF16),
            pltpu.VMEM((SEQ, DIM), BF16),
            pltpu.VMEM((2, SEQ, SEQ), F32),
            pltpu.VMEM((4, SEQ, HEAD), BF16),
            pltpu.VMEM((2, 8, 8, DIM), BF16),
            dma((GROUP, 2, 3)), dma((GROUP, 2, 3)),
            dma((GROUP, 2, 2)), dma((GROUP, 2, 2)),
            dma((GROUP, 2, 3)), dma((GROUP, 2, 3)),
            dma((2,)), dma((2,)),
            dma((5,)), dma((5,)),
            dma((GROUP, 2)), dma((GROUP, 2)),
            dma((GROUP, 3)), dma((GROUP, 3)),
            dma((2,)), dma((7,)), dma((2,)), dma((2,)),
        ],
        compiler_params=pltpu.CompilerParams(collective_id=0, has_side_effects=True, vmem_limit_bytes=60 * 1024 * 1024),
        name="gather_layer",
    )(h_loc, dy_loc, w1, w3, wq, wk, wv, w2, wo, cos_t, sin_t)


ITEMS = 2 * GROUP


def scatter_kernel(y_part, dh_part, y_sum, dh_sum, b1, b2, b3, own, fin, s1, r1, s2, r2, s3, r3, osem, fsem, ssem, rsem):
    z, y, x, core = dims()
    sib = index(z, y, x, 1 - core)
    xn = index(z, y, 1 - x, core)
    yn = index(z, 1 - y, x, core)
    zn = [index(lax.rem(z + k, 4), y, x, core) for k in (1, 2, 3)]
    entry_barrier([sib, xn, yn] + zn)
    parts = (y_part, dh_part)
    sums = (y_sum, dh_sum)

    def q1(b, s):
        n = 2 * b + s
        copies = []
        for k in range(2):
            src = parts[s].at[b, rows16((k * 2 + 1 - x) * 64, 64), 0:HALF]
            copies.append(remote(src, b1.at[n, 0, k * 64 : k * 64 + 64], s1.at[n, k], r1.at[n, k], xn))
        src = parts[s].at[b, rows16((1 - y) * 128, 128), HALF:DIM]
        copies.append(remote(src, b1.at[n, 1], s1.at[n, 2], r1.at[n, 2], yn))
        return copies

    def load(b, s):
        copies = []
        for k in range(2):
            src = parts[s].at[b, rows16((k * 2 + x) * 64, 64), 0:HALF]
            copies.append(pltpu.make_async_copy(src, own.at[s, 0, k * 64 : k * 64 + 64], osem.at[s, k]))
        src = parts[s].at[b, rows16(y * 128, 128), HALF:DIM]
        copies.append(pltpu.make_async_copy(src, own.at[s, 1], osem.at[s, 2]))
        return copies

    def q2(n):
        return [
            remote(b1.at[n, 0, rows16((1 - y) * 64, 64)], b2.at[n, 0], s2.at[n, 0], r2.at[n, 0], yn),
            remote(b1.at[n, 1, rows16((1 - x) * 64, 64)], b2.at[n, 1], s2.at[n, 1], r2.at[n, 1], xn),
        ]

    def q3(n):
        copies = []
        for k in range(3):
            rows = rows16(lax.rem(z + k + 1, 4) * 16, 16)
            copies.append(remote(b2.at[n, :, rows, :], b3.at[n, k], s3.at[n, k], r3.at[n, k], zn[k]))
        return copies

    def store(b, s):
        n = 2 * b + s
        far = remote(fin.at[n, 1 - core], sums[s].at[8 * core + b], ssem.at[n], rsem.at[n], sib)
        near = pltpu.make_async_copy(fin.at[n, core], sums[s].at[8 * core + b], fsem.at[n])
        return far, near

    def start(copies):
        for c in copies:
            c.start()

    def wait_recv(copies):
        for c in copies:
            c.wait_recv()

    def add1(b, s):
        n = 2 * b + s
        wait_recv(q1(b, s))
        for c in load(b, s):
            c.wait()

        def tile(t, c):
            cols = lanes(t * 256, 256)
            for k in range(2):
                b1[n, k, :, cols] = (b1[n, k, :, cols].astype(F32) + own[s, k, :, cols].astype(F32)).astype(BF16)
            return c

        lax.fori_loop(0, HALF // 256, tile, 0)
        start(q2(n))

    def add2(n):
        wait_recv(q2(n))

        def tile(t, c):
            cols = lanes(t * 256, 256)
            mine = (rows16(y * 64, 64), rows16(x * 64, 64))
            for k in range(2):
                b2[n, k, :, cols] = (b2[n, k, :, cols].astype(F32) + b1[n, k, mine[k], cols].astype(F32)).astype(BF16)
            return c

        lax.fori_loop(0, HALF // 256, tile, 0)
        start(q3(n))

    def add3(b, s):
        n = 2 * b + s
        wait_recv(q3(n))

        def tile(t, c):
            cols = lanes(t * 256, 256)
            for k in range(2):
                total = b2[n, k, rows16(z * 16, 16), cols].astype(F32)
                for j in range(3):
                    total = total + b3[n, j, k, :, cols].astype(F32)
                fin[n, 0, :, lanes(k * HALF + t * 256, 256)] = total[0:8].astype(BF16)
                fin[n, 1, :, lanes(k * HALF + t * 256, 256)] = total[8:16].astype(BF16)
            return c

        lax.fori_loop(0, HALF // 256, tile, 0)
        start(store(b, s))

    for s in range(2):
        start(load(0, s))
    for b in range(2):
        for s in range(2):
            start(q1(b, s))

    def step(b, carry):
        for s in range(2):
            n = 2 * b + s

            @pl.when(b < GROUP)
            def _():
                add1(b, s)

            @pl.when(b < GROUP - 1)
            def _():
                start(load(b + 1, s))

            @pl.when(b < GROUP - 2)
            def _():
                start(q1(b + 2, s))

            @pl.when((n >= 1) & (n < ITEMS + 1))
            def _():
                add2(n - 1)

            @pl.when((n >= 2) & (n < ITEMS + 2))
            def _():
                add3(b - 1, s)

        return carry

    lax.fori_loop(0, GROUP + 1, step, 0)

    def finish(b, carry):
        for s in range(2):
            n = 2 * b + s
            for c in q1(b, s) + q2(n) + q3(n):
                c.wait_send()
            far, near = store(b, s)
            near.wait()
            far.wait()
        return carry

    lax.fori_loop(0, GROUP, finish, 0)


def scatter_call(y_part, dh_part):
    any_spec = pl.BlockSpec(memory_space=pl.ANY)
    dma = pltpu.SemaphoreType.DMA
    return pl.pallas_call(
        scatter_kernel,
        out_shape=[jax.ShapeDtypeStruct((2 * GROUP, 8, DIM), BF16)] * 2,
        in_specs=[any_spec] * 2,
        out_specs=[any_spec] * 2,
        scratch_shapes=[
            pltpu.VMEM((ITEMS, 2, 128, HALF), BF16),
            pltpu.VMEM((ITEMS, 2, 64, HALF), BF16),
            pltpu.VMEM((ITEMS, 3, 2, 16, HALF), BF16),
            pltpu.VMEM((2, 2, 128, HALF), BF16),
            pltpu.VMEM((ITEMS, 2, 8, DIM), BF16),
            dma((ITEMS, 3)), dma((ITEMS, 3)),
            dma((ITEMS, 2)), dma((ITEMS, 2)),
            dma((ITEMS, 3)), dma((ITEMS, 3)),
            dma((2, 3)), dma((ITEMS,)), dma((ITEMS,)), dma((ITEMS,)),
        ],
        compiler_params=pltpu.CompilerParams(collective_id=1, has_side_effects=True, vmem_limit_bytes=48 * 1024 * 1024),
        name="scatter_sums",
    )(y_part, dh_part)


def rope_tables():
    half = HEAD // 2
    inv_freq = ROPE_BASE ** (-jnp.arange(half, dtype=F32) * 2.0 / HEAD)
    pos = row_position(jnp.arange(SEQ, dtype=jnp.int32)).astype(F32)
    angles = pos[:, None] * inv_freq[None, :]
    cos, sin = jnp.cos(angles), jnp.sin(angles)
    return jnp.concatenate([cos, cos], axis=1), jnp.concatenate([-sin, sin], axis=1)


def solution(mesh):
    def layer_shard(x_loc, dy_loc, ln_gain, w_query, w_key, w_value, w_out, w_gate, w_up, w_down):
        residual = x_loc.astype(F32)
        centered = residual - jnp.mean(residual, axis=-1, keepdims=True)
        inv_std = lax.rsqrt(jnp.mean(centered * centered, axis=-1, keepdims=True) + LN_EPS)
        x_hat = centered * inv_std
        h_loc = (ln_gain * x_hat).astype(BF16)
        cos_t, sin_t = rope_tables()
        wq = w_query.reshape(DIM, HEAD)
        wo = w_out.reshape(HEAD, DIM)
        h_all, dy_all, h_sib, dy_sib, y_part, dh_part, g_all, zo_all, g_sib, zo_sib = gather_call(
            h_loc, dy_loc, w_gate, w_up, wq, w_key, w_value, w_down, wo, cos_t, sin_t
        )

        def grad_in(lo, hi):
            near = jnp.einsum("bld,blf->df", h_all, g_all[:, :, lo:hi], preferred_element_type=F32)
            return (near + jnp.einsum("bld,blf->df", h_sib, g_sib[:, :, lo:hi], preferred_element_type=F32)).astype(BF16)

        def grad_out(lo, hi, sib_lo, sib_hi):
            near = jnp.einsum("blf,bld->fd", zo_all[:, :, lo:hi], dy_all, preferred_element_type=F32)
            return (near + jnp.einsum("blf,bld->fd", zo_sib[:, :, sib_lo:sib_hi], dy_sib, preferred_element_type=F32)).astype(BF16)

        grad_w_gate = grad_in(0, FFN)
        grad_w_up = grad_in(FFN, 2 * FFN)
        grad_w_query = grad_in(2 * FFN, OWN).reshape(DIM, 1, HEAD)
        grad_w_down = grad_out(0, FFN, 0, FFN)
        grad_w_out = grad_out(OCOL[0], OCOL[0] + HEAD, FFN, FFN + HEAD).reshape(1, HEAD, DIM)
        grad_kv = lax.psum(jnp.einsum("bld,blk->dk", h_all, g_all[:, :, KEY:NCAT], preferred_element_type=F32), "tp")

        y_sum, dh_sum = scatter_call(y_part, dh_part)
        y_loc = (residual + y_sum.astype(F32)).astype(BF16)
        grad_normed = dh_sum.astype(F32)
        grad_gain = lax.psum(jnp.sum(grad_normed * x_hat, axis=(0, 1)), "tp")
        grad_hat = grad_normed * ln_gain
        grad_x = (
            inv_std * (grad_hat - jnp.mean(grad_hat, axis=-1, keepdims=True) - x_hat * jnp.mean(grad_hat * x_hat, axis=-1, keepdims=True))
            + dy_loc.astype(F32)
        )
        return (
            y_loc,
            grad_x.astype(BF16),
            grad_gain,
            grad_w_query,
            grad_kv[:, 0:HEAD].astype(BF16),
            grad_kv[:, HEAD:].astype(BF16),
            grad_w_out,
            grad_w_gate,
            grad_w_up,
            grad_w_down,
        )

    act_spec = P(None, "tp", None)
    weight_specs = (P(), P(None, "tp", None), P(), P(), P("tp", None, None), P(None, "tp"), P(None, "tp"), P("tp", None))
    return jax.shard_map(layer_shard, mesh=mesh, in_specs=(act_spec, act_spec) + weight_specs, out_specs=(act_spec, act_spec) + weight_specs, check_vma=False)
```

```python
import jax
import jax.numpy as jnp
from jax import lax
from jax.experimental import pallas as pl
from jax.experimental.pallas import tpu as pltpu
from jax.sharding import PartitionSpec as P

LN_EPS = 1e-6
ROPE_BASE = 10000.0
MESH = pl.DeviceIdType.MESH
F32 = jnp.float32
BF16 = jnp.bfloat16
ALL = slice(None)
PAIR = range(2)
LANES = 128
W = 256
VMEM_BYTES = 67043328

GROUP = 8
ITEMS = 2 * GROUP
ROWS = 8
BLOCK = 2 * ROWS
LINE = 4 * BLOCK
SEQ = 4 * LINE
TALL = (2, 2, LINE)
DIM = 4096
HEAD = 128
FFN = 512
OUT = FFN + HEAD
OWN = 2 * FFN + HEAD
KEY = 2 * OWN
VAL = KEY + HEAD
NCAT = VAL + HEAD
NZO = 2 * OUT
QCOL = (2 * FFN, OWN + 2 * FFN)
OCOL = (2 * FFN, 2 * FFN + HEAD)
NEAR = GROUP * SEQ

EARLY = 5
DEPTH = 5
COPIES = 14


class Columns:
    def __init__(self, a):
        self.a, self.c = a, DIM // 2 - a
        self.left = (slice(0, a), slice(a, 2 * a))
        self.both_left = slice(0, 2 * a)
        self.right = (slice(2 * a, 2 * a + self.c), slice(2 * a + self.c, DIM))
        self.both_right = slice(2 * a, DIM)
        self.halves = (slice(0, self.c), slice(self.c, 2 * self.c))


GCOL = Columns(1280)
SCOL = Columns(1536)


def place():
    i = lax.axis_index("tp")
    return lax.div(i, 8), lax.rem(lax.div(i, 4), 2), lax.rem(lax.div(i, 2), 2), lax.rem(i, 2)


def index(z, y, x, core):
    return ((z * 2 + y) * 2 + x) * 2 + core


def rows8(start, size):
    return pl.ds(pl.multiple_of(start, ROWS), size)


def rows16(start, size):
    return pl.ds(pl.multiple_of(start, BLOCK), size)


def lanes(start, size):
    return pl.ds(pl.multiple_of(start, LANES), size)


def step_of(t, size):
    return lanes(t * size, size)


def loop(count, body):
    lo, hi = count if isinstance(count, tuple) else (0, count)

    def run(i, carry):
        body(i)
        return carry

    lax.fori_loop(lo, hi, run, 0)


def remote(src, dst, sems, target):
    return pltpu.make_async_remote_copy(src, dst, *sems, device_id=(target,), device_id_type=MESH)


def start(copies):
    for c in copies:
        c.start()


def wait(copies):
    for c in copies:
        c.wait()


def wait_recv(copies):
    for c in copies:
        c.wait_recv()


def wait_send(copies):
    for c in copies:
        c.wait_send()


def partners_of(z, y, x, core):
    chips = [index(lax.rem(z + k, 4), y, x, core) for k in (1, 2, 3)]
    return [index(z, y, x, 1 - core), index(z, y, 1 - x, core), index(z, 1 - y, x, core)] + chips


def entry_barrier(partners):
    barrier = pltpu.get_barrier_semaphore()
    for partner in partners:
        pl.semaphore_signal(barrier, inc=1, device_id=(partner,), device_id_type=MESH)
    pl.semaphore_wait(barrier, len(partners))


def dot_nt(a, b):
    return lax.dot_general(a, b, (((1,), (1,)), ((), ())), preferred_element_type=F32)


def dot_tn(a, b):
    return lax.dot_general(a, b, (((0,), (0,)), ((), ())), preferred_element_type=F32)


def dot_nn(a, b):
    return jnp.dot(a, b, preferred_element_type=F32)


def add_into(dst, src, width):
    def tile(t):
        cols = step_of(t, W)
        dst[..., cols] = (dst[..., cols].astype(F32) + src[..., cols].astype(F32)).astype(BF16)

    loop(width // W, tile)


def row_position(r):
    return ((r // BLOCK) % 4) * LINE + (r // (2 * LINE)) * (2 * BLOCK) + ((r // LINE) % 2) * BLOCK + r % BLOCK


class Line:
    def __init__(self, z, y, x, core):
        low = lax.div(z, 2)
        odd = lax.rem(z, 2)
        self.mid = low != odd
        self.end = low == odd
        side = index(z + 1 - 2 * odd, y, x, core)
        across = index(3 - z, y, x, core)
        self.three = rows16(BLOCK - BLOCK * low, 3 * BLOCK)
        self.half = rows16(2 * BLOCK * low, 2 * BLOCK)
        self.other = rows16(2 * BLOCK - 2 * BLOCK * low, 2 * BLOCK)
        self.tip = rows16(3 * BLOCK * low, BLOCK)
        self.own = rows16(BLOCK * z, BLOCK)
        self.spread = ((self.own, side), (self.half, across), (self.three, side))
        self.merge = ((self.three, side), (self.other, across), (self.tip, side))


class Transfer:
    def __init__(self, spot, send, recv, lo, hi):
        self.z, self.y, self.x, self.core = spot
        self.lo, self.hi = lo, hi
        self.line = Line(*spot)
        self.sib, self.xn, self.yn, *self.zn = partners_of(*spot)
        self.send, self.recv, self.keys = send, recv, {}

    def sems(self, slot, key):
        k = self.keys.setdefault(key, len(self.keys))
        return self.send.at[slot, k], self.recv.at[slot, k]

    def on_end(self, body):
        pl.when(self.line.end)(body)

    def on_mid(self, body):
        pl.when(self.line.mid)(body)

    def tick(self, m):
        for k, stage in reversed(list(enumerate(self.stages))):
            n = m - k

            @pl.when((n >= self.lo) & (n < self.hi))
            def _(stage=stage, n=n):
                stage(n)


class Gather(Transfer):
    def __init__(self, spot, buf, send, recv):
        super().__init__(spot, send, recv, 0, ITEMS)
        self.buf = buf
        self.stages = (self.stage0, self.stage1, self.stage2, self.stage3, self.stage4, self.stage5)

    def copy(self, n, key, ys, xs, rows, cols, target):
        view = self.buf.at[lax.div(n, 2), lax.rem(n, 2), ys, xs, rows, cols]
        return remote(view, view, self.sems(n, key), target)

    def za(self, n, step):
        rows, target = self.line.spread[step]
        return self.copy(n, ("za", step), self.y, self.x, rows, GCOL.both_left, target)

    def zc(self, n, step):
        rows, target = self.line.spread[step]
        return self.copy(n, ("zc", step), ALL, ALL, rows, GCOL.both_right, target)

    def c1(self, n):
        cols, own = GCOL.right, self.line.own
        return [self.copy(n, "c1x", self.y, self.x, own, cols[0], self.xn), self.copy(n, "c1y", self.y, self.x, own, cols[1], self.yn)]

    def c2(self, n):
        cols, own = GCOL.right, self.line.own
        return [self.copy(n, "c2y", self.y, ALL, own, cols[0], self.yn), self.copy(n, "c2x", ALL, self.x, own, cols[1], self.xn)]

    def a1(self, n):
        cols = GCOL.left
        return [self.copy(n, "a1y", self.y, self.x, ALL, cols[0], self.yn), self.copy(n, "a1x", self.y, self.x, ALL, cols[1], self.xn)]

    def a2(self, n):
        cols = GCOL.left
        return [self.copy(n, "a2x", ALL, self.x, ALL, cols[0], self.xn), self.copy(n, "a2y", self.y, ALL, ALL, cols[1], self.yn)]

    def pass_on(self, chain, n, step):
        def body():
            chain(n, step - 1).wait_recv()
            chain(n, step).start()

        self.on_mid(body)

    def stage0(self, n):
        self.on_end(lambda: self.za(n, 0).start())
        start(self.c1(n))

    def stage1(self, n):
        self.pass_on(self.za, n, 1)
        wait_recv(self.c1(n))
        start(self.c2(n))

    def stage2(self, n):
        self.pass_on(self.za, n, 2)
        wait_recv(self.c2(n))
        self.on_end(lambda: self.zc(n, 0).start())

    def stage3(self, n):
        self.on_end(lambda: self.za(n, 2).wait_recv())
        start(self.a1(n))
        self.pass_on(self.zc, n, 1)

    def stage4(self, n):
        wait_recv(self.a1(n))
        start(self.a2(n))
        self.pass_on(self.zc, n, 2)

    def stage5(self, n):
        wait_recv(self.a2(n))
        self.on_end(lambda: self.zc(n, 2).wait_recv())

    def finish(self, n):
        wait_send(self.c1(n) + self.c2(n) + self.a1(n) + self.a2(n))
        self.on_end(lambda: wait_send([self.za(n, 0), self.zc(n, 0)]))
        self.on_mid(lambda: wait_send([chain(n, step) for chain in (self.za, self.zc) for step in (1, 2)]))


def scatter_shapes():
    a, c = SCOL.a, SCOL.c
    return dict(
        b1=(4, 2, 2, LINE, a), b2=(6, 2, LINE, a), za0=(3, 2, 3 * BLOCK, a), za1=(3, 2, 2 * BLOCK, a), za2=(4, 2, BLOCK, a),
        own_a=(2, 2, 2, LINE, a), own_c=(4, *TALL, 2 * c), zc0=(4, 2, 2, 3 * BLOCK, 2 * c), zc1=(3, 2, 2, 2 * BLOCK, 2 * c),
        zc2=(5, 2, 2, BLOCK, 2 * c), h1=(3, 2, 2, BLOCK, c), h2=(3, 2, BLOCK, c), fin=(3, 2, ROWS, DIM),
    )


SLOTS = 6


def scatter_scratch():
    dma = pltpu.SemaphoreType.DMA
    buffers = [pltpu.VMEM(s, BF16) for s in scatter_shapes().values()]
    return buffers + [dma((SLOTS, COPIES)), dma((SLOTS, COPIES)), dma((SLOTS, 3)), dma((ITEMS,)), dma((ITEMS,)), dma((ITEMS,))]


class Scatter(Transfer):
    def __init__(self, spot, parts, sums, lo, hi, refs):
        shapes = scatter_shapes()
        self.depth = {name: s[0] for name, s in shapes.items()}
        self.ring = dict(zip(shapes, refs))
        send, recv, self.lsem, *self.store_sems = refs[len(shapes) :]
        super().__init__(spot, send, recv, lo, hi)
        self.parts, self.sums = parts, sums
        self.stages = (self.stage0, self.stage1, self.stage2, self.stage3, self.stage4, self.stage5)

    def slot(self, name, n, *at):
        return self.ring[name].at[(lax.rem(n, self.depth[name]), *at)]

    def copy(self, n, key, src, dst, target):
        return remote(src, dst, self.sems(lax.rem(n, SLOTS), key), target)

    def a1(self, n):
        cols = SCOL.left
        return [
            self.copy(n, "a1x", self.parts.at[n, :, 1 - self.x, :, cols[0]], self.slot("b1", n, 0), self.xn),
            self.copy(n, "a1y", self.parts.at[n, 1 - self.y, :, :, cols[1]], self.slot("b1", n, 1), self.yn),
        ]

    def a2(self, n):
        return [
            self.copy(n, "a2y", self.slot("b1", n, 0, 1 - self.y), self.slot("b2", n, 0), self.yn),
            self.copy(n, "a2x", self.slot("b1", n, 1, 1 - self.x), self.slot("b2", n, 1), self.xn),
        ]

    def za(self, n, step):
        rows, target = self.line.merge[step]
        key = f"za{step}"
        return self.copy(n, key, self.slot("b2", n, ALL, rows, ALL), self.slot(key, n), target)

    def zc(self, n, step):
        rows, target = self.line.merge[step]
        key = f"zc{step}"
        src = self.slot("own_c", n, ALL, ALL, rows, ALL) if step else self.parts.at[n, :, :, rows, SCOL.both_right]
        return self.copy(n, key, src, self.slot(key, n), target)

    def h1(self, n):
        cols = SCOL.halves
        return [
            self.copy(n, "h1y", self.slot("zc2", n, 1 - self.y, ALL, ALL, cols[0]), self.slot("h1", n, 0), self.yn),
            self.copy(n, "h1x", self.slot("zc2", n, ALL, 1 - self.x, ALL, cols[1]), self.slot("h1", n, 1), self.xn),
        ]

    def h2(self, n):
        cols = SCOL.halves
        return [
            self.copy(n, "h2x", self.slot("zc2", n, self.y, 1 - self.x, ALL, cols[0]), self.slot("h2", n, 0), self.xn),
            self.copy(n, "h2y", self.slot("zc2", n, 1 - self.y, self.x, ALL, cols[1]), self.slot("h2", n, 1), self.yn),
        ]

    def loads(self, n):
        sem = self.lsem.at[lax.rem(n, SLOTS)]
        views = (
            (self.parts.at[n, :, self.x, :, SCOL.left[0]], self.slot("own_a", n, 0)),
            (self.parts.at[n, self.y, :, :, SCOL.left[1]], self.slot("own_a", n, 1)),
            (self.parts.at[n, :, :, :, SCOL.both_right], self.slot("own_c", n)),
        )
        return [pltpu.make_async_copy(src, dst, sem.at[k]) for k, (src, dst) in enumerate(views)]

    def store(self, n):
        to = self.sums.at[lax.rem(n, 2), self.core, lax.div(n, 2) - self.lo // 2]
        near, send, recv = self.store_sems
        far = remote(self.slot("fin", n, 1 - self.core), to, (send.at[n], recv.at[n]), self.sib)
        return pltpu.make_async_copy(self.slot("fin", n, self.core), to, near.at[n]), far

    def stored(self, n):
        near, far = self.store(n)
        near.wait()
        far.wait_send()

    def stage0(self, n):
        start(self.a1(n))
        self.on_end(lambda: self.zc(n, 0).start())
        start(self.loads(n))

    def stage1(self, n):
        wait(self.loads(n))
        wait_recv(self.a1(n))
        for c in PAIR:
            add_into(self.slot("b1", n, c), self.slot("own_a", n, c), SCOL.a)
        start(self.a2(n))

        def middle():
            self.zc(n, 0).wait_recv()
            add_into(self.slot("own_c", n, ALL, ALL, self.line.three), self.slot("zc0", n), 2 * SCOL.c)
            self.zc(n, 1).start()

        self.on_mid(middle)
        wait_send(self.a1(n))
        self.on_end(lambda: self.zc(n, 0).wait_send())

    def stage2(self, n):
        wait_recv(self.a2(n))
        for c, mine in enumerate((self.y, self.x)):
            add_into(self.slot("b2", n, c), self.slot("b1", n, c, mine), SCOL.a)
        self.on_end(lambda: self.za(n, 0).start())

        def middle():
            self.zc(n, 1).wait_recv()
            add_into(self.slot("own_c", n, ALL, ALL, self.line.half), self.slot("zc1", n), 2 * SCOL.c)
            self.zc(n, 2).start()
            self.zc(n, 1).wait_send()

        self.on_mid(middle)
        wait_send(self.a2(n))

    def stage3(self, n):
        own_c = self.slot("own_c", n, ALL, ALL, self.line.own)

        def middle():
            self.za(n, 0).wait_recv()
            add_into(self.slot("b2", n, ALL, self.line.three), self.slot("za0", n), SCOL.a)
            self.za(n, 1).start()
            self.slot("zc2", n)[...] = own_c[...]

        def tip():
            self.zc(n, 2).wait_recv()
            add_into(self.slot("zc2", n), own_c, 2 * SCOL.c)

        self.on_mid(middle)
        self.on_end(tip)
        start(self.h1(n))
        self.on_mid(lambda: self.zc(n, 2).wait_send())
        self.on_end(lambda: self.za(n, 0).wait_send())

    def stage4(self, n):
        def middle():
            self.za(n, 1).wait_recv()
            add_into(self.slot("b2", n, ALL, self.line.half), self.slot("za1", n), SCOL.a)
            self.za(n, 2).start()
            self.za(n, 1).wait_send()

        self.on_mid(middle)
        wait_recv(self.h1(n))
        cols = SCOL.halves
        add_into(self.slot("zc2", n, self.y, ALL, ALL, cols[0]), self.slot("h1", n, 0), SCOL.c)
        add_into(self.slot("zc2", n, ALL, self.x, ALL, cols[1]), self.slot("h1", n, 1), SCOL.c)
        start(self.h2(n))
        wait_send(self.h1(n))

    def stage5(self, n):
        pl.when(n >= self.lo + self.depth["fin"])(lambda: self.stored(n - self.depth["fin"]))

        def tip():
            self.za(n, 2).wait_recv()
            add_into(self.slot("b2", n, ALL, self.line.own), self.slot("za2", n), SCOL.a)

        self.on_end(tip)
        self.on_mid(lambda: self.za(n, 2).wait_send())
        wait_recv(self.h2(n))
        fin = self.slot("fin", n)

        def put(total, col):
            for core in PAIR:
                fin[core, :, lanes(col, W)] = total[core * ROWS : (core + 1) * ROWS].astype(BF16)

        def left(t):
            for c in PAIR:
                put(self.slot("b2", n, c, self.line.own)[:, step_of(t, W)].astype(F32), c * SCOL.a + t * W)

        def right(t):
            for c in PAIR:
                mine = self.slot("zc2", n, self.y, self.x)[:, lanes(c * SCOL.c + t * W, W)].astype(F32)
                put(mine + self.slot("h2", n, c)[:, step_of(t, W)].astype(F32), 2 * SCOL.a + c * SCOL.c + t * W)

        loop(SCOL.a // W, left)
        loop(SCOL.c // W, right)
        start(self.store(n))
        wait_send(self.h2(n))

    def finish(self):
        for n in range(self.hi - self.depth["fin"], self.hi):
            self.stored(n)
        loop((self.lo, self.hi), lambda n: wait_recv(self.store(n)[1:]))


def gather_kernel(
    h_loc, dy_loc, w1, w3, wq, wk, wv, w2, wo, cos_t, sin_t,
    full, full_sib, parts, g_all, zo_all, g_sib, zo_sib, sums,
    wcat, w2o, hv, dyv, proj, zo, g, yo, dho, probs, qs, stage,
    gsend, grecv, sx, rx, sw, rw, ss, rs, sg, rg, lsem, wsem, osem, gsem, *scatter_refs,
):
    spot = place()
    z, y, x, core = spot
    partners = partners_of(*spot)
    sib = partners[0]
    entry_barrier(partners)
    gather = Gather(spot, full, gsend, grecv)
    scatter = Scatter(spot, parts, sums, 0, 2 * EARLY, scatter_refs)

    mine = rows8(BLOCK * z + ROWS * core, ROWS)
    locs = (h_loc, dy_loc)
    to = [full.at[:, s, y, x, mine, :] for s in PAIR]
    swaps = [remote(locs[s].at[rows8(GROUP * (1 - core), GROUP)], to[s], (sx.at[s], rx.at[s]), sib) for s in PAIR]
    takes = [pltpu.make_async_copy(locs[s].at[rows8(GROUP * core, GROUP)], stage.at[s], lsem.at[s]) for s in PAIR]
    puts = [pltpu.make_async_copy(stage.at[s], to[s], lsem.at[s]) for s in PAIR]
    start(swaps + takes)
    for s in PAIR:
        takes[s].wait()
        puts[s].start()
    wait(puts)
    wait_recv(swaps)
    loop(2, gather.tick)

    spots = (
        (w1, wcat.at[:, 0:FFN], wcat.at[:, OWN : OWN + FFN]),
        (w3, wcat.at[:, FFN : 2 * FFN], wcat.at[:, OWN + FFN : OWN + 2 * FFN]),
        (wq, wcat.at[:, 2 * FFN : OWN], wcat.at[:, OWN + 2 * FFN : KEY]),
        (w2, w2o.at[0:FFN], w2o.at[FFN : 2 * FFN]),
        (wo, w2o.at[OCOL[0] : OCOL[1]], w2o.at[OCOL[1] : NZO]),
    )
    shared = ((wk, wcat.at[:, KEY:VAL]), (wv, wcat.at[:, VAL:NCAT]))
    weights = [(w, near) for w, near, _ in spots] + list(shared)
    local = [pltpu.make_async_copy(w, near, wsem.at[k]) for k, (w, near) in enumerate(weights)]
    far = [remote(w, there, (sw.at[k], rw.at[k]), sib) for k, (w, _, there) in enumerate(spots)]
    start(local + far)
    loop((2, DEPTH + 1), gather.tick)

    def load(b, s):
        return pltpu.make_async_copy(full.at[b, s], (hv, dyv)[s], lsem.at[s])

    def sib_copy(b, s):
        return remote(full.at[b, s], full_sib.at[b, s], (ss.at[b, s], rs.at[b, s]), sib)

    def arrived(b, s):
        load(b, s).start()
        sib_copy(b, s).start()

    arrived(0, 0)
    wait(local)
    wait_recv(far)

    def gz_copies(b):
        rows = rows16(b * SEQ, SEQ)
        views = (
            (g.at[:, OWN:KEY], g_sib.at[rows]),
            (zo.at[:, FFN : 2 * FFN], zo_sib.at[rows, 0:FFN]),
            (zo.at[:, OCOL[1] : NZO], zo_sib.at[rows, FFN:OUT]),
        )
        return [remote(src, dst, (sg.at[b, k], rg.at[b, k]), sib) for k, (src, dst) in enumerate(views)]

    def gz_local(b):
        rows = rows16(b * SEQ, SEQ)
        return [pltpu.make_async_copy(g, g_all.at[rows], gsem.at[0]), pltpu.make_async_copy(zo, zo_all.at[rows], gsem.at[1])]

    def out(b, s):
        return pltpu.make_async_copy((yo, dho)[s], parts.at[2 * b + s], osem.at[s])

    def drained(b):
        wait(gz_local(b) + [out(b, s) for s in PAIR])
        wait_send(gz_copies(b))

    scale = HEAD ** -0.5

    def rotate(v, back=False):
        turn = pltpu.roll(v, HEAD // 2, 1) * sin_t[...]
        return v * cos_t[...] + (-turn if back else turn)

    def flat(ref):
        return ref[...].reshape(SEQ, DIM)

    def gate_up(t):
        at = t * W + lax.div(t, 2) * (OWN - FFN)
        return lanes(at, W), lanes(at + FFN, W)

    wide = lambda t: step_of(t, FFN)

    def batch_step(b):
        gather.tick(2 * b + DEPTH + 1)
        arrived(b, 1)
        load(b, 0).wait()

        def proj_tile(t):
            proj[:, wide(t)] = dot_nn(flat(hv), wcat[:, wide(t)])

        loop(NCAT // FFN, proj_tile)
        pl.when(b > 0)(lambda: drained(b - 1))
        scatter.tick(2 * b - 2)

        def hidden_tile(t):
            gate_at, up_at = gate_up(t)
            gate = proj[:, gate_at]
            zo[:, step_of(t, W)] = (gate * jax.nn.sigmoid(gate) * proj[:, up_at]).astype(BF16)

        loop(2 * FFN // W, hidden_tile)
        keys = rotate(proj[:, KEY:VAL]).astype(BF16)
        vals = proj[:, VAL:NCAT].astype(BF16)
        qs[2] = keys
        qs[3] = vals
        causal = row_position(lax.broadcasted_iota(jnp.int32, (SEQ, SEQ), 0)) >= row_position(lax.broadcasted_iota(jnp.int32, (SEQ, SEQ), 1))
        for hd in PAIR:
            query = rotate(proj[:, QCOL[hd] : QCOL[hd] + HEAD]).astype(BF16)
            qs[hd] = query
            scores = jnp.where(causal, dot_nt(query, keys) * scale, -1e30)
            e = jnp.exp(scores - jnp.max(scores, axis=-1, keepdims=True))
            p = e / jnp.sum(e, axis=-1, keepdims=True)
            probs[hd] = p
            zo[:, OCOL[hd] : OCOL[hd] + HEAD] = dot_nn(p.astype(BF16), vals).astype(BF16)

        gather.tick(2 * b + DEPTH + 2)
        pl.when(b < GROUP - 1)(lambda: arrived(b + 1, 0))

        def y_tile(t):
            yo[:, :, :, wide(t)] = dot_nn(zo[...], w2o[:, wide(t)]).astype(BF16).reshape(*TALL, FFN)

        loop(DIM // FFN, y_tile)
        out(b, 0).start()
        load(b, 1).wait()

        def dz_tile(t):
            dz = dot_nt(flat(dyv), w2o[rows16(t * W, W), :])
            gate_at, up_at = gate_up(t)
            gate = proj[:, gate_at]
            sig = jax.nn.sigmoid(gate)
            g[:, gate_at] = (dz * proj[:, up_at] * sig * (1.0 + gate * (1.0 - sig))).astype(BF16)
            g[:, up_at] = (dz * (gate * sig)).astype(BF16)

        loop(2 * FFN // W, dz_tile)
        scatter.tick(2 * b - 1)
        d_heads = dot_nt(flat(dyv), w2o[2 * FFN : NZO, :]).astype(BF16)
        d_keys = d_vals = jnp.zeros((SEQ, HEAD), F32)
        for hd in PAIR:
            d_out = d_heads[:, hd * HEAD : (hd + 1) * HEAD]
            p = probs[hd]
            d_probs = dot_nt(d_out, qs[3])
            d_vals = d_vals + dot_tn(p.astype(BF16), d_out)
            row_dot = jnp.sum(p * d_probs, axis=-1, keepdims=True)
            d_scores = (p * (d_probs - row_dot) * scale).astype(BF16)
            g[:, QCOL[hd] : QCOL[hd] + HEAD] = rotate(dot_nn(d_scores, qs[2]), True).astype(BF16)
            d_keys = d_keys + dot_tn(d_scores, qs[hd])
        g[:, KEY:VAL] = rotate(d_keys, True).astype(BF16)
        g[:, VAL:NCAT] = d_vals.astype(BF16)

        def dh_tile(t):
            dho[:, :, :, wide(t)] = dot_nt(g[...], wcat[rows16(t * FFN, FFN), :]).astype(BF16).reshape(*TALL, FFN)

        loop(DIM // FFN, dh_tile)
        out(b, 1).start()
        start(gz_local(b) + gz_copies(b))

    loop(GROUP, batch_step)
    drained(GROUP - 1)
    loop((ITEMS - 2, 2 * EARLY + DEPTH), scatter.tick)
    scatter.finish()

    def finish(b):
        for s in PAIR:
            gather.finish(2 * b + s)
            sib_copy(b, s).wait()
        wait_recv(gz_copies(b))

    loop(GROUP, finish)
    wait_send(swaps + far)


def gather_call(*args):
    any_spec = pl.BlockSpec(memory_space=pl.ANY)
    vmem_spec = pl.BlockSpec(memory_space=pltpu.VMEM)
    dma = pltpu.SemaphoreType.DMA
    tall = (*TALL, DIM)
    shapes = [(GROUP, 2, *tall)] * 2 + [(ITEMS, *tall), (NEAR, NCAT), (NEAR, NZO), (NEAR, OWN), (NEAR, OUT), (2, 2, EARLY, ROWS, DIM)]
    vmem = [(DIM, NCAT), (NZO, DIM), tall, tall, (SEQ, NCAT), (SEQ, NZO), (SEQ, NCAT), tall, tall, (2, SEQ, SEQ), (4, SEQ, HEAD), (2, GROUP, ROWS, DIM)]
    types = [BF16] * 4 + [F32] + [BF16] * 4 + [F32] + [BF16] * 2
    pairs = [(ITEMS, COPIES), (2,), (5,), (GROUP, 2), (GROUP, 3)]
    return pl.pallas_call(
        gather_kernel,
        out_shape=[jax.ShapeDtypeStruct(s, BF16) for s in shapes],
        in_specs=[any_spec] * (len(args) - 2) + [vmem_spec] * 2,
        out_specs=[any_spec] * len(shapes),
        scratch_shapes=[
            *[pltpu.VMEM(s, t) for s, t in zip(vmem, types)],
            *[dma(s) for s in pairs for _ in PAIR],
            *[dma((k,)) for k in (2, 7, 2, 2)],
            *scatter_scratch(),
        ],
        compiler_params=pltpu.CompilerParams(collective_id=0, has_side_effects=True, vmem_limit_bytes=VMEM_BYTES),
        name="gather_layer",
    )(*args)


TILE = 512
STEPS = DIM // TILE
KV = 2 * HEAD
KCOL = OWN + OUT
NBIG = KCOL + KV
QUARTER = DIM // 4
EIGHTH = DIM // 8
KROWS = KV // 4


def scatter_kernel(
    full, full_sib, parts, g_all, zo_all, g_sib, zo_sib,
    sums, dw1, dw3, dwq, dw2, dwo, dwk, dwv,
    big, tiles, out1, outq, out2, kvp, k1, k2, k3, kc, k4, kvo,
    lsem, tsem, o1sem, o2sem, ksend, krecv, kosem, *scatter_refs,
):
    spot = place()
    z, y, x, core = spot
    partners = partners_of(*spot)
    sib, xn, yn, *zn = partners
    entry_barrier(partners)
    scatter = Scatter(spot, parts, sums, 2 * EARLY, ITEMS, scatter_refs)
    scatter.tick(2 * EARLY)

    near, away = slice(0, NEAR), slice(NEAR, 2 * NEAR)
    views = (
        (g_all.at[:, KEY:NCAT], big.at[near, KCOL:NBIG]),
        (g_all.at[:, 0:OWN], big.at[near, 0:OWN]),
        (g_sib, big.at[away, 0:OWN]),
        (zo_all.at[:, 0:FFN], big.at[near, OWN : OWN + FFN]),
        (zo_all.at[:, OCOL[0] : OCOL[1]], big.at[near, OWN + FFN : KCOL]),
        (zo_sib, big.at[away, OWN:KCOL]),
    )
    loads = [pltpu.make_async_copy(src, dst, lsem.at[k]) for k, (src, dst) in enumerate(views)]
    start(loads)

    def tile_load(u, s):
        slot = lax.rem(u, 2)
        sources = (full, full_sib)
        return [pltpu.make_async_copy(sources[k].at[:, s, :, :, :, step_of(u, TILE)], tiles.at[slot, k], tsem.at[slot, k]) for k in PAIR]

    tile_load(0, 0)[0].start()
    loads[0].wait()

    def kv_tile(u):
        pl.when(u < STEPS - 1)(lambda: tile_load(u + 1, 0)[0].start())
        tile_load(u, 0)[0].wait()
        kvp[:, step_of(u, TILE)] = dot_tn(big[near, KCOL:NBIG], tiles[lax.rem(u, 2), 0].reshape(NEAR, TILE))

    loop(STEPS, kv_tile)
    start(tile_load(0, 0))

    half = core * (DIM // 2)
    quarter = (half, half + QUARTER)
    ring = ((x, y, xn, yn), (y, x, yn, xn))
    first = [quarter[c] + ring[c][0] * EIGHTH for c in PAIR]
    second = [first[c] + ring[c][1] * W for c in PAIR]
    mine = rows16(z * KROWS, KROWS)
    hops = {}

    def hop(step, src, dst, target):
        group = hops.setdefault(step, [])
        group.append(remote(src, dst, (ksend.at[step, len(group)], krecv.at[step, len(group)]), target))

    hop(0, kvp.at[:, lanes(DIM // 2 - half, DIM // 2)], k1, sib)
    for c in PAIR:
        a, b, an, bn = ring[c]
        hop(1, kvp.at[:, lanes(quarter[c] + (1 - a) * EIGHTH, EIGHTH)], k2.at[c], an)
        hop(2, kvp.at[:, lanes(first[c] + (1 - b) * W, W)], k3.at[c], bn)
        same = kvo.at[:, lanes(second[c], W)]
        hop(5, same, same, bn)
        same = kvo.at[:, lanes(first[c], EIGHTH)]
        hop(6, same, same, an)
    for k, there in enumerate(zn):
        hop(3, kc.at[rows16(lax.rem(z + k + 1, 4) * KROWS, KROWS)], k4.at[k], there)
        for c in PAIR:
            same = kvo.at[mine, lanes(second[c], W)]
            hop(4, same, same, there)
    same = kvo.at[:, lanes(half, DIM // 2)]
    hop(7, same, same, sib)
    kv_out = [pltpu.make_async_copy(kvo.at[s * HEAD : (s + 1) * HEAD], (dwk, dwv)[s], kosem.at[s]) for s in PAIR]

    def kv_add(src, at, width):
        def tile(t):
            cols = lanes(at + t * W, W)
            kvp[:, cols] = kvp[:, cols] + src[:, step_of(t, W)]

        loop(width // W, tile)

    def kv_first():
        kv_add(k1, half, DIM // 2)

    def kv_second():
        for c in PAIR:
            kv_add(k2.at[c], first[c], EIGHTH)

    def kv_third():
        for c in PAIR:
            kc[:, c * W : (c + 1) * W] = kvp[:, lanes(second[c], W)] + k3[c]

    def kv_round():
        total = kc[mine, :] + k4[0] + k4[1] + k4[2]
        for c in PAIR:
            kvo[mine, lanes(second[c], W)] = total[:, c * W : (c + 1) * W].astype(BF16)

    works = (kv_first, kv_second, kv_third, kv_round)

    def kv_step(j):
        for step in range(len(hops)):

            @pl.when(j == step)
            def _(step=step):
                wait_recv(hops[step])
                if step < len(works):
                    works[step]()
                start(hops.get(step + 1, kv_out))

    start(hops[0])
    wait(loads[1:])

    def out_copies(u):
        slot = lax.rem(u, 2)
        rows, cols = step_of(u, TILE), step_of(u, TILE)
        sem = o1sem.at[slot]
        return [
            pltpu.make_async_copy(out1.at[slot, :, 0:FFN], dw1.at[rows], sem.at[0]),
            pltpu.make_async_copy(out1.at[slot, :, FFN : 2 * FFN], dw3.at[rows], sem.at[1]),
            pltpu.make_async_copy(outq.at[slot], dwq.at[:, cols], sem.at[2]),
        ]

    def out2_copies(u):
        slot, cols = lax.rem(u, 2), step_of(u, TILE)
        sem = o2sem.at[slot]
        return [
            pltpu.make_async_copy(out2.at[slot, 0:FFN], dw2.at[:, cols], sem.at[0]),
            pltpu.make_async_copy(out2.at[slot, FFN:OUT], dwo.at[:, cols], sem.at[1]),
        ]

    def tokens(u):
        return tiles[lax.rem(u, 2)].reshape(2 * NEAR, TILE)

    def grad_in(u):
        wait(tile_load(u, 0))
        pl.when(u < STEPS - 1)(lambda: start(tile_load(u + 1, 0)))
        pl.when(u == STEPS - 1)(lambda: start(tile_load(0, 1)))
        pl.when(u > 1)(lambda: wait(out_copies(u - 2)))
        slot = lax.rem(u, 2)
        for s in PAIR:
            out1[slot, :, s * FFN : (s + 1) * FFN] = dot_tn(tokens(u), big[:, s * FFN : (s + 1) * FFN]).astype(BF16)
        outq[slot] = dot_tn(big[:, 2 * FFN : OWN], tokens(u)).astype(BF16)
        start(out_copies(u))

    def grad_out(u):
        wait(tile_load(u, 1))
        pl.when(u < STEPS - 1)(lambda: start(tile_load(u + 1, 1)))
        pl.when(u > 1)(lambda: wait(out2_copies(u - 2)))
        out2[lax.rem(u, 2)] = dot_tn(big[:, OWN:KCOL], tokens(u)).astype(BF16)
        start(out2_copies(u))

    ticks = 2 * EARLY + 1

    def first_half(u):
        scatter.tick(ticks + u)
        grad_in(u)
        kv_step(u)

    def second_half(u):
        pl.when(lax.rem(u, 2) == 0)(lambda: scatter.tick(ticks + STEPS + lax.div(u, 2)))
        grad_out(u)

    loop(STEPS, first_half)
    loop(STEPS, second_half)
    for u in (STEPS - 2, STEPS - 1):
        wait(out_copies(u) + out2_copies(u))
    wait(kv_out)
    for group in hops.values():
        wait_send(group)
    scatter.finish()


def scatter_call(*args):
    any_spec = pl.BlockSpec(memory_space=pl.ANY)
    dma = pltpu.SemaphoreType.DMA
    shapes = [(2, 2, GROUP - EARLY, ROWS, DIM), (DIM, FFN), (DIM, FFN), (HEAD, DIM), (FFN, DIM), (HEAD, DIM), (HEAD, DIM), (HEAD, DIM)]
    half = DIM // 2
    assert STEPS + STEPS // 2 >= 2 * (GROUP - EARLY) + DEPTH - 1
    narrow = [(2 * NEAR, NBIG), (2, 2, GROUP, *TALL, TILE), (2, TILE, 2 * FFN), (2, HEAD, TILE), (2, OUT, TILE)]
    sums = [(KV, DIM), (KV, half), (2, KV, EIGHTH), (2, KV, W), (KV, 2 * W), (3, KROWS, 2 * W)]
    return pl.pallas_call(
        scatter_kernel,
        out_shape=[jax.ShapeDtypeStruct(s, BF16) for s in shapes],
        in_specs=[any_spec] * len(args),
        out_specs=[any_spec] * len(shapes),
        scratch_shapes=[
            *[pltpu.VMEM(s, BF16) for s in narrow],
            *[pltpu.VMEM(s, F32) for s in sums],
            pltpu.VMEM((KV, DIM), BF16),
            *[dma(s) for s in ((6,), (2, 2), (2, 3), (2, 2), (8, 6), (8, 6), (2,))],
            *scatter_scratch(),
        ],
        compiler_params=pltpu.CompilerParams(collective_id=1, has_side_effects=True, vmem_limit_bytes=VMEM_BYTES),
        name="scatter_grads",
    )(*args)


def total_kernel(part, out, acc, got, send, recv):
    spot = place()
    z = spot[0]
    partners = partners_of(*spot)
    entry_barrier(partners)
    near = partners[: len(partners) - 3]
    acc[0] = part[...]
    for k, there in enumerate(near):
        hop = remote(acc.at[k], got.at[k], (send.at[k], recv.at[k]), there)
        hop.start()
        hop.wait_recv()
        acc[k + 1] = acc[k] + got[k]
        hop.wait_send()
    last = len(near)
    hops = [remote(acc.at[last], out.at[z], (send.at[last + k], recv.at[last + k]), there) for k, there in enumerate(partners[last:])]
    start(hops)
    out[z] = acc[last]
    wait(hops)


def total_call(part):
    shape = (DIM // LANES, LANES)
    spec = pl.BlockSpec(memory_space=pltpu.VMEM)
    dma = pltpu.SemaphoreType.DMA
    chips = pl.pallas_call(
        total_kernel,
        out_shape=jax.ShapeDtypeStruct((4, *shape), F32),
        in_specs=[spec],
        out_specs=spec,
        scratch_shapes=[pltpu.VMEM((4, *shape), F32), pltpu.VMEM((3, *shape), F32), dma((6,)), dma((6,))],
        compiler_params=pltpu.CompilerParams(collective_id=2, has_side_effects=True),
        name="total_gain",
    )(part.reshape(shape))
    return jnp.sum(chips, axis=0).reshape(DIM)


def rope_tables():
    inv_freq = ROPE_BASE ** (-jnp.arange(HEAD // 2, dtype=F32) * 2.0 / HEAD)
    pos = row_position(jnp.arange(SEQ, dtype=jnp.int32)).astype(F32)
    angles = pos[:, None] * inv_freq[None, :]
    cos, sin = jnp.cos(angles), jnp.sin(angles)
    return jnp.concatenate([cos, cos], axis=1), jnp.concatenate([-sin, sin], axis=1)


def solution(mesh):
    def layer_shard(x_loc, dy_loc, ln_gain, w_query, w_key, w_value, w_out, w_gate, w_up, w_down):
        def mean(v):
            return jnp.mean(v, axis=-1, keepdims=True)

        residual = x_loc.astype(F32)
        centered = residual - mean(residual)
        inv_std = lax.rsqrt(mean(centered * centered) + LN_EPS)
        x_hat = centered * inv_std
        h_loc = (ln_gain * x_hat).astype(BF16)
        wq = w_query.reshape(DIM, HEAD)
        wo = w_out.reshape(HEAD, DIM)
        *kept, early = gather_call(h_loc, dy_loc, w_gate, w_up, wq, w_key, w_value, w_down, wo, *rope_tables())
        late, dw1, dw3, dwq, dw2, dwo, dwk, dwv = scatter_call(*kept)
        sums = jnp.concatenate([early, late], axis=2).reshape(2, ITEMS, ROWS, DIM).astype(F32)
        y_loc = (residual + sums[0]).astype(BF16)
        grad_normed = sums[1]
        grad_gain = total_call(jnp.sum(grad_normed * x_hat, axis=(0, 1)))
        grad_hat = grad_normed * ln_gain
        grad_x = inv_std * (grad_hat - mean(grad_hat) - x_hat * mean(grad_hat * x_hat)) + dy_loc.astype(F32)
        grad_query = dwq.T.reshape(DIM, 1, HEAD)
        return y_loc, grad_x.astype(BF16), grad_gain, grad_query, dwk.T, dwv.T, dwo.reshape(1, HEAD, DIM), dw1, dw3, dw2

    act = P(None, "tp", None)
    head, columns, lead, every = P(None, "tp", None), P(None, "tp"), P("tp"), P()
    specs = (act, act, every, head, every, every, lead, columns, columns, lead)
    return jax.shard_map(layer_shard, mesh=mesh, in_specs=specs, out_specs=specs, check_vma=False)
```

```python
import jax
import jax.numpy as jnp
from jax import lax
from jax.experimental import pallas as pl
from jax.experimental.pallas import tpu as pltpu
from jax.sharding import PartitionSpec as P

LN_EPS = 1e-6
ROPE_BASE = 10000.0
MESH = pl.DeviceIdType.MESH
F32 = jnp.float32
BF16 = jnp.bfloat16
ALL = slice(None)
PAIR = range(2)
LANES = 128
W = 256
VMEM_BYTES = 67043328

GROUP = 8
ITEMS = 2 * GROUP
ROWS = 8
BLOCK = 2 * ROWS
LINE = 4 * BLOCK
SEQ = 4 * LINE
TALL = (2, 2, LINE)
DIM = 4096
HEAD = 128
FFN = 512
OUT = FFN + HEAD
OWN = 2 * FFN + HEAD
KEY = 2 * OWN
VAL = KEY + HEAD
NCAT = VAL + HEAD
NZO = 2 * OUT
QCOL = (2 * FFN, OWN + 2 * FFN)
OCOL = (2 * FFN, 2 * FFN + HEAD)
NEAR = GROUP * SEQ

SLOW = 3
DEPTH = 5
COPIES = 14


class Columns:
    def __init__(self, a):
        self.a, self.c = a, DIM // 2 - a
        self.left = (slice(0, a), slice(a, 2 * a))
        self.both_left = slice(0, 2 * a)
        self.right = (slice(2 * a, 2 * a + self.c), slice(2 * a + self.c, DIM))
        self.both_right = slice(2 * a, DIM)
        self.halves = (slice(0, self.c), slice(self.c, 2 * self.c))


GCOL = SCOL = Columns(1280)


def place():
    i = lax.axis_index("tp")
    return lax.div(i, 8), lax.rem(lax.div(i, 4), 2), lax.rem(lax.div(i, 2), 2), lax.rem(i, 2)


def index(z, y, x, core):
    return ((z * 2 + y) * 2 + x) * 2 + core


def rows8(start, size):
    return pl.ds(pl.multiple_of(start, ROWS), size)


def rows16(start, size):
    return pl.ds(pl.multiple_of(start, BLOCK), size)


def lanes(start, size):
    return pl.ds(pl.multiple_of(start, LANES), size)


def step_of(t, size):
    return lanes(t * size, size)


def loop(count, body):
    lo, hi = count if isinstance(count, tuple) else (0, count)

    def run(i, carry):
        body(i)
        return carry

    lax.fori_loop(lo, hi, run, 0)


def remote(src, dst, sems, target):
    return pltpu.make_async_remote_copy(src, dst, *sems, device_id=(target,), device_id_type=MESH)


def start(copies):
    for c in copies:
        c.start()


def wait(copies):
    for c in copies:
        c.wait()


def wait_recv(copies):
    for c in copies:
        c.wait_recv()


def wait_send(copies):
    for c in copies:
        c.wait_send()


def partners_of(z, y, x, core):
    chips = [index(lax.rem(z + k, 4), y, x, core) for k in (1, 2, 3)]
    return [index(z, y, x, 1 - core), index(z, y, 1 - x, core), index(z, 1 - y, x, core)] + chips


def entry_barrier(partners):
    barrier = pltpu.get_barrier_semaphore()
    for partner in partners:
        pl.semaphore_signal(barrier, inc=1, device_id=(partner,), device_id_type=MESH)
    pl.semaphore_wait(barrier, len(partners))


def dot_nt(a, b):
    return lax.dot_general(a, b, (((1,), (1,)), ((), ())), preferred_element_type=F32)


def dot_tn(a, b):
    return lax.dot_general(a, b, (((0,), (0,)), ((), ())), preferred_element_type=F32)


def dot_nn(a, b):
    return jnp.dot(a, b, preferred_element_type=F32)


def add_into(dst, src, width):
    def tile(t):
        cols = step_of(t, W)
        dst[..., cols] = (dst[..., cols].astype(F32) + src[..., cols].astype(F32)).astype(BF16)

    loop(width // W, tile)


def row_position(r):
    return ((r // BLOCK) % 4) * LINE + (r // (2 * LINE)) * (2 * BLOCK) + ((r // LINE) % 2) * BLOCK + r % BLOCK


class Line:
    def __init__(self, z, y, x, core):
        low = lax.div(z, 2)
        odd = lax.rem(z, 2)
        self.mid = low != odd
        self.end = low == odd
        side = index(z + 1 - 2 * odd, y, x, core)
        across = index(3 - z, y, x, core)
        self.three = rows16(BLOCK - BLOCK * low, 3 * BLOCK)
        self.half = rows16(2 * BLOCK * low, 2 * BLOCK)
        self.other = rows16(2 * BLOCK - 2 * BLOCK * low, 2 * BLOCK)
        self.tip = rows16(3 * BLOCK * low, BLOCK)
        self.own = rows16(BLOCK * z, BLOCK)
        self.spread = ((self.own, side), (self.half, across), (self.three, side))
        self.merge = ((self.three, side), (self.other, across), (self.tip, side))


class Transfer:
    def __init__(self, spot, send, recv):
        self.z, self.y, self.x, self.core = spot
        self.line = Line(*spot)
        self.sib, self.xn, self.yn, *self.zn = partners_of(*spot)
        self.send, self.recv, self.keys = send, recv, {}

    def sems(self, slot, key):
        k = self.keys.setdefault(key, len(self.keys))
        return self.send.at[slot, k], self.recv.at[slot, k]

    def on_end(self, body):
        pl.when(self.line.end)(body)

    def on_mid(self, body):
        pl.when(self.line.mid)(body)

    def tick(self, m):
        for k, stage in reversed(list(enumerate(self.stages))):
            n = m - k
            pl.when((n >= 0) & (n < ITEMS))(lambda stage=stage, n=n: stage(n))


class Gather(Transfer):
    def __init__(self, spot, buf, send, recv):
        super().__init__(spot, send, recv)
        self.buf = buf
        self.stages = (self.stage0, self.stage1, self.stage2, self.stage3, self.stage4, self.stage5)

    def copy(self, n, key, ys, xs, rows, cols, target):
        view = self.buf.at[lax.div(n, 2), lax.rem(n, 2), ys, xs, rows, cols]
        return remote(view, view, self.sems(n, key), target)

    def za(self, n, step):
        rows, target = self.line.spread[step]
        return self.copy(n, ("za", step), self.y, self.x, rows, GCOL.both_left, target)

    def zc(self, n, step):
        rows, target = self.line.spread[step]
        return self.copy(n, ("zc", step), ALL, ALL, rows, GCOL.both_right, target)

    def c1(self, n):
        cols, own = GCOL.right, self.line.own
        return [self.copy(n, "c1x", self.y, self.x, own, cols[0], self.xn), self.copy(n, "c1y", self.y, self.x, own, cols[1], self.yn)]

    def c2(self, n):
        cols, own = GCOL.right, self.line.own
        return [self.copy(n, "c2y", self.y, ALL, own, cols[0], self.yn), self.copy(n, "c2x", ALL, self.x, own, cols[1], self.xn)]

    def a1(self, n):
        cols = GCOL.left
        return [self.copy(n, "a1y", self.y, self.x, ALL, cols[0], self.yn), self.copy(n, "a1x", self.y, self.x, ALL, cols[1], self.xn)]

    def a2(self, n):
        cols = GCOL.left
        return [self.copy(n, "a2x", ALL, self.x, ALL, cols[0], self.xn), self.copy(n, "a2y", self.y, ALL, ALL, cols[1], self.yn)]

    def pass_on(self, chain, n, step):
        def body():
            chain(n, step - 1).wait_recv()
            chain(n, step).start()

        self.on_mid(body)

    def stage0(self, n):
        self.on_end(lambda: self.za(n, 0).start())
        start(self.c1(n))

    def stage1(self, n):
        self.pass_on(self.za, n, 1)
        wait_recv(self.c1(n))
        start(self.c2(n))

    def stage2(self, n):
        self.pass_on(self.za, n, 2)
        wait_recv(self.c2(n))
        self.on_end(lambda: self.zc(n, 0).start())

    def stage3(self, n):
        self.on_end(lambda: self.za(n, 2).wait_recv())
        start(self.a1(n))
        self.pass_on(self.zc, n, 1)

    def stage4(self, n):
        wait_recv(self.a1(n))
        start(self.a2(n))
        self.pass_on(self.zc, n, 2)

    def stage5(self, n):
        wait_recv(self.a2(n))
        self.on_end(lambda: self.zc(n, 2).wait_recv())

    def finish(self, n):
        wait_send(self.c1(n) + self.c2(n) + self.a1(n) + self.a2(n))
        self.on_end(lambda: wait_send([self.za(n, 0), self.zc(n, 0)]))
        self.on_mid(lambda: wait_send([chain(n, step) for chain in (self.za, self.zc) for step in (1, 2)]))


def scatter_shapes():
    a, c = SCOL.a, SCOL.c
    return dict(
        b1=(3, 2, 2, LINE, a), b2=(5, 2, LINE, a), za0=(3, 2, 3 * BLOCK, a), za1=(3, 2, 2 * BLOCK, a), za2=(4, 2, BLOCK, a),
        own_a=(2, 2, 2, LINE, a), own_c=(4, *TALL, 2 * c), zc0=(3, 2, 2, 3 * BLOCK, 2 * c), zc1=(3, 2, 2, 2 * BLOCK, 2 * c),
        zc2=(4, 2, 2, BLOCK, 2 * c), h1=(3, 2, 2, BLOCK, c), h2=(3, 2, BLOCK, c), fin=(3, 2, ROWS, DIM),
    )


SLOTS = 6


def scatter_scratch():
    dma = pltpu.SemaphoreType.DMA
    buffers = [pltpu.VMEM(s, BF16) for s in scatter_shapes().values()]
    return buffers + [dma((SLOTS, COPIES)), dma((SLOTS, COPIES)), dma((SLOTS, 3)), dma((ITEMS,)), dma((ITEMS,))]


class Scatter(Transfer):
    def __init__(self, spot, parts, sums, refs):
        shapes = scatter_shapes()
        self.depth = {name: s[0] for name, s in shapes.items()}
        self.ring = dict(zip(shapes, refs))
        send, recv, self.lsem, *self.store_sems = refs[len(shapes) :]
        super().__init__(spot, send, recv)
        self.parts, self.sums = parts, sums
        self.stages = (self.stage0, self.stage1, self.stage2, self.stage3, self.stage4, self.stage5)

    def slot(self, name, n, *at):
        return self.ring[name].at[(lax.rem(n, self.depth[name]), *at)]

    def copy(self, n, key, src, dst, target):
        return remote(src, dst, self.sems(lax.rem(n, SLOTS), key), target)

    def a1(self, n):
        cols = SCOL.left
        return [
            self.copy(n, "a1x", self.parts.at[n, :, 1 - self.x, :, cols[0]], self.slot("b1", n, 0), self.xn),
            self.copy(n, "a1y", self.parts.at[n, 1 - self.y, :, :, cols[1]], self.slot("b1", n, 1), self.yn),
        ]

    def a2(self, n):
        return [
            self.copy(n, "a2y", self.slot("b1", n, 0, 1 - self.y), self.slot("b2", n, 0), self.yn),
            self.copy(n, "a2x", self.slot("b1", n, 1, 1 - self.x), self.slot("b2", n, 1), self.xn),
        ]

    def za(self, n, step):
        rows, target = self.line.merge[step]
        key = f"za{step}"
        return self.copy(n, key, self.slot("b2", n, ALL, rows, ALL), self.slot(key, n), target)

    def zc(self, n, step):
        rows, target = self.line.merge[step]
        key = f"zc{step}"
        src = self.slot("own_c", n, ALL, ALL, rows, ALL) if step else self.parts.at[n, :, :, rows, SCOL.both_right]
        return self.copy(n, key, src, self.slot(key, n), target)

    def h1(self, n):
        cols = SCOL.halves
        return [
            self.copy(n, "h1y", self.slot("zc2", n, 1 - self.y, ALL, ALL, cols[0]), self.slot("h1", n, 0), self.yn),
            self.copy(n, "h1x", self.slot("zc2", n, ALL, 1 - self.x, ALL, cols[1]), self.slot("h1", n, 1), self.xn),
        ]

    def h2(self, n):
        cols = SCOL.halves
        return [
            self.copy(n, "h2x", self.slot("zc2", n, self.y, 1 - self.x, ALL, cols[0]), self.slot("h2", n, 0), self.xn),
            self.copy(n, "h2y", self.slot("zc2", n, 1 - self.y, self.x, ALL, cols[1]), self.slot("h2", n, 1), self.yn),
        ]

    def loads(self, n):
        sem = self.lsem.at[lax.rem(n, SLOTS)]
        views = (
            (self.parts.at[n, :, self.x, :, SCOL.left[0]], self.slot("own_a", n, 0)),
            (self.parts.at[n, self.y, :, :, SCOL.left[1]], self.slot("own_a", n, 1)),
            (self.parts.at[n, :, :, :, SCOL.both_right], self.slot("own_c", n)),
        )
        return [pltpu.make_async_copy(src, dst, sem.at[k]) for k, (src, dst) in enumerate(views)]

    def kept(self, n):
        return self.sums.at[lax.rem(n, 2), self.core, lax.div(n, 2)]

    def store(self, n):
        send, recv = self.store_sems
        return remote(self.slot("fin", n, 1 - self.core), self.kept(n), (send.at[n], recv.at[n]), self.sib)

    def stage0(self, n):
        start(self.a1(n))
        self.on_end(lambda: self.zc(n, 0).start())
        start(self.loads(n))

    def stage1(self, n):
        wait(self.loads(n))
        wait_recv(self.a1(n))
        for c in PAIR:
            add_into(self.slot("b1", n, c), self.slot("own_a", n, c), SCOL.a)
        start(self.a2(n))

        def middle():
            self.zc(n, 0).wait_recv()
            add_into(self.slot("own_c", n, ALL, ALL, self.line.three), self.slot("zc0", n), 2 * SCOL.c)
            self.zc(n, 1).start()

        self.on_mid(middle)
        wait_send(self.a1(n))
        self.on_end(lambda: self.zc(n, 0).wait_send())

    def stage2(self, n):
        wait_recv(self.a2(n))
        for c, mine in enumerate((self.y, self.x)):
            add_into(self.slot("b2", n, c), self.slot("b1", n, c, mine), SCOL.a)
        self.on_end(lambda: self.za(n, 0).start())

        def middle():
            self.zc(n, 1).wait_recv()
            add_into(self.slot("own_c", n, ALL, ALL, self.line.half), self.slot("zc1", n), 2 * SCOL.c)
            self.zc(n, 2).start()
            self.zc(n, 1).wait_send()

        self.on_mid(middle)
        wait_send(self.a2(n))

    def stage3(self, n):
        own_c = self.slot("own_c", n, ALL, ALL, self.line.own)

        def middle():
            self.za(n, 0).wait_recv()
            add_into(self.slot("b2", n, ALL, self.line.three), self.slot("za0", n), SCOL.a)
            self.za(n, 1).start()
            self.slot("zc2", n)[...] = own_c[...]

        def tip():
            self.zc(n, 2).wait_recv()
            add_into(self.slot("zc2", n), own_c, 2 * SCOL.c)

        self.on_mid(middle)
        self.on_end(tip)
        start(self.h1(n))
        self.on_mid(lambda: self.zc(n, 2).wait_send())
        self.on_end(lambda: self.za(n, 0).wait_send())

    def stage4(self, n):
        def middle():
            self.za(n, 1).wait_recv()
            add_into(self.slot("b2", n, ALL, self.line.half), self.slot("za1", n), SCOL.a)
            self.za(n, 2).start()
            self.za(n, 1).wait_send()

        self.on_mid(middle)
        wait_recv(self.h1(n))
        cols = SCOL.halves
        add_into(self.slot("zc2", n, self.y, ALL, ALL, cols[0]), self.slot("h1", n, 0), SCOL.c)
        add_into(self.slot("zc2", n, ALL, self.x, ALL, cols[1]), self.slot("h1", n, 1), SCOL.c)
        start(self.h2(n))
        wait_send(self.h1(n))

    def stage5(self, n):
        pl.when(n >= self.depth["fin"])(lambda: self.store(n - self.depth["fin"]).wait_send())

        def tip():
            self.za(n, 2).wait_recv()
            add_into(self.slot("b2", n, ALL, self.line.own), self.slot("za2", n), SCOL.a)

        self.on_end(tip)
        self.on_mid(lambda: self.za(n, 2).wait_send())
        wait_recv(self.h2(n))
        fin = self.slot("fin", n)

        def put(total, col):
            for core in PAIR:
                fin[core, :, lanes(col, W)] = total[core * ROWS : (core + 1) * ROWS].astype(BF16)

        def left(t):
            for c in PAIR:
                put(self.slot("b2", n, c, self.line.own)[:, step_of(t, W)].astype(F32), c * SCOL.a + t * W)

        def right(t):
            for c in PAIR:
                mine = self.slot("zc2", n, self.y, self.x)[:, lanes(c * SCOL.c + t * W, W)].astype(F32)
                put(mine + self.slot("h2", n, c)[:, step_of(t, W)].astype(F32), 2 * SCOL.a + c * SCOL.c + t * W)

        loop(SCOL.a // W, left)
        loop(SCOL.c // W, right)
        self.store(n).start()
        self.kept(n)[...] = fin[self.core]
        wait_send(self.h2(n))

    def finish(self):
        loop((ITEMS - self.depth["fin"], ITEMS), lambda n: self.store(n).wait_send())
        loop(ITEMS, lambda n: self.store(n).wait_recv())


TILE = 512
STEPS = DIM // TILE
KV = 2 * HEAD
KCOL = OWN + OUT
NBIG = KCOL + KV
QUARTER = DIM // 4
EIGHTH = DIM // 8
KROWS = KV // 4


def layer_kernel(
    h_loc, dy_tok, x_loc, dy_loc, w1, w3, wq, wk, wv, w2, wo, gain, cos_t, sin_t,
    full, full_sib, parts, g_all, zo_all, g_sib, zo_sib, y_out, dx_out, dgain, dw1, dw3, dwq, dw2, dwo, dwk, dwv,
    gsend, grecv, sx, rx, sw, rw, ss, rs, sg, rg, ksend, krecv, lsem, wsem, osem, gsem,
    tsem, o1sem, o2sem, hsend, hrecv, ready, sums, *scatter_refs,
):
    spot = place()
    z, y, x, core = spot
    partners = partners_of(*spot)
    sib, xn, yn, *zn = partners
    entry_barrier(partners)
    gather = Gather(spot, full, gsend, grecv)
    scatter = Scatter(spot, parts, sums, scatter_refs)

    def meet(others):
        for there in others:
            pl.semaphore_signal(ready, inc=1, device_id=(there,), device_id_type=MESH)
        pl.semaphore_wait(ready, len(others))

    def activations(wcat, w2o, hv, dyv, proj, zo, g, yo, dho, probs, qs, stage):
        mine = rows8(BLOCK * z + ROWS * core, ROWS)
        locs = (h_loc, dy_tok)
        to = [full.at[:, s, y, x, mine, :] for s in PAIR]
        swaps = [remote(locs[s].at[rows8(GROUP * (1 - core), GROUP)], to[s], (sx.at[s], rx.at[s]), sib) for s in PAIR]
        takes = [pltpu.make_async_copy(locs[s].at[rows8(GROUP * core, GROUP)], stage.at[s], lsem.at[s]) for s in PAIR]
        puts = [pltpu.make_async_copy(stage.at[s], to[s], lsem.at[s]) for s in PAIR]
        start(swaps + takes)
        for s in PAIR:
            takes[s].wait()
            puts[s].start()
        wait(puts)
        wait_recv(swaps)
        loop(2, gather.tick)

        spots = (
            (w1, wcat.at[:, 0:FFN], wcat.at[:, OWN : OWN + FFN]),
            (w3, wcat.at[:, FFN : 2 * FFN], wcat.at[:, OWN + FFN : OWN + 2 * FFN]),
            (wq, wcat.at[:, 2 * FFN : OWN], wcat.at[:, OWN + 2 * FFN : KEY]),
            (w2, w2o.at[0:FFN], w2o.at[FFN : 2 * FFN]),
            (wo, w2o.at[OCOL[0] : OCOL[1]], w2o.at[OCOL[1] : NZO]),
        )
        shared = ((wk, wcat.at[:, KEY:VAL]), (wv, wcat.at[:, VAL:NCAT]))
        weights = [(w, near) for w, near, _ in spots] + list(shared)
        local = [pltpu.make_async_copy(w, near, wsem.at[k]) for k, (w, near) in enumerate(weights)]
        far = [remote(w, there, (sw.at[k], rw.at[k]), sib) for k, (w, _, there) in enumerate(spots)]
        start(local)
        meet([sib])
        start(far)
        loop((2, DEPTH + 1), gather.tick)

        def load(b, s):
            return pltpu.make_async_copy(full.at[b, s], (hv, dyv)[s], lsem.at[s])

        def sib_copy(b, s):
            return remote(full.at[b, s], full_sib.at[b, s], (ss.at[b, s], rs.at[b, s]), sib)

        def arrived(b, s):
            load(b, s).start()
            sib_copy(b, s).start()

        arrived(0, 0)
        wait(local)
        wait_recv(far)

        def gz_copies(b):
            rows = rows16(b * SEQ, SEQ)
            views = (
                (g.at[:, OWN:KEY], g_sib.at[rows]),
                (zo.at[:, FFN : 2 * FFN], zo_sib.at[rows, 0:FFN]),
                (zo.at[:, OCOL[1] : NZO], zo_sib.at[rows, FFN:OUT]),
            )
            return [remote(src, dst, (sg.at[b, k], rg.at[b, k]), sib) for k, (src, dst) in enumerate(views)]

        def gz_local(b):
            rows = rows16(b * SEQ, SEQ)
            return [pltpu.make_async_copy(g, g_all.at[rows], gsem.at[0]), pltpu.make_async_copy(zo, zo_all.at[rows], gsem.at[1])]

        def out(b, s):
            return pltpu.make_async_copy((yo, dho)[s], parts.at[2 * b + s], osem.at[s])

        def drained(b):
            wait([*gz_local(b), out(b, 1)])
            wait_send(gz_copies(b))

        scale = HEAD ** -0.5

        def rotate(v, back=False):
            turn = pltpu.roll(v, HEAD // 2, 1) * sin_t[...]
            return v * cos_t[...] + (-turn if back else turn)

        def flat(ref):
            return ref[...].reshape(SEQ, DIM)

        def gate_up(t):
            at = t * W + lax.div(t, 2) * (OWN - FFN)
            return lanes(at, W), lanes(at + FFN, W)

        wide = lambda t: step_of(t, FFN)

        def batch_step(b):
            ahead = 2 * b + DEPTH + 1
            behind = b - 1 + lax.max(b - SLOW, 0)
            pl.when(b > 0)(lambda: out(b - 1, 0).wait())
            scatter.tick(behind)
            load(b, 0).wait()

            def proj_tile(t):
                proj[:, wide(t)] = dot_nn(flat(hv), wcat[:, wide(t)])

            loop(NCAT // FFN, proj_tile)
            pl.when(b > 0)(lambda: drained(b - 1))

            def hidden_tile(t):
                gate_at, up_at = gate_up(t)
                gate = proj[:, gate_at]
                zo[:, step_of(t, W)] = (gate * jax.nn.sigmoid(gate) * proj[:, up_at]).astype(BF16)

            loop(2 * FFN // W, hidden_tile)
            keys = rotate(proj[:, KEY:VAL]).astype(BF16)
            vals = proj[:, VAL:NCAT].astype(BF16)
            qs[2] = keys
            qs[3] = vals
            causal = row_position(lax.broadcasted_iota(jnp.int32, (SEQ, SEQ), 0)) >= row_position(lax.broadcasted_iota(jnp.int32, (SEQ, SEQ), 1))
            for hd in PAIR:
                query = rotate(proj[:, QCOL[hd] : QCOL[hd] + HEAD]).astype(BF16)
                qs[hd] = query
                scores = jnp.where(causal, dot_nt(query, keys) * scale, -1e30)
                e = jnp.exp(scores - jnp.max(scores, axis=-1, keepdims=True))
                p = e / jnp.sum(e, axis=-1, keepdims=True)
                probs[hd] = p
                zo[:, OCOL[hd] : OCOL[hd] + HEAD] = dot_nn(p.astype(BF16), vals).astype(BF16)

            gather.tick(ahead)
            arrived(b, 1)

            def y_tile(t):
                yo[:, :, :, wide(t)] = dot_nn(zo[...], w2o[:, wide(t)]).astype(BF16).reshape(*TALL, FFN)

            loop(DIM // FFN, y_tile)
            out(b, 0).start()
            load(b, 1).wait()

            def dz_tile(t):
                dz = dot_nt(flat(dyv), w2o[rows16(t * W, W), :])
                gate_at, up_at = gate_up(t)
                gate = proj[:, gate_at]
                sig = jax.nn.sigmoid(gate)
                g[:, gate_at] = (dz * proj[:, up_at] * sig * (1.0 + gate * (1.0 - sig))).astype(BF16)
                g[:, up_at] = (dz * (gate * sig)).astype(BF16)

            loop(2 * FFN // W, dz_tile)
            pl.when(b >= SLOW)(lambda: scatter.tick(behind + 1))
            d_heads = dot_nt(flat(dyv), w2o[2 * FFN : NZO, :]).astype(BF16)
            d_keys = d_vals = jnp.zeros((SEQ, HEAD), F32)
            for hd in PAIR:
                d_out = d_heads[:, hd * HEAD : (hd + 1) * HEAD]
                p = probs[hd]
                d_probs = dot_nt(d_out, qs[3])
                d_vals = d_vals + dot_tn(p.astype(BF16), d_out)
                row_dot = jnp.sum(p * d_probs, axis=-1, keepdims=True)
                d_scores = (p * (d_probs - row_dot) * scale).astype(BF16)
                g[:, QCOL[hd] : QCOL[hd] + HEAD] = rotate(dot_nn(d_scores, qs[2]), True).astype(BF16)
                d_keys = d_keys + dot_tn(d_scores, qs[hd])
            g[:, KEY:VAL] = rotate(d_keys, True).astype(BF16)
            g[:, VAL:NCAT] = d_vals.astype(BF16)
            gather.tick(ahead + 1)
            pl.when(b < GROUP - 1)(lambda: arrived(b + 1, 0))

            def dh_tile(t):
                dho[:, :, :, wide(t)] = dot_nt(g[...], wcat[rows16(t * FFN, FFN), :]).astype(BF16).reshape(*TALL, FFN)

            loop(DIM // FFN, dh_tile)
            out(b, 1).start()
            start(gz_local(b) + gz_copies(b))

        loop(GROUP, batch_step)
        out(GROUP - 1, 0).wait()
        drained(GROUP - 1)

        def finish(b):
            for s in PAIR:
                gather.finish(2 * b + s)
                sib_copy(b, s).wait()
            wait_recv(gz_copies(b))

        loop(GROUP, finish)
        wait_send(swaps + far)


    def gradients(big, tiles, out1, outq, out2, kvo, kvt, kvp, k1, k2, k3, kc, k4, gacc, gpart, ggot, gz):
        near, away = slice(0, NEAR), slice(NEAR, 2 * NEAR)
        views = (
            (g_all.at[:, KEY:NCAT], big.at[near, KCOL:NBIG]),
            (g_all.at[:, 0:OWN], big.at[near, 0:OWN]),
            (g_sib, big.at[away, 0:OWN]),
            (zo_all.at[:, 0:FFN], big.at[near, OWN : OWN + FFN]),
            (zo_all.at[:, OCOL[0] : OCOL[1]], big.at[near, OWN + FFN : KCOL]),
            (zo_sib, big.at[away, OWN:KCOL]),
        )
        loads = [pltpu.make_async_copy(src, dst, lsem.at[k]) for k, (src, dst) in enumerate(views)]
        start(loads)

        def tile_load(u, s):
            slot = lax.rem(u, 2)
            sources = (full, full_sib)
            return [pltpu.make_async_copy(sources[k].at[:, s, :, :, :, step_of(u, TILE)], tiles.at[slot, k], tsem.at[slot, k]) for k in PAIR]

        tile_load(0, 0)[0].start()
        loads[0].wait()

        def kv_tile(u):
            pl.when(u < STEPS - 1)(lambda: tile_load(u + 1, 0)[0].start())
            tile_load(u, 0)[0].wait()
            kvp[:, step_of(u, TILE)] = dot_tn(big[near, KCOL:NBIG], tiles[lax.rem(u, 2), 0].reshape(NEAR, TILE))

        loop(STEPS, kv_tile)
        start(tile_load(0, 0))

        half = core * (DIM // 2)
        quarter = (half, half + QUARTER)
        ring = ((x, y, xn, yn), (y, x, yn, xn))
        first = [quarter[c] + ring[c][0] * EIGHTH for c in PAIR]
        second = [first[c] + ring[c][1] * W for c in PAIR]
        mine = rows16(z * KROWS, KROWS)
        hops = {}

        def hop(step, src, dst, target):
            group = hops.setdefault(step, [])
            group.append(remote(src, dst, (ksend.at[step, len(group)], krecv.at[step, len(group)]), target))

        hop(0, kvp.at[:, lanes(DIM // 2 - half, DIM // 2)], k1, sib)
        for c in PAIR:
            a, b, an, bn = ring[c]
            hop(1, kvp.at[:, lanes(quarter[c] + (1 - a) * EIGHTH, EIGHTH)], k2.at[c], an)
            hop(2, kvp.at[:, lanes(first[c] + (1 - b) * W, W)], k3.at[c], bn)
            same = kvo.at[:, lanes(second[c], W)]
            hop(5, same, same, bn)
            same = kvo.at[:, lanes(first[c], EIGHTH)]
            hop(6, same, same, an)
        for k, there in enumerate(zn):
            hop(3, kc.at[rows16(lax.rem(z + k + 1, 4) * KROWS, KROWS)], k4.at[k], there)
            for c in PAIR:
                same = kvo.at[mine, lanes(second[c], W)]
                hop(4, same, same, there)
        same = kvo.at[:, lanes(half, DIM // 2)]
        hop(7, same, same, sib)

        def kv_add(src, at, width):
            def tile(t):
                cols = lanes(at + t * W, W)
                kvp[:, cols] = kvp[:, cols] + src[:, step_of(t, W)]

            loop(width // W, tile)

        def kv_first():
            kv_add(k1, half, DIM // 2)

        def kv_second():
            for c in PAIR:
                kv_add(k2.at[c], first[c], EIGHTH)

        def kv_third():
            for c in PAIR:
                kc[:, c * W : (c + 1) * W] = kvp[:, lanes(second[c], W)] + k3[c]

        def kv_round():
            total = kc[mine, :] + k4[0] + k4[1] + k4[2]
            for c in PAIR:
                kvo[mine, lanes(second[c], W)] = total[:, c * W : (c + 1) * W].astype(BF16)

        def kv_turn(t):
            rows = step_of(t, TILE)
            for s in PAIR:
                kvt[s] = kvo[s * HEAD : (s + 1) * HEAD, rows].astype(F32).T.astype(BF16)
            copies = [pltpu.make_async_copy(kvt.at[s], (dwk, dwv)[s].at[rows], osem.at[s]) for s in PAIR]
            start(copies)
            wait(copies)

        works = (kv_first, kv_second, kv_third, kv_round)

        def kv_step(j):
            for step in range(len(hops)):

                @pl.when(j == step)
                def _(step=step):
                    wait_recv(hops[step])
                    if step < len(works):
                        works[step]()
                    elif step == len(hops) - 1:
                        loop(STEPS, kv_turn)
                    start(hops.get(step + 1, ()))

        meet(partners)
        start(hops[0])
        ticks = 2 * GROUP - 1 - SLOW
        scatter.tick(ticks)
        wait(loads[1:])

        def out_copies(u):
            slot = lax.rem(u, 2)
            rows = step_of(u, TILE)
            sem = o1sem.at[slot]
            return [
                pltpu.make_async_copy(out1.at[slot, :, 0:FFN], dw1.at[rows], sem.at[0]),
                pltpu.make_async_copy(out1.at[slot, :, FFN : 2 * FFN], dw3.at[rows], sem.at[1]),
                pltpu.make_async_copy(outq.at[slot], dwq.at[rows], sem.at[2]),
            ]

        def out2_copies(u):
            slot, cols = lax.rem(u, 2), step_of(u, TILE)
            sem = o2sem.at[slot]
            return [
                pltpu.make_async_copy(out2.at[slot, 0:FFN], dw2.at[:, cols], sem.at[0]),
                pltpu.make_async_copy(out2.at[slot, FFN:OUT], dwo.at[:, cols], sem.at[1]),
            ]

        def mean(v):
            return jnp.mean(v, axis=-1, keepdims=True)

        def token_step(i):
            first = i * 2
            spans = [rows16(k * ITEMS * ROWS + i * BLOCK, BLOCK) for k in range(4)]

            def total(s):
                return sums[s, lax.div(first, GROUP), pl.ds(lax.rem(first, GROUP), 2)].astype(F32).reshape(BLOCK, DIM)

            def both(k):
                return jnp.concatenate([big[spans[k], :], big[spans[k + 1], :]], axis=1).astype(F32)

            def keep(k, value):
                big[spans[k], :] = value[:, 0:NBIG].astype(BF16)
                big[spans[k + 1], :] = value[:, NBIG:DIM].astype(BF16)

            res = both(0)
            d_norm = total(1)
            centered = res - mean(res)
            inv_std = lax.rsqrt(mean(centered * centered) + LN_EPS)
            x_hat = centered * inv_std
            gacc[...] = gacc[...] + d_norm * x_hat
            d_hat = d_norm * gain[...]
            dx = inv_std * (d_hat - mean(d_hat) - x_hat * mean(d_hat * x_hat)) + both(2)
            keep(0, res + total(0))
            keep(2, dx)

        def tokens_of(arrays, inward):
            copies = []
            for k in range(4):
                here = big.at[k * ITEMS * ROWS : (k + 1) * ITEMS * ROWS]
                there = arrays[k // 2].at[:, k % 2 * NBIG : (k % 2 + 1) * NBIG]
                src, dst = (there, here) if inward else (here, there)
                copies.append(pltpu.make_async_copy(src, dst, lsem.at[k]))
            return copies

        tokens_in, results = tokens_of((x_loc, dy_loc), True), tokens_of((y_out, dx_out), False)
        gain_out = pltpu.make_async_copy(gpart.at[0], dgain, osem.at[0])

        def finalize():
            start(tokens_in)
            gacc[...] = jnp.zeros_like(gacc)
            wait(tokens_in)
            loop(GROUP, token_step)
            start(results)
            gpart[0] = jnp.sum(gacc[...], axis=0, keepdims=True)
            near = partners[:3]
            for k, there in enumerate(near):
                step = remote(gpart.at[k], ggot.at[k], (hsend.at[k], hrecv.at[k]), there)
                step.start()
                step.wait_recv()
                gpart[k + 1] = gpart[k] + ggot[k]
                step.wait_send()
            steps = [remote(gpart.at[3], gz.at[z], (hsend.at[3 + k], hrecv.at[3 + k]), there) for k, there in enumerate(zn)]
            start(steps)
            gz[z] = gpart[3]
            wait(steps)
            gpart[0] = gz[0] + gz[1] + gz[2] + gz[3]
            gain_out.start()
            gain_out.wait()

        def tokens(u):
            return tiles[lax.rem(u, 2)].reshape(2 * NEAR, TILE)

        def grad_in(u):
            wait(tile_load(u, 0))
            pl.when(u < STEPS - 1)(lambda: start(tile_load(u + 1, 0)))
            pl.when(u == STEPS - 1)(lambda: start(tile_load(0, 1)))
            pl.when(u > 1)(lambda: wait(out_copies(u - 2)))
            slot = lax.rem(u, 2)
            for s in PAIR:
                out1[slot, :, s * FFN : (s + 1) * FFN] = dot_tn(tokens(u), big[:, s * FFN : (s + 1) * FFN]).astype(BF16)
            outq[slot] = dot_tn(big[:, 2 * FFN : OWN], tokens(u)).T.astype(BF16)
            start(out_copies(u))

        def grad_out(u):
            wait(tile_load(u, 1))
            pl.when(u < STEPS - 1)(lambda: start(tile_load(u + 1, 1)))
            pl.when(u > 1)(lambda: wait(out2_copies(u - 2)))
            slot = lax.rem(u, 2)
            out2[slot, 0:FFN] = dot_tn(big[:, OWN : OWN + FFN], tokens(u)).astype(BF16)
            out2[slot, FFN:OUT] = dot_tn(big[:, OWN + FFN : KCOL], tokens(u)).astype(BF16)
            start(out2_copies(u))

        def pairs(first, grad):
            def body(j):
                scatter.tick(ticks + 1 + first + j)
                grad(2 * j)
                kv_step(first + j)
                grad(2 * j + 1)

            loop(STEPS // 2, body)

        pairs(0, grad_in)
        pairs(STEPS // 2, grad_out)
        scatter.finish()
        finalize()
        for u in (STEPS - 2, STEPS - 1):
            wait(out_copies(u) + out2_copies(u))
        wait(results)
        for group in hops.values():
            wait_send(group)


    tall = (*TALL, DIM)
    half = DIM // 2
    wide = [(DIM, NCAT), (NZO, DIM), tall, tall, (SEQ, NCAT), (SEQ, NZO), (SEQ, NCAT), tall, tall, (2, SEQ, SEQ), (4, SEQ, HEAD), (2, GROUP, ROWS, DIM)]
    types = [BF16] * 4 + [F32] + [BF16] * 4 + [F32] + [BF16] * 2
    pl.run_scoped(activations, *[pltpu.VMEM(s, t) for s, t in zip(wide, types)])
    narrow = [(2 * NEAR, NBIG), (2, 2, GROUP, *TALL, TILE), (2, TILE, 2 * FFN), (2, TILE, HEAD), (2, OUT, TILE), (KV, DIM), (2, TILE, HEAD)]
    totals = [(KV, DIM), (KV, half), (2, KV, EIGHTH), (2, KV, W), (KV, 2 * W), (3, KROWS, 2 * W), (BLOCK, DIM), (4, 1, DIM), (3, 1, DIM), (4, 1, DIM)]
    buffers = [pltpu.VMEM(s, BF16) for s in narrow] + [pltpu.VMEM(s, F32) for s in totals]
    pl.run_scoped(gradients, *buffers)


def layer_call(*args):
    any_spec = pl.BlockSpec(memory_space=pl.ANY)
    vmem_spec = pl.BlockSpec(memory_space=pltpu.VMEM)
    dma = pltpu.SemaphoreType.DMA
    tall = (*TALL, DIM)
    kept = [(GROUP, 2, *tall)] * 2 + [(ITEMS, *tall), (NEAR, NCAT), (NEAR, NZO), (NEAR, OWN), (NEAR, OUT)]
    shapes = kept + [(ITEMS * ROWS, DIM)] * 2 + [(1, DIM), (DIM, FFN), (DIM, FFN), (DIM, HEAD), (FFN, DIM), (HEAD, DIM), (DIM, HEAD), (DIM, HEAD)]
    types = [BF16] * len(shapes)
    types[len(kept) + 2] = F32
    pairs = [(ITEMS, COPIES), (2,), (5,), (GROUP, 2), (GROUP, 3), (8, 6)]
    results = pl.pallas_call(
        layer_kernel,
        out_shape=[jax.ShapeDtypeStruct(s, t) for s, t in zip(shapes, types)],
        in_specs=[any_spec] * (len(args) - 3) + [vmem_spec] * 3,
        out_specs=[any_spec] * len(shapes),
        scratch_shapes=[
            *[dma(s) for s in pairs for _ in PAIR],
            *[dma(s) for s in ((6,), (7,), (2,), (2,), (2, 2), (2, 3), (2, 2), (6,), (6,))],
            pltpu.SemaphoreType.REGULAR,
            pltpu.VMEM((2, 2, GROUP, ROWS, DIM), BF16),
            *scatter_scratch(),
        ],
        compiler_params=pltpu.CompilerParams(collective_id=0, has_side_effects=True, vmem_limit_bytes=VMEM_BYTES),
        name="layer",
    )(*args)
    return results[len(kept) :]


def rope_tables():
    inv_freq = ROPE_BASE ** (-jnp.arange(HEAD // 2, dtype=F32) * 2.0 / HEAD)
    pos = row_position(jnp.arange(SEQ, dtype=jnp.int32)).astype(F32)
    angles = pos[:, None] * inv_freq[None, :]
    cos, sin = jnp.cos(angles), jnp.sin(angles)
    return jnp.concatenate([cos, cos], axis=1), jnp.concatenate([-sin, sin], axis=1)


def solution(mesh):
    def layer_shard(x_loc, dy_loc, ln_gain, w_query, w_key, w_value, w_out, w_gate, w_up, w_down):
        def mean(v):
            return jnp.mean(v, axis=-1, keepdims=True)

        residual = x_loc.astype(F32)
        centered = residual - mean(residual)
        h_loc = (ln_gain * (centered * lax.rsqrt(mean(centered * centered) + LN_EPS))).astype(BF16)
        wq = w_query.reshape(DIM, HEAD)
        wo = w_out.reshape(HEAD, DIM)
        weights = (w_gate, w_up, wq, w_key, w_value, w_down, wo)
        flat = (ITEMS * ROWS, DIM)
        y_loc, grad_x, dgain, dw1, dw3, dwq, dw2, dwo, dwk, dwv = layer_call(
            h_loc, dy_loc, x_loc.reshape(flat), dy_loc.reshape(flat), *weights, ln_gain.reshape(1, DIM), *rope_tables()
        )
        y_loc, grad_x = (v.reshape(x_loc.shape) for v in (y_loc, grad_x))
        return y_loc, grad_x, dgain.reshape(DIM), dwq.reshape(DIM, 1, HEAD), dwk, dwv, dwo.reshape(1, HEAD, DIM), dw1, dw3, dw2

    act = P(None, "tp", None)
    head, columns, lead, every = P(None, "tp", None), P(None, "tp"), P("tp"), P()
    specs = (act, act, every, head, every, every, lead, columns, columns, lead)
    return jax.shard_map(layer_shard, mesh=mesh, in_specs=specs, out_specs=specs, check_vma=False)
```

```python
import jax
import jax.numpy as jnp
from jax import lax
from jax.experimental import pallas as pl
from jax.experimental.pallas import tpu as pltpu
from jax.sharding import PartitionSpec as P

LN_EPS = 1e-6
ROPE_BASE = 10000.0
MESH = pl.DeviceIdType.MESH
F32 = jnp.float32
BF16 = jnp.bfloat16
ALL = slice(None)
PAIR = range(2)
LANES = 128
W = 256
VMEM_BYTES = 67043328

GROUP = 8
ITEMS = 2 * GROUP
ROWS = 8
BLOCK = 2 * ROWS
LINE = 4 * BLOCK
SEQ = 4 * LINE
TALL = (2, 2, LINE)
DIM = 4096
HEAD = 128
FFN = 512
OUT = FFN + HEAD
OWN = 2 * FFN + HEAD
KEY = 2 * OWN
VAL = KEY + HEAD
NCAT = VAL + HEAD
NZO = 2 * OUT
QCOL = (2 * FFN, OWN + 2 * FFN)
OCOL = (2 * FFN, 2 * FFN + HEAD)
NEAR = GROUP * SEQ

DEPTH = 5
COPIES = 14


class Columns:
    def __init__(self, a):
        self.a, self.c = a, DIM // 2 - a
        self.left = (slice(0, a), slice(a, 2 * a))
        self.both_left = slice(0, 2 * a)
        self.right = (slice(2 * a, 2 * a + self.c), slice(2 * a + self.c, DIM))
        self.both_right = slice(2 * a, DIM)
        self.halves = (slice(0, self.c), slice(self.c, 2 * self.c))


GCOL = SCOL = Columns(1280)


def place():
    i = lax.axis_index("tp")
    return lax.div(i, 8), lax.rem(lax.div(i, 4), 2), lax.rem(lax.div(i, 2), 2), lax.rem(i, 2)


def index(z, y, x, core):
    return ((z * 2 + y) * 2 + x) * 2 + core


def rows8(start, size):
    return pl.ds(pl.multiple_of(start, ROWS), size)


def rows16(start, size):
    return pl.ds(pl.multiple_of(start, BLOCK), size)


def lanes(start, size):
    return pl.ds(pl.multiple_of(start, LANES), size)


def step_of(t, size):
    return lanes(t * size, size)


def loop(count, body):
    lo, hi = count if isinstance(count, tuple) else (0, count)

    def run(i, carry):
        body(i)
        return carry

    lax.fori_loop(lo, hi, run, 0)


def remote(src, dst, sems, target):
    return pltpu.make_async_remote_copy(src, dst, *sems, device_id=(target,), device_id_type=MESH)


def start(copies):
    for c in copies:
        c.start()


def wait(copies):
    for c in copies:
        c.wait()


def wait_recv(copies):
    for c in copies:
        c.wait_recv()


def wait_send(copies):
    for c in copies:
        c.wait_send()


def partners_of(z, y, x, core):
    chips = [index(lax.rem(z + k, 4), y, x, core) for k in (1, 2, 3)]
    return [index(z, y, x, 1 - core), index(z, y, 1 - x, core), index(z, 1 - y, x, core)] + chips


def entry_barrier(partners):
    barrier = pltpu.get_barrier_semaphore()
    for partner in partners:
        pl.semaphore_signal(barrier, inc=1, device_id=(partner,), device_id_type=MESH)
    pl.semaphore_wait(barrier, len(partners))


def dot_nt(a, b):
    return lax.dot_general(a, b, (((1,), (1,)), ((), ())), preferred_element_type=F32)


def dot_tn(a, b):
    return lax.dot_general(a, b, (((0,), (0,)), ((), ())), preferred_element_type=F32)


def dot_nn(a, b):
    return jnp.dot(a, b, preferred_element_type=F32)


def add_into(dst, src, width):
    def tile(t):
        cols = step_of(t, W)
        dst[..., cols] = (dst[..., cols].astype(F32) + src[..., cols].astype(F32)).astype(BF16)

    loop(width // W, tile)


def row_position(r):
    return ((r // BLOCK) % 4) * LINE + (r // (2 * LINE)) * (2 * BLOCK) + ((r // LINE) % 2) * BLOCK + r % BLOCK


class Line:
    def __init__(self, z, y, x, core):
        low = lax.div(z, 2)
        odd = lax.rem(z, 2)
        self.mid = low != odd
        self.end = low == odd
        side = index(z + 1 - 2 * odd, y, x, core)
        across = index(3 - z, y, x, core)
        self.three = rows16(BLOCK - BLOCK * low, 3 * BLOCK)
        self.half = rows16(2 * BLOCK * low, 2 * BLOCK)
        self.other = rows16(2 * BLOCK - 2 * BLOCK * low, 2 * BLOCK)
        self.tip = rows16(3 * BLOCK * low, BLOCK)
        self.own = rows16(BLOCK * z, BLOCK)
        self.spread = ((self.own, side), (self.half, across), (self.three, side))
        self.merge = ((self.three, side), (self.other, across), (self.tip, side))


class Transfer:
    def __init__(self, spot, send, recv):
        self.z, self.y, self.x, self.core = spot
        self.line = Line(*spot)
        self.sib, self.xn, self.yn, *self.zn = partners_of(*spot)
        self.send, self.recv, self.keys = send, recv, {}

    def sems(self, slot, key):
        k = self.keys.setdefault(key, len(self.keys))
        return self.send.at[slot, k], self.recv.at[slot, k]

    def on_end(self, body):
        pl.when(self.line.end)(body)

    def on_mid(self, body):
        pl.when(self.line.mid)(body)

    def tick(self, m):
        for k, stage in reversed(list(enumerate(self.stages))):
            n = m - k
            pl.when((n >= 0) & (n < ITEMS))(lambda stage=stage, n=n: stage(n))


class Gather(Transfer):
    def __init__(self, spot, buf, send, recv):
        super().__init__(spot, send, recv)
        self.buf = buf
        self.stages = (self.stage0, self.stage1, self.stage2, self.stage3, self.stage4, self.stage5)

    def copy(self, n, key, ys, xs, rows, cols, target):
        view = self.buf.at[lax.div(n, 2), lax.rem(n, 2), ys, xs, rows, cols]
        return remote(view, view, self.sems(n, key), target)

    def za(self, n, step):
        rows, target = self.line.spread[step]
        return self.copy(n, ("za", step), self.y, self.x, rows, GCOL.both_left, target)

    def zc(self, n, step):
        rows, target = self.line.spread[step]
        return self.copy(n, ("zc", step), ALL, ALL, rows, GCOL.both_right, target)

    def c1(self, n):
        cols, own = GCOL.right, self.line.own
        return [self.copy(n, "c1x", self.y, self.x, own, cols[0], self.xn), self.copy(n, "c1y", self.y, self.x, own, cols[1], self.yn)]

    def c2(self, n):
        cols, own = GCOL.right, self.line.own
        return [self.copy(n, "c2y", self.y, ALL, own, cols[0], self.yn), self.copy(n, "c2x", ALL, self.x, own, cols[1], self.xn)]

    def a1(self, n):
        cols = GCOL.left
        return [self.copy(n, "a1y", self.y, self.x, ALL, cols[0], self.yn), self.copy(n, "a1x", self.y, self.x, ALL, cols[1], self.xn)]

    def a2(self, n):
        cols = GCOL.left
        return [self.copy(n, "a2x", ALL, self.x, ALL, cols[0], self.xn), self.copy(n, "a2y", self.y, ALL, ALL, cols[1], self.yn)]

    def pass_on(self, chain, n, step):
        def body():
            chain(n, step - 1).wait_recv()
            chain(n, step).start()

        self.on_mid(body)

    def stage0(self, n):
        self.on_end(lambda: self.za(n, 0).start())
        start(self.c1(n))

    def stage1(self, n):
        self.pass_on(self.za, n, 1)
        wait_recv(self.c1(n))
        start(self.c2(n))

    def stage2(self, n):
        self.pass_on(self.za, n, 2)
        wait_recv(self.c2(n))
        self.on_end(lambda: self.zc(n, 0).start())

    def stage3(self, n):
        self.on_end(lambda: self.za(n, 2).wait_recv())
        start(self.a1(n))
        self.pass_on(self.zc, n, 1)

    def stage4(self, n):
        wait_recv(self.a1(n))
        start(self.a2(n))
        self.pass_on(self.zc, n, 2)

    def stage5(self, n):
        wait_recv(self.a2(n))
        self.on_end(lambda: self.zc(n, 2).wait_recv())

    def finish(self, n):
        wait_send(self.c1(n) + self.c2(n) + self.a1(n) + self.a2(n))
        self.on_end(lambda: wait_send([self.za(n, 0), self.zc(n, 0)]))
        self.on_mid(lambda: wait_send([chain(n, step) for chain in (self.za, self.zc) for step in (1, 2)]))


def scatter_shapes():
    a, c = SCOL.a, SCOL.c
    return dict(
        b1=(3, 2, 2, LINE, a), b2=(5, 2, LINE, a), za0=(3, 2, 3 * BLOCK, a), za1=(3, 2, 2 * BLOCK, a), za2=(4, 2, BLOCK, a),
        own_a=(2, 2, 2, LINE, a), own_c=(4, *TALL, 2 * c), zc0=(3, 2, 2, 3 * BLOCK, 2 * c), zc1=(3, 2, 2, 2 * BLOCK, 2 * c),
        zc2=(4, 2, 2, BLOCK, 2 * c), h1=(3, 2, 2, BLOCK, c), h2=(3, 2, BLOCK, c), fin=(3, 2, ROWS, DIM),
    )


SLOTS = 6


def scatter_scratch():
    dma = pltpu.SemaphoreType.DMA
    buffers = [pltpu.VMEM(s, BF16) for s in scatter_shapes().values()]
    return buffers + [dma((SLOTS, COPIES)), dma((SLOTS, COPIES)), dma((SLOTS, 3)), dma((ITEMS,)), dma((ITEMS,))]


class Scatter(Transfer):
    def __init__(self, spot, parts, sums, refs):
        shapes = scatter_shapes()
        self.depth = {name: s[0] for name, s in shapes.items()}
        self.ring = dict(zip(shapes, refs))
        send, recv, self.lsem, *self.store_sems = refs[len(shapes) :]
        super().__init__(spot, send, recv)
        self.parts, self.sums = parts, sums
        self.stages = (self.stage0, self.stage1, self.stage2, self.stage3, self.stage4, self.stage5)

    def slot(self, name, n, *at):
        return self.ring[name].at[(lax.rem(n, self.depth[name]), *at)]

    def copy(self, n, key, src, dst, target):
        return remote(src, dst, self.sems(lax.rem(n, SLOTS), key), target)

    def a1(self, n):
        cols = SCOL.left
        return [
            self.copy(n, "a1x", self.parts.at[n, :, 1 - self.x, :, cols[0]], self.slot("b1", n, 0), self.xn),
            self.copy(n, "a1y", self.parts.at[n, 1 - self.y, :, :, cols[1]], self.slot("b1", n, 1), self.yn),
        ]

    def a2(self, n):
        return [
            self.copy(n, "a2y", self.slot("b1", n, 0, 1 - self.y), self.slot("b2", n, 0), self.yn),
            self.copy(n, "a2x", self.slot("b1", n, 1, 1 - self.x), self.slot("b2", n, 1), self.xn),
        ]

    def za(self, n, step):
        rows, target = self.line.merge[step]
        key = f"za{step}"
        return self.copy(n, key, self.slot("b2", n, ALL, rows, ALL), self.slot(key, n), target)

    def zc(self, n, step):
        rows, target = self.line.merge[step]
        key = f"zc{step}"
        src = self.slot("own_c", n, ALL, ALL, rows, ALL) if step else self.parts.at[n, :, :, rows, SCOL.both_right]
        return self.copy(n, key, src, self.slot(key, n), target)

    def h1(self, n):
        cols = SCOL.halves
        return [
            self.copy(n, "h1y", self.slot("zc2", n, 1 - self.y, ALL, ALL, cols[0]), self.slot("h1", n, 0), self.yn),
            self.copy(n, "h1x", self.slot("zc2", n, ALL, 1 - self.x, ALL, cols[1]), self.slot("h1", n, 1), self.xn),
        ]

    def h2(self, n):
        cols = SCOL.halves
        return [
            self.copy(n, "h2x", self.slot("zc2", n, self.y, 1 - self.x, ALL, cols[0]), self.slot("h2", n, 0), self.xn),
            self.copy(n, "h2y", self.slot("zc2", n, 1 - self.y, self.x, ALL, cols[1]), self.slot("h2", n, 1), self.yn),
        ]

    def loads(self, n):
        sem = self.lsem.at[lax.rem(n, SLOTS)]
        views = (
            (self.parts.at[n, :, self.x, :, SCOL.left[0]], self.slot("own_a", n, 0)),
            (self.parts.at[n, self.y, :, :, SCOL.left[1]], self.slot("own_a", n, 1)),
            (self.parts.at[n, :, :, :, SCOL.both_right], self.slot("own_c", n)),
        )
        return [pltpu.make_async_copy(src, dst, sem.at[k]) for k, (src, dst) in enumerate(views)]

    def kept(self, n):
        return self.sums.at[lax.rem(n, 2), self.core, lax.div(n, 2)]

    def store(self, n):
        send, recv = self.store_sems
        return remote(self.slot("fin", n, 1 - self.core), self.kept(n), (send.at[n], recv.at[n]), self.sib)

    def stage0(self, n):
        start(self.a1(n))
        self.on_end(lambda: self.zc(n, 0).start())
        start(self.loads(n))

    def stage1(self, n):
        wait(self.loads(n))
        wait_recv(self.a1(n))
        for c in PAIR:
            add_into(self.slot("b1", n, c), self.slot("own_a", n, c), SCOL.a)
        start(self.a2(n))

        def middle():
            self.zc(n, 0).wait_recv()
            add_into(self.slot("own_c", n, ALL, ALL, self.line.three), self.slot("zc0", n), 2 * SCOL.c)
            self.zc(n, 1).start()

        self.on_mid(middle)
        wait_send(self.a1(n))
        self.on_end(lambda: self.zc(n, 0).wait_send())

    def stage2(self, n):
        wait_recv(self.a2(n))
        for c, mine in enumerate((self.y, self.x)):
            add_into(self.slot("b2", n, c), self.slot("b1", n, c, mine), SCOL.a)
        self.on_end(lambda: self.za(n, 0).start())

        def middle():
            self.zc(n, 1).wait_recv()
            add_into(self.slot("own_c", n, ALL, ALL, self.line.half), self.slot("zc1", n), 2 * SCOL.c)
            self.zc(n, 2).start()
            self.zc(n, 1).wait_send()

        self.on_mid(middle)
        wait_send(self.a2(n))

    def stage3(self, n):
        own_c = self.slot("own_c", n, ALL, ALL, self.line.own)

        def middle():
            self.za(n, 0).wait_recv()
            add_into(self.slot("b2", n, ALL, self.line.three), self.slot("za0", n), SCOL.a)
            self.za(n, 1).start()
            self.slot("zc2", n)[...] = own_c[...]

        def tip():
            self.zc(n, 2).wait_recv()
            add_into(self.slot("zc2", n), own_c, 2 * SCOL.c)

        self.on_mid(middle)
        self.on_end(tip)
        start(self.h1(n))
        self.on_mid(lambda: self.zc(n, 2).wait_send())
        self.on_end(lambda: self.za(n, 0).wait_send())

    def stage4(self, n):
        def middle():
            self.za(n, 1).wait_recv()
            add_into(self.slot("b2", n, ALL, self.line.half), self.slot("za1", n), SCOL.a)
            self.za(n, 2).start()
            self.za(n, 1).wait_send()

        self.on_mid(middle)
        wait_recv(self.h1(n))
        cols = SCOL.halves
        add_into(self.slot("zc2", n, self.y, ALL, ALL, cols[0]), self.slot("h1", n, 0), SCOL.c)
        add_into(self.slot("zc2", n, ALL, self.x, ALL, cols[1]), self.slot("h1", n, 1), SCOL.c)
        start(self.h2(n))
        wait_send(self.h1(n))

    def stage5(self, n):
        pl.when(n >= self.depth["fin"])(lambda: self.store(n - self.depth["fin"]).wait_send())

        def tip():
            self.za(n, 2).wait_recv()
            add_into(self.slot("b2", n, ALL, self.line.own), self.slot("za2", n), SCOL.a)

        self.on_end(tip)
        self.on_mid(lambda: self.za(n, 2).wait_send())
        wait_recv(self.h2(n))
        fin = self.slot("fin", n)

        def put(total, col):
            for core in PAIR:
                fin[core, :, lanes(col, W)] = total[core * ROWS : (core + 1) * ROWS].astype(BF16)

        def left(t):
            for c in PAIR:
                put(self.slot("b2", n, c, self.line.own)[:, step_of(t, W)].astype(F32), c * SCOL.a + t * W)

        def right(t):
            for c in PAIR:
                mine = self.slot("zc2", n, self.y, self.x)[:, lanes(c * SCOL.c + t * W, W)].astype(F32)
                put(mine + self.slot("h2", n, c)[:, step_of(t, W)].astype(F32), 2 * SCOL.a + c * SCOL.c + t * W)

        loop(SCOL.a // W, left)
        loop(SCOL.c // W, right)
        self.store(n).start()
        self.kept(n)[...] = fin[self.core]
        wait_send(self.h2(n))

    def finish(self):
        loop((ITEMS - self.depth["fin"], ITEMS), lambda n: self.store(n).wait_send())
        loop(ITEMS, lambda n: self.store(n).wait_recv())


TILE = 512
STEPS = DIM // TILE
KV = 2 * HEAD
KCOL = OWN + OUT
NBIG = KCOL + KV
QUARTER = DIM // 4
EIGHTH = DIM // 8
KROWS = KV // 4


def layer_kernel(
    h_loc, dy_loc, x_loc, w1, w3, wq, wk, wv, w2, wo, cos_t, sin_t,
    full, full_sib, parts, g_all, zo_all, g_sib, zo_sib, sums_out, dgain, dw1, dw3, dwq, dw2, dwo, dwk, dwv,
    gsend, grecv, sx, rx, sw, rw, ss, rs, sg, rg, ksend, krecv, lsem, wsem, osem, gsem,
    tsem, o1sem, o2sem, hsend, hrecv, ready, sums, *scatter_refs,
):
    spot = place()
    z, y, x, core = spot
    partners = partners_of(*spot)
    sib, xn, yn, *zn = partners
    entry_barrier(partners)
    gather = Gather(spot, full, gsend, grecv)
    scatter = Scatter(spot, parts, sums, scatter_refs)

    def meet(others):
        for there in others:
            pl.semaphore_signal(ready, inc=1, device_id=(there,), device_id_type=MESH)
        pl.semaphore_wait(ready, len(others))

    def activations(wcat, w2o, hv, dyv, proj, zo, g, yo, dho, probs, qs, stage):
        mine = rows8(BLOCK * z + ROWS * core, ROWS)
        locs = (h_loc, dy_loc)
        to = [full.at[:, s, y, x, mine, :] for s in PAIR]
        swaps = [remote(locs[s].at[rows8(GROUP * (1 - core), GROUP)], to[s], (sx.at[s], rx.at[s]), sib) for s in PAIR]
        takes = [pltpu.make_async_copy(locs[s].at[rows8(GROUP * core, GROUP)], stage.at[s], lsem.at[s]) for s in PAIR]
        puts = [pltpu.make_async_copy(stage.at[s], to[s], lsem.at[s]) for s in PAIR]
        start(swaps + takes)
        for s in PAIR:
            takes[s].wait()
            puts[s].start()
        wait(puts)
        wait_recv(swaps)
        loop(2, gather.tick)

        spots = (
            (w1, wcat.at[:, 0:FFN], wcat.at[:, OWN : OWN + FFN]),
            (w3, wcat.at[:, FFN : 2 * FFN], wcat.at[:, OWN + FFN : OWN + 2 * FFN]),
            (wq, wcat.at[:, 2 * FFN : OWN], wcat.at[:, OWN + 2 * FFN : KEY]),
            (w2, w2o.at[0:FFN], w2o.at[FFN : 2 * FFN]),
            (wo, w2o.at[OCOL[0] : OCOL[1]], w2o.at[OCOL[1] : NZO]),
        )
        shared = ((wk, wcat.at[:, KEY:VAL]), (wv, wcat.at[:, VAL:NCAT]))
        weights = [(w, near) for w, near, _ in spots] + list(shared)
        local = [pltpu.make_async_copy(w, near, wsem.at[k]) for k, (w, near) in enumerate(weights)]
        far = [remote(w, there, (sw.at[k], rw.at[k]), sib) for k, (w, _, there) in enumerate(spots)]
        start(local)
        meet([sib])
        start(far)
        loop((2, DEPTH + 1), gather.tick)

        def load(b, s):
            return pltpu.make_async_copy(full.at[b, s], (hv, dyv)[s], lsem.at[s])

        def sib_copy(b, s):
            return remote(full.at[b, s], full_sib.at[b, s], (ss.at[b, s], rs.at[b, s]), sib)

        def arrived(b, s):
            load(b, s).start()
            sib_copy(b, s).start()

        arrived(0, 0)
        wait(local)
        wait_recv(far)

        def gz_copies(b):
            rows = rows16(b * SEQ, SEQ)
            views = (
                (g.at[:, OWN:KEY], g_sib.at[rows]),
                (zo.at[:, FFN : 2 * FFN], zo_sib.at[rows, 0:FFN]),
                (zo.at[:, OCOL[1] : NZO], zo_sib.at[rows, FFN:OUT]),
            )
            return [remote(src, dst, (sg.at[b, k], rg.at[b, k]), sib) for k, (src, dst) in enumerate(views)]

        def gz_local(b):
            rows = rows16(b * SEQ, SEQ)
            return [pltpu.make_async_copy(g, g_all.at[rows], gsem.at[0]), pltpu.make_async_copy(zo, zo_all.at[rows], gsem.at[1])]

        def out(b, s):
            return pltpu.make_async_copy((yo, dho)[s], parts.at[2 * b + s], osem.at[s])

        def drained(b):
            wait([*gz_local(b), out(b, 1)])
            wait_send(gz_copies(b))

        scale = HEAD ** -0.5

        def rotate(v, back=False):
            turn = pltpu.roll(v, HEAD // 2, 1) * sin_t[...]
            return v * cos_t[...] + (-turn if back else turn)

        def flat(ref):
            return ref[...].reshape(SEQ, DIM)

        def gate_up(t):
            at = t * W + lax.div(t, 2) * (OWN - FFN)
            return lanes(at, W), lanes(at + FFN, W)

        wide = lambda t: step_of(t, FFN)

        def batch_step(b):
            ahead = 2 * b + DEPTH + 1
            load(b, 0).wait()

            def proj_tile(t):
                proj[:, wide(t)] = dot_nn(flat(hv), wcat[:, wide(t)])

            loop(NCAT // FFN, proj_tile)
            pl.when(b > 0)(lambda: drained(b - 1))
            scatter.tick(2 * b - 1)

            def hidden_tile(t):
                gate_at, up_at = gate_up(t)
                gate = proj[:, gate_at]
                zo[:, step_of(t, W)] = (gate * jax.nn.sigmoid(gate) * proj[:, up_at]).astype(BF16)

            loop(2 * FFN // W, hidden_tile)
            keys = rotate(proj[:, KEY:VAL]).astype(BF16)
            vals = proj[:, VAL:NCAT].astype(BF16)
            qs[2] = keys
            qs[3] = vals
            causal = row_position(lax.broadcasted_iota(jnp.int32, (SEQ, SEQ), 0)) >= row_position(lax.broadcasted_iota(jnp.int32, (SEQ, SEQ), 1))
            for hd in PAIR:
                query = rotate(proj[:, QCOL[hd] : QCOL[hd] + HEAD]).astype(BF16)
                qs[hd] = query
                scores = jnp.where(causal, dot_nt(query, keys) * scale, -1e30)
                e = jnp.exp(scores - jnp.max(scores, axis=-1, keepdims=True))
                p = e / jnp.sum(e, axis=-1, keepdims=True)
                probs[hd] = p
                zo[:, OCOL[hd] : OCOL[hd] + HEAD] = dot_nn(p.astype(BF16), vals).astype(BF16)

            gather.tick(ahead)
            arrived(b, 1)

            def y_tile(t):
                yo[:, :, :, wide(t)] = dot_nn(zo[...], w2o[:, wide(t)]).astype(BF16).reshape(*TALL, FFN)

            loop(DIM // FFN, y_tile)
            out(b, 0).start()
            load(b, 1).wait()

            def dz_tile(t):
                dz = dot_nt(flat(dyv), w2o[rows16(t * W, W), :])
                gate_at, up_at = gate_up(t)
                gate = proj[:, gate_at]
                sig = jax.nn.sigmoid(gate)
                g[:, gate_at] = (dz * proj[:, up_at] * sig * (1.0 + gate * (1.0 - sig))).astype(BF16)
                g[:, up_at] = (dz * (gate * sig)).astype(BF16)

            loop(2 * FFN // W, dz_tile)
            out(b, 0).wait()
            scatter.tick(2 * b)
            d_heads = dot_nt(flat(dyv), w2o[2 * FFN : NZO, :]).astype(BF16)
            d_keys = d_vals = jnp.zeros((SEQ, HEAD), F32)
            for hd in PAIR:
                d_out = d_heads[:, hd * HEAD : (hd + 1) * HEAD]
                p = probs[hd]
                d_probs = dot_nt(d_out, qs[3])
                d_vals = d_vals + dot_tn(p.astype(BF16), d_out)
                row_dot = jnp.sum(p * d_probs, axis=-1, keepdims=True)
                d_scores = (p * (d_probs - row_dot) * scale).astype(BF16)
                g[:, QCOL[hd] : QCOL[hd] + HEAD] = rotate(dot_nn(d_scores, qs[2]), True).astype(BF16)
                d_keys = d_keys + dot_tn(d_scores, qs[hd])
            g[:, KEY:VAL] = rotate(d_keys, True).astype(BF16)
            g[:, VAL:NCAT] = d_vals.astype(BF16)
            gather.tick(ahead + 1)
            pl.when(b < GROUP - 1)(lambda: arrived(b + 1, 0))

            def dh_tile(t):
                dho[:, :, :, wide(t)] = dot_nt(g[...], wcat[rows16(t * FFN, FFN), :]).astype(BF16).reshape(*TALL, FFN)

            loop(DIM // FFN, dh_tile)
            out(b, 1).start()
            start(gz_local(b) + gz_copies(b))

        loop(GROUP, batch_step)
        drained(GROUP - 1)

        def finish(b):
            for s in PAIR:
                gather.finish(2 * b + s)
                sib_copy(b, s).wait()
            wait_recv(gz_copies(b))

        loop(GROUP, finish)
        wait_send(swaps + far)


    def gradients(big, tiles, out1, outq, out2, kvo, kvt, xb, kvp, k1, k2, k3, kc, k4, gacc, gpart, ggot, gz):
        x_in = pltpu.make_async_copy(x_loc, xb, gsem.at[0])
        x_in.start()
        near, away = slice(0, NEAR), slice(NEAR, 2 * NEAR)
        views = (
            (g_all.at[:, KEY:NCAT], big.at[near, KCOL:NBIG]),
            (g_all.at[:, 0:OWN], big.at[near, 0:OWN]),
            (g_sib, big.at[away, 0:OWN]),
            (zo_all.at[:, 0:FFN], big.at[near, OWN : OWN + FFN]),
            (zo_all.at[:, OCOL[0] : OCOL[1]], big.at[near, OWN + FFN : KCOL]),
            (zo_sib, big.at[away, OWN:KCOL]),
        )
        loads = [pltpu.make_async_copy(src, dst, lsem.at[k]) for k, (src, dst) in enumerate(views)]
        start(loads)

        def tile_load(u, s):
            slot = lax.rem(u, 2)
            sources = (full, full_sib)
            return [pltpu.make_async_copy(sources[k].at[:, s, :, :, :, step_of(u, TILE)], tiles.at[slot, k], tsem.at[slot, k]) for k in PAIR]

        tile_load(0, 0)[0].start()
        loads[0].wait()

        def kv_tile(u):
            pl.when(u < STEPS - 1)(lambda: tile_load(u + 1, 0)[0].start())
            tile_load(u, 0)[0].wait()
            kvp[:, step_of(u, TILE)] = dot_tn(big[near, KCOL:NBIG], tiles[lax.rem(u, 2), 0].reshape(NEAR, TILE))

        loop(STEPS, kv_tile)
        start(tile_load(0, 0))

        half = core * (DIM // 2)
        quarter = (half, half + QUARTER)
        ring = ((x, y, xn, yn), (y, x, yn, xn))
        first = [quarter[c] + ring[c][0] * EIGHTH for c in PAIR]
        second = [first[c] + ring[c][1] * W for c in PAIR]
        mine = rows16(z * KROWS, KROWS)
        hops = {}

        def hop(step, src, dst, target):
            group = hops.setdefault(step, [])
            group.append(remote(src, dst, (ksend.at[step, len(group)], krecv.at[step, len(group)]), target))

        hop(0, kvp.at[:, lanes(DIM // 2 - half, DIM // 2)], k1, sib)
        for c in PAIR:
            a, b, an, bn = ring[c]
            hop(1, kvp.at[:, lanes(quarter[c] + (1 - a) * EIGHTH, EIGHTH)], k2.at[c], an)
            hop(2, kvp.at[:, lanes(first[c] + (1 - b) * W, W)], k3.at[c], bn)
            same = kvo.at[:, lanes(second[c], W)]
            hop(5, same, same, bn)
            same = kvo.at[:, lanes(first[c], EIGHTH)]
            hop(6, same, same, an)
        for k, there in enumerate(zn):
            hop(3, kc.at[rows16(lax.rem(z + k + 1, 4) * KROWS, KROWS)], k4.at[k], there)
            for c in PAIR:
                same = kvo.at[mine, lanes(second[c], W)]
                hop(4, same, same, there)
        same = kvo.at[:, lanes(half, DIM // 2)]
        hop(7, same, same, sib)

        def kv_add(src, at, width):
            def tile(t):
                cols = lanes(at + t * W, W)
                kvp[:, cols] = kvp[:, cols] + src[:, step_of(t, W)]

            loop(width // W, tile)

        def kv_first():
            kv_add(k1, half, DIM // 2)

        def kv_second():
            for c in PAIR:
                kv_add(k2.at[c], first[c], EIGHTH)

        def kv_third():
            for c in PAIR:
                kc[:, c * W : (c + 1) * W] = kvp[:, lanes(second[c], W)] + k3[c]

        def kv_round():
            total = kc[mine, :] + k4[0] + k4[1] + k4[2]
            for c in PAIR:
                kvo[mine, lanes(second[c], W)] = total[:, c * W : (c + 1) * W].astype(BF16)

        def kv_turn(t):
            rows = step_of(t, TILE)
            for s in PAIR:
                kvt[s] = kvo[s * HEAD : (s + 1) * HEAD, rows].astype(F32).T.astype(BF16)
            copies = [pltpu.make_async_copy(kvt.at[s], (dwk, dwv)[s].at[rows], osem.at[s]) for s in PAIR]
            start(copies)
            wait(copies)

        works = (kv_first, kv_second, kv_third, kv_round)

        def kv_step(j):
            for step in range(len(hops)):

                @pl.when(j == step)
                def _(step=step):
                    wait_recv(hops[step])
                    if step < len(works):
                        works[step]()
                    elif step == len(hops) - 1:
                        loop(STEPS, kv_turn)
                    start(hops.get(step + 1, ()))

        meet(partners)
        start(hops[0])
        ticks = 2 * GROUP - 1
        scatter.tick(ticks)
        wait(loads[1:])

        def out_copies(u):
            slot = lax.rem(u, 2)
            rows = step_of(u, TILE)
            sem = o1sem.at[slot]
            return [
                pltpu.make_async_copy(out1.at[slot, :, 0:FFN], dw1.at[rows], sem.at[0]),
                pltpu.make_async_copy(out1.at[slot, :, FFN : 2 * FFN], dw3.at[rows], sem.at[1]),
                pltpu.make_async_copy(outq.at[slot], dwq.at[rows], sem.at[2]),
            ]

        def out2_copies(u):
            slot, cols = lax.rem(u, 2), step_of(u, TILE)
            sem = o2sem.at[slot]
            return [
                pltpu.make_async_copy(out2.at[slot, 0:FFN], dw2.at[:, cols], sem.at[0]),
                pltpu.make_async_copy(out2.at[slot, FFN:OUT], dwo.at[:, cols], sem.at[1]),
            ]

        def gain_step(i):
            first = i * 2
            two = pl.ds(lax.rem(first, GROUP), 2)
            x_hat, _ = normalize(xb[pl.ds(first, 2)].astype(F32).reshape(BLOCK, DIM))
            gacc[...] = gacc[...] + sums[1, lax.div(first, GROUP), two].astype(F32).reshape(BLOCK, DIM) * x_hat

        near = partners[: len(partners) - len(zn)]
        gain_hops = [remote(gpart.at[k], ggot.at[k], (hsend.at[k], hrecv.at[k]), there) for k, there in enumerate(near)]
        last = len(near)
        gain_last = [remote(gpart.at[last], gz.at[z], (hsend.at[last + k], hrecv.at[last + k]), there) for k, there in enumerate(zn)]
        results = pltpu.make_async_copy(sums, sums_out, osem.at[0])
        gain_out = pltpu.make_async_copy(gpart.at[0], dgain, osem.at[1])

        def gain_start():
            x_in.wait()
            gacc[...] = jnp.zeros_like(gacc)
            loop(GROUP, gain_step)
            gpart[0] = jnp.sum(gacc[...], axis=0, keepdims=True)
            gain_hops[0].start()

        def gain_hop(k):
            gain_hops[k].wait_recv()
            gpart[k + 1] = gpart[k] + ggot[k]
            start(gain_hops[k + 1 : k + 2] or gain_last)

        def gain_finish():
            results.start()
            for k in range(len(near)):
                gain_hop(k)
            gz[z] = gpart[last]
            wait(gain_last)
            wait_send(gain_hops)
            gpart[0] = gz[0] + gz[1] + gz[2] + gz[3]
            gain_out.start()
            gain_out.wait()
            results.wait()

        def tokens(u):
            return tiles[lax.rem(u, 2)].reshape(2 * NEAR, TILE)

        def grad_in(u):
            wait(tile_load(u, 0))
            pl.when(u < STEPS - 1)(lambda: start(tile_load(u + 1, 0)))
            pl.when(u == STEPS - 1)(lambda: start(tile_load(0, 1)))
            pl.when(u > 1)(lambda: wait(out_copies(u - 2)))
            slot = lax.rem(u, 2)
            for s in PAIR:
                out1[slot, :, s * FFN : (s + 1) * FFN] = dot_tn(tokens(u), big[:, s * FFN : (s + 1) * FFN]).astype(BF16)
            outq[slot] = dot_tn(big[:, 2 * FFN : OWN], tokens(u)).T.astype(BF16)
            start(out_copies(u))

        def grad_out(u):
            wait(tile_load(u, 1))
            pl.when(u < STEPS - 1)(lambda: start(tile_load(u + 1, 1)))
            pl.when(u > 1)(lambda: wait(out2_copies(u - 2)))
            slot = lax.rem(u, 2)
            out2[slot, 0:FFN] = dot_tn(big[:, OWN : OWN + FFN], tokens(u)).astype(BF16)
            out2[slot, FFN:OUT] = dot_tn(big[:, OWN + FFN : KCOL], tokens(u)).astype(BF16)
            start(out2_copies(u))

        def first_half(j):
            grad_in(2 * j)
            pl.when(lax.rem(j, 2) == 1)(lambda: scatter.tick(ticks + 1 + lax.div(j, 2)))
            grad_in(2 * j + 1)
            kv_step(j)

        def second_half(j):
            grad_out(2 * j)
            scatter.tick(ticks + 3 + j)
            grad_out(2 * j + 1)
            kv_step(STEPS // 2 + j)

        loop(STEPS // 2, first_half)
        loop(STEPS // 2 - 1, second_half)
        scatter.finish()
        gain_start()
        loop((STEPS - 2, STEPS), grad_out)
        kv_step(STEPS - 1)
        gain_finish()
        for u in (STEPS - 2, STEPS - 1):
            wait(out_copies(u) + out2_copies(u))
        for group in hops.values():
            wait_send(group)


    tall = (*TALL, DIM)
    half = DIM // 2
    wide = [(DIM, NCAT), (NZO, DIM), tall, tall, (SEQ, NCAT), (SEQ, NZO), (SEQ, NCAT), tall, tall, (2, SEQ, SEQ), (4, SEQ, HEAD), (2, GROUP, ROWS, DIM)]
    types = [BF16] * 4 + [F32] + [BF16] * 4 + [F32] + [BF16] * 2
    pl.run_scoped(activations, *[pltpu.VMEM(s, t) for s, t in zip(wide, types)])
    narrow = [(2 * NEAR, NBIG), (2, 2, GROUP, *TALL, TILE), (2, TILE, 2 * FFN), (2, TILE, HEAD), (2, OUT, TILE), (KV, DIM), (2, TILE, HEAD), (ITEMS, ROWS, DIM)]
    totals = [(KV, DIM), (KV, half), (2, KV, EIGHTH), (2, KV, W), (KV, 2 * W), (3, KROWS, 2 * W), (BLOCK, DIM), (4, 1, DIM), (3, 1, DIM), (4, 1, DIM)]
    buffers = [pltpu.VMEM(s, BF16) for s in narrow] + [pltpu.VMEM(s, F32) for s in totals]
    pl.run_scoped(gradients, *buffers)


def layer_call(*args):
    any_spec = pl.BlockSpec(memory_space=pl.ANY)
    vmem_spec = pl.BlockSpec(memory_space=pltpu.VMEM)
    dma = pltpu.SemaphoreType.DMA
    tall = (*TALL, DIM)
    kept = [(GROUP, 2, *tall)] * 2 + [(ITEMS, *tall), (NEAR, NCAT), (NEAR, NZO), (NEAR, OWN), (NEAR, OUT)]
    shapes = kept + [(2, 2, GROUP, ROWS, DIM), (1, DIM), (DIM, FFN), (DIM, FFN), (DIM, HEAD), (FFN, DIM), (HEAD, DIM), (DIM, HEAD), (DIM, HEAD)]
    types = [BF16] * len(shapes)
    types[len(kept) + 1] = F32
    pairs = [(ITEMS, COPIES), (2,), (5,), (GROUP, 2), (GROUP, 3), (8, 6)]
    results = pl.pallas_call(
        layer_kernel,
        out_shape=[jax.ShapeDtypeStruct(s, t) for s, t in zip(shapes, types)],
        in_specs=[any_spec] * (len(args) - 2) + [vmem_spec] * 2,
        out_specs=[any_spec] * len(shapes),
        scratch_shapes=[
            *[dma(s) for s in pairs for _ in PAIR],
            *[dma(s) for s in ((6,), (7,), (2,), (2,), (2, 2), (2, 3), (2, 2), (6,), (6,))],
            pltpu.SemaphoreType.REGULAR,
            pltpu.VMEM((2, 2, GROUP, ROWS, DIM), BF16),
            *scatter_scratch(),
        ],
        compiler_params=pltpu.CompilerParams(collective_id=0, has_side_effects=True, vmem_limit_bytes=VMEM_BYTES),
        name="layer",
    )(*args)
    return results[len(kept) :]


def normalize(x):
    centered = x - mean(x)
    inv_std = lax.rsqrt(mean(centered * centered) + LN_EPS)
    return centered * inv_std, inv_std


def mean(v):
    return jnp.mean(v, axis=-1, keepdims=True)


def finish_kernel(sums, x_loc, dy_loc, gain, *refs):
    *refs, sv, xv, dyv, sem = refs
    count = len(refs) // 3
    sources, (y_out, dx_out, *refs) = refs[:count], refs[count:]
    places, buffers = refs[:count], refs[count:]
    loads = [pltpu.make_async_copy(src, dst, sem.at[k]) for k, (src, dst) in enumerate(zip((sums, x_loc, dy_loc, *sources), (sv, xv, dyv, *buffers)))]
    stores = [pltpu.make_async_copy(src, dst, sem.at[k]) for k, (src, dst) in enumerate(zip((xv, dyv), (y_out, dx_out)))]
    moved = [pltpu.make_async_copy(src, dst, sem.at[3 + k]) for k, (src, dst) in enumerate(zip(buffers, places))]
    start(loads)
    wait(loads[:3])

    def step(i):
        rows = rows16(i * BLOCK, BLOCK)
        res = xv[rows, :].astype(F32)
        x_hat, inv_std = normalize(res)
        d_hat = sv[1, rows, :].astype(F32) * gain[...]
        dx = inv_std * (d_hat - mean(d_hat) - x_hat * mean(d_hat * x_hat)) + dyv[rows, :].astype(F32)
        xv[rows, :] = (res + sv[0, rows, :].astype(F32)).astype(BF16)
        dyv[rows, :] = dx.astype(BF16)

    for k, c in enumerate(moved):
        loop((k, k + 1), step)
        loads[3 + k].wait()
        c.start()
    loop((len(moved), GROUP), step)
    start(stores)
    wait(stores + moved)


def finish_call(sums, x, dy, gain, *grads):
    any_spec = pl.BlockSpec(memory_space=pl.ANY)
    shapes = [x.shape] * 2 + [v.shape for v in grads]
    types = [BF16] * 2 + [v.dtype for v in grads]
    tokens = [sums.shape, x.shape, x.shape]
    return pl.pallas_call(
        finish_kernel,
        out_shape=[jax.ShapeDtypeStruct(s, t) for s, t in zip(shapes, types)],
        in_specs=[any_spec] * 3 + [pl.BlockSpec(memory_space=pltpu.VMEM)] + [any_spec] * len(grads),
        out_specs=[any_spec] * len(shapes),
        scratch_shapes=[
            *[pltpu.VMEM(v.shape, v.dtype) for v in grads],
            *[pltpu.VMEM(s, BF16) for s in tokens],
            pltpu.SemaphoreType.DMA((3 + len(grads),)),
        ],
        compiler_params=pltpu.CompilerParams(vmem_limit_bytes=VMEM_BYTES),
        name="finish",
    )(sums, x, dy, gain, *grads)


def rope_tables():
    inv_freq = ROPE_BASE ** (-jnp.arange(HEAD // 2, dtype=F32) * 2.0 / HEAD)
    pos = row_position(jnp.arange(SEQ, dtype=jnp.int32)).astype(F32)
    angles = pos[:, None] * inv_freq[None, :]
    cos, sin = jnp.cos(angles), jnp.sin(angles)
    return jnp.concatenate([cos, cos], axis=1), jnp.concatenate([-sin, sin], axis=1)


def solution(mesh):
    def layer_shard(x_loc, dy_loc, ln_gain, w_query, w_key, w_value, w_out, w_gate, w_up, w_down):
        h_loc = (ln_gain * normalize(x_loc.astype(F32))[0]).astype(BF16)
        weights = (w_gate, w_up, w_query.reshape(DIM, HEAD), w_key, w_value, w_down, w_out.reshape(HEAD, DIM))
        sums, *grads = layer_call(h_loc, dy_loc, x_loc, *weights, *rope_tables())
        flat = (ITEMS * ROWS, DIM)
        y_loc, grad_x, dgain, dw1, dw3, dwq, dw2, dwo, dwk, dwv = finish_call(
            sums.reshape(2, *flat), x_loc.reshape(flat), dy_loc.reshape(flat), ln_gain.reshape(1, DIM), *grads
        )
        y_loc, grad_x = (v.reshape(x_loc.shape) for v in (y_loc, grad_x))
        return y_loc, grad_x, dgain.reshape(DIM), dwq.reshape(DIM, 1, HEAD), dwk, dwv, dwo.reshape(1, HEAD, DIM), dw1, dw3, dw2

    act = P(None, "tp", None)
    head, columns, lead, every = P(None, "tp", None), P(None, "tp"), P("tp"), P()
    specs = (act, act, every, head, every, every, lead, columns, columns, lead)
    return jax.shard_map(layer_shard, mesh=mesh, in_specs=specs, out_specs=specs, check_vma=False)
```

```python
import jax
import jax.numpy as jnp
import numpy as np
from jax import lax
from jax.experimental import pallas as pl
from jax.experimental.pallas import tpu as pltpu
from jax.sharding import PartitionSpec as P

LN_EPS = 1e-6
ROPE_BASE = 10000.0
MESH = pl.DeviceIdType.MESH
KEEP = dict(axis=-1, keepdims=True)
F32 = jnp.float32
BF16 = jnp.bfloat16
ALL = slice(None)
PAIR = range(2)
LANES = 128
W = 256
VMEM_BYTES = 67043328

GROUP = 8
ITEMS = 2 * GROUP
ROWS = 8
BLOCK = 2 * ROWS
LINE = 4 * BLOCK
SEQ = 4 * LINE
TALL = (2, 2, LINE)
DIM = 4096
HEAD = 128
FFN = 512
OUT = FFN + HEAD
OWN = 2 * FFN + HEAD
KEY = 2 * OWN
VAL = KEY + HEAD
NCAT = VAL + HEAD
NZO = 2 * OUT
QCOL = (2 * FFN, OWN + 2 * FFN)
OCOL = (2 * FFN, 2 * FFN + HEAD)
NEAR = GROUP * SEQ

DEPTH = 5
COPIES = 14


class Columns:
    def __init__(self, a):
        self.a, self.c = a, DIM // 2 - a
        self.left = (slice(0, a), slice(a, 2 * a))
        self.both_left = slice(0, 2 * a)
        self.right = (slice(2 * a, 2 * a + self.c), slice(2 * a + self.c, DIM))
        self.both_right = slice(2 * a, DIM)
        self.halves = (slice(0, self.c), slice(self.c, 2 * self.c))


GCOL = SCOL = Columns(1280)


def place():
    i = lax.axis_index("tp")
    return lax.div(i, 8), lax.rem(lax.div(i, 4), 2), lax.rem(lax.div(i, 2), 2), lax.rem(i, 2)


def index(z, y, x, core):
    return ((z * 2 + y) * 2 + x) * 2 + core


def rows8(start, size):
    return pl.ds(pl.multiple_of(start, ROWS), size)


def rows16(start, size):
    return pl.ds(pl.multiple_of(start, BLOCK), size)


def lanes(start, size):
    return pl.ds(pl.multiple_of(start, LANES), size)


def step_of(t, size):
    return lanes(t * size, size)


def loop(count, body):
    lo, hi = count if isinstance(count, tuple) else (0, count)

    def run(i, carry):
        body(i)
        return carry

    lax.fori_loop(lo, hi, run, 0)


def remote(src, dst, sems, target):
    return pltpu.make_async_remote_copy(src, dst, *sems, device_id=(target,), device_id_type=MESH)


def start(copies):
    for c in copies:
        c.start()


def wait(copies):
    for c in copies:
        c.wait()


def wait_recv(copies):
    for c in copies:
        c.wait_recv()


def wait_send(copies):
    for c in copies:
        c.wait_send()


def partners_of(z, y, x, core):
    chips = [index(lax.rem(z + k, 4), y, x, core) for k in (1, 2, 3)]
    return [index(z, y, x, 1 - core), index(z, y, 1 - x, core), index(z, 1 - y, x, core)] + chips


def greet(semaphore, others):
    for there in others:
        pl.semaphore_signal(semaphore, inc=1, device_id=(there,), device_id_type=MESH)


def dot_nt(a, b):
    return lax.dot_general(a, b, (((1,), (1,)), ((), ())), preferred_element_type=F32)


def dot_tn(a, b):
    return lax.dot_general(a, b, (((0,), (0,)), ((), ())), preferred_element_type=F32)


def dot_nn(a, b):
    return jnp.dot(a, b, preferred_element_type=F32)


def normalize(x):
    centered = x - mean(x)
    inv_std = lax.rsqrt(mean(centered * centered) + LN_EPS)
    return centered * inv_std, inv_std


def mean(v):
    return jnp.mean(v, **KEEP)


def add_into(dst, src, width):
    def tile(t):
        cols = step_of(t, W)
        dst[..., cols] = (dst[..., cols].astype(F32) + src[..., cols].astype(F32)).astype(BF16)

    loop(width // W, tile)


def row_position(r):
    return ((r // BLOCK) % 4) * LINE + (r // (2 * LINE)) * (2 * BLOCK) + ((r // LINE) % 2) * BLOCK + r % BLOCK


class Line:
    def __init__(self, z, y, x, core):
        low = lax.div(z, 2)
        odd = lax.rem(z, 2)
        self.mid = low != odd
        self.end = low == odd
        side = index(z + 1 - 2 * odd, y, x, core)
        across = index(3 - z, y, x, core)
        self.three = rows16(BLOCK - BLOCK * low, 3 * BLOCK)
        self.half = rows16(2 * BLOCK * low, 2 * BLOCK)
        self.other = rows16(2 * BLOCK - 2 * BLOCK * low, 2 * BLOCK)
        self.tip = rows16(3 * BLOCK * low, BLOCK)
        self.own = rows16(BLOCK * z, BLOCK)
        self.spread = ((self.own, side), (self.half, across), (self.three, side))
        self.merge = ((self.three, side), (self.other, across), (self.tip, side))


class Transfer:
    def __init__(self, spot, send, recv):
        self.z, self.y, self.x, self.core = spot
        self.line = Line(*spot)
        self.sib, self.xn, self.yn, *self.zn = partners_of(*spot)
        self.send, self.recv, self.keys = send, recv, {}

    def sems(self, slot, key):
        k = self.keys.setdefault(key, len(self.keys))
        return self.send.at[slot, k], self.recv.at[slot, k]

    def on_end(self, body):
        pl.when(self.line.end)(body)

    def on_mid(self, body):
        pl.when(self.line.mid)(body)

    def tick(self, m):
        for k, stage in reversed(list(enumerate(self.stages))):
            n = m - k
            pl.when((n >= 0) & (n < ITEMS))(lambda stage=stage, n=n: stage(n))


class Gather(Transfer):
    def __init__(self, spot, buf, send, recv):
        super().__init__(spot, send, recv)
        self.buf = buf
        self.stages = (self.stage0, self.stage1, self.stage2, self.stage3, self.stage4, self.stage5)

    def copy(self, n, key, ys, xs, rows, cols, target):
        view = self.buf.at[lax.div(n, 2), lax.rem(n, 2), ys, xs, rows, cols]
        return remote(view, view, self.sems(n, key), target)

    def za(self, n, step):
        rows, target = self.line.spread[step]
        return self.copy(n, ("za", step), self.y, self.x, rows, GCOL.both_left, target)

    def zc(self, n, step):
        rows, target = self.line.spread[step]
        return self.copy(n, ("zc", step), ALL, ALL, rows, GCOL.both_right, target)

    def c1(self, n):
        cols, own = GCOL.right, self.line.own
        return [self.copy(n, "c1x", self.y, self.x, own, cols[0], self.xn), self.copy(n, "c1y", self.y, self.x, own, cols[1], self.yn)]

    def c2(self, n):
        cols, own = GCOL.right, self.line.own
        return [self.copy(n, "c2y", self.y, ALL, own, cols[0], self.yn), self.copy(n, "c2x", ALL, self.x, own, cols[1], self.xn)]

    def a1(self, n):
        cols = GCOL.left
        return [self.copy(n, "a1y", self.y, self.x, ALL, cols[0], self.yn), self.copy(n, "a1x", self.y, self.x, ALL, cols[1], self.xn)]

    def a2(self, n):
        cols = GCOL.left
        return [self.copy(n, "a2x", ALL, self.x, ALL, cols[0], self.xn), self.copy(n, "a2y", self.y, ALL, ALL, cols[1], self.yn)]

    def pass_on(self, chain, n, step):
        def body():
            chain(n, step - 1).wait_recv()
            chain(n, step).start()

        self.on_mid(body)

    def stage0(self, n):
        self.on_end(lambda: self.za(n, 0).start())
        start(self.c1(n))

    def stage1(self, n):
        self.pass_on(self.za, n, 1)
        wait_recv(self.c1(n))
        start(self.c2(n))

    def stage2(self, n):
        self.pass_on(self.za, n, 2)
        wait_recv(self.c2(n))
        self.on_end(lambda: self.zc(n, 0).start())

    def stage3(self, n):
        self.on_end(lambda: self.za(n, 2).wait_recv())
        start(self.a1(n))
        self.pass_on(self.zc, n, 1)

    def stage4(self, n):
        wait_recv(self.a1(n))
        start(self.a2(n))
        self.pass_on(self.zc, n, 2)

    def stage5(self, n):
        wait_recv(self.a2(n))
        self.on_end(lambda: self.zc(n, 2).wait_recv())

    def finish(self, n):
        wait_send(self.c1(n) + self.c2(n) + self.a1(n) + self.a2(n))
        self.on_end(lambda: wait_send([self.za(n, 0), self.zc(n, 0)]))
        self.on_mid(lambda: wait_send([chain(n, step) for chain in (self.za, self.zc) for step in (1, 2)]))


def scatter_shapes():
    a, c = SCOL.a, SCOL.c
    return dict(
        b1=(3, 2, 2, LINE, a), b2=(5, 2, LINE, a), za0=(3, 2, 3 * BLOCK, a), za1=(3, 2, 2 * BLOCK, a), za2=(4, 2, BLOCK, a),
        own_a=(2, 2, 2, LINE, a), own_c=(4, *TALL, 2 * c), zc0=(3, 2, 2, 3 * BLOCK, 2 * c), zc1=(3, 2, 2, 2 * BLOCK, 2 * c),
        zc2=(4, 2, 2, BLOCK, 2 * c), h1=(3, 2, 2, BLOCK, c), h2=(3, 2, BLOCK, c), fin=(3, 2, ROWS, DIM),
    )


SLOTS = 6


def scatter_scratch():
    dma = pltpu.SemaphoreType.DMA
    buffers = [pltpu.VMEM(s, BF16) for s in scatter_shapes().values()]
    return buffers + [dma((SLOTS, COPIES)), dma((SLOTS, COPIES)), dma((SLOTS, 3)), dma((ITEMS,)), dma((ITEMS,))]


class Scatter(Transfer):
    def __init__(self, spot, parts, sums, refs):
        shapes = scatter_shapes()
        self.depth = {name: s[0] for name, s in shapes.items()}
        self.ring = dict(zip(shapes, refs))
        send, recv, self.lsem, *self.store_sems = refs[len(shapes) :]
        super().__init__(spot, send, recv)
        self.parts, self.sums = parts, sums
        self.stages = (self.stage0, self.stage1, self.stage2, self.stage3, self.stage4, self.stage5)

    def slot(self, name, n, *at):
        return self.ring[name].at[(lax.rem(n, self.depth[name]), *at)]

    def copy(self, n, key, src, dst, target):
        return remote(src, dst, self.sems(lax.rem(n, SLOTS), key), target)

    def a1(self, n):
        cols = SCOL.left
        return [
            self.copy(n, "a1x", self.parts.at[n, :, 1 - self.x, :, cols[0]], self.slot("b1", n, 0), self.xn),
            self.copy(n, "a1y", self.parts.at[n, 1 - self.y, :, :, cols[1]], self.slot("b1", n, 1), self.yn),
        ]

    def a2(self, n):
        return [
            self.copy(n, "a2y", self.slot("b1", n, 0, 1 - self.y), self.slot("b2", n, 0), self.yn),
            self.copy(n, "a2x", self.slot("b1", n, 1, 1 - self.x), self.slot("b2", n, 1), self.xn),
        ]

    def za(self, n, step):
        rows, target = self.line.merge[step]
        key = f"za{step}"
        return self.copy(n, key, self.slot("b2", n, ALL, rows, ALL), self.slot(key, n), target)

    def zc(self, n, step):
        rows, target = self.line.merge[step]
        key = f"zc{step}"
        src = self.slot("own_c", n, ALL, ALL, rows, ALL) if step else self.parts.at[n, :, :, rows, SCOL.both_right]
        return self.copy(n, key, src, self.slot(key, n), target)

    def h1(self, n):
        cols = SCOL.halves
        return [
            self.copy(n, "h1y", self.slot("zc2", n, 1 - self.y, ALL, ALL, cols[0]), self.slot("h1", n, 0), self.yn),
            self.copy(n, "h1x", self.slot("zc2", n, ALL, 1 - self.x, ALL, cols[1]), self.slot("h1", n, 1), self.xn),
        ]

    def h2(self, n):
        cols = SCOL.halves
        return [
            self.copy(n, "h2x", self.slot("zc2", n, self.y, 1 - self.x, ALL, cols[0]), self.slot("h2", n, 0), self.xn),
            self.copy(n, "h2y", self.slot("zc2", n, 1 - self.y, self.x, ALL, cols[1]), self.slot("h2", n, 1), self.yn),
        ]

    def loads(self, n):
        sem = self.lsem.at[lax.rem(n, SLOTS)]
        views = (
            (self.parts.at[n, :, self.x, :, SCOL.left[0]], self.slot("own_a", n, 0)),
            (self.parts.at[n, self.y, :, :, SCOL.left[1]], self.slot("own_a", n, 1)),
            (self.parts.at[n, :, :, :, SCOL.both_right], self.slot("own_c", n)),
        )
        return [pltpu.make_async_copy(src, dst, sem.at[k]) for k, (src, dst) in enumerate(views)]

    def kept(self, n):
        return self.sums.at[lax.rem(n, 2), self.core, lax.div(n, 2)]

    def store(self, n):
        send, recv = self.store_sems
        return remote(self.slot("fin", n, 1 - self.core), self.kept(n), (send.at[n], recv.at[n]), self.sib)

    def stage0(self, n):
        start(self.a1(n))
        self.on_end(lambda: self.zc(n, 0).start())
        start(self.loads(n))

    def stage1(self, n):
        wait(self.loads(n))
        wait_recv(self.a1(n))
        for c in PAIR:
            add_into(self.slot("b1", n, c), self.slot("own_a", n, c), SCOL.a)
        start(self.a2(n))

        def middle():
            self.zc(n, 0).wait_recv()
            add_into(self.slot("own_c", n, ALL, ALL, self.line.three), self.slot("zc0", n), 2 * SCOL.c)
            self.zc(n, 1).start()

        self.on_mid(middle)
        wait_send(self.a1(n))
        self.on_end(lambda: self.zc(n, 0).wait_send())

    def stage2(self, n):
        wait_recv(self.a2(n))
        for c, mine in enumerate((self.y, self.x)):
            add_into(self.slot("b2", n, c), self.slot("b1", n, c, mine), SCOL.a)
        self.on_end(lambda: self.za(n, 0).start())

        def middle():
            self.zc(n, 1).wait_recv()
            add_into(self.slot("own_c", n, ALL, ALL, self.line.half), self.slot("zc1", n), 2 * SCOL.c)
            self.zc(n, 2).start()
            self.zc(n, 1).wait_send()

        self.on_mid(middle)
        wait_send(self.a2(n))

    def stage3(self, n):
        own_c = self.slot("own_c", n, ALL, ALL, self.line.own)

        def middle():
            self.za(n, 0).wait_recv()
            add_into(self.slot("b2", n, ALL, self.line.three), self.slot("za0", n), SCOL.a)
            self.za(n, 1).start()
            self.slot("zc2", n)[...] = own_c[...]

        def tip():
            self.zc(n, 2).wait_recv()
            add_into(self.slot("zc2", n), own_c, 2 * SCOL.c)

        self.on_mid(middle)
        self.on_end(tip)
        start(self.h1(n))
        self.on_mid(lambda: self.zc(n, 2).wait_send())
        self.on_end(lambda: self.za(n, 0).wait_send())

    def stage4(self, n):
        def middle():
            self.za(n, 1).wait_recv()
            add_into(self.slot("b2", n, ALL, self.line.half), self.slot("za1", n), SCOL.a)
            self.za(n, 2).start()
            self.za(n, 1).wait_send()

        self.on_mid(middle)
        wait_recv(self.h1(n))
        cols = SCOL.halves
        add_into(self.slot("zc2", n, self.y, ALL, ALL, cols[0]), self.slot("h1", n, 0), SCOL.c)
        add_into(self.slot("zc2", n, ALL, self.x, ALL, cols[1]), self.slot("h1", n, 1), SCOL.c)
        start(self.h2(n))
        wait_send(self.h1(n))

    def stage5(self, n):
        pl.when(n >= self.depth["fin"])(lambda: self.store(n - self.depth["fin"]).wait_send())

        def tip():
            self.za(n, 2).wait_recv()
            add_into(self.slot("b2", n, ALL, self.line.own), self.slot("za2", n), SCOL.a)

        self.on_end(tip)
        self.on_mid(lambda: self.za(n, 2).wait_send())
        wait_recv(self.h2(n))
        fin = self.slot("fin", n)

        def put(total, col):
            for core in PAIR:
                fin[core, :, lanes(col, W)] = total[core * ROWS : (core + 1) * ROWS].astype(BF16)

        def left(t):
            for c in PAIR:
                put(self.slot("b2", n, c, self.line.own)[:, step_of(t, W)].astype(F32), c * SCOL.a + t * W)

        def right(t):
            for c in PAIR:
                mine = self.slot("zc2", n, self.y, self.x)[:, lanes(c * SCOL.c + t * W, W)].astype(F32)
                put(mine + self.slot("h2", n, c)[:, step_of(t, W)].astype(F32), 2 * SCOL.a + c * SCOL.c + t * W)

        loop(SCOL.a // W, left)
        loop(SCOL.c // W, right)
        self.store(n).start()
        self.kept(n)[...] = fin[self.core]
        wait_send(self.h2(n))

    def finish(self):
        loop((ITEMS - self.depth["fin"], ITEMS), lambda n: self.store(n).wait_send())
        loop(ITEMS, lambda n: self.store(n).wait_recv())


TILE = 512
STEPS = DIM // TILE
KV = 2 * HEAD
KCOL = OWN + OUT
NBIG = KCOL + KV
QUARTER = DIM // 4
EIGHTH = DIM // 8
KROWS = KV // 4


def layer_kernel(
    x_loc, dy_loc, gain, w1, w3, wq, wk, wv, w2, wo, cos_t, sin_t,
    full, full_sib, parts, g_all, zo_all, g_sib, zo_sib, sums_out, dgain, dw1, dw3, dwq, dw2, dwo, dwk, dwv,
    gsend, grecv, sx, rx, sw, rw, ss, rs, sg, rg, ksend, krecv, lsem, wsem, osem, gsem,
    tsem, o1sem, o2sem, hsend, hrecv, ready, sums, *scatter_refs,
):
    spot = place()
    z, y, x, core = spot
    partners = partners_of(*spot)
    sib, xn, yn, *zn = partners
    barrier = pltpu.get_barrier_semaphore()
    greet(barrier, partners)
    gather = Gather(spot, full, gsend, grecv)
    scatter = Scatter(spot, parts, sums, scatter_refs)

    def meet(others):
        greet(ready, others)
        pl.semaphore_wait(ready, len(others))

    def activations(wcat, w2o, hv, dyv, proj, zo, g, yo, dho, probs, qs, stage, dy_own):
        own, far_half = (rows8(GROUP * c, GROUP) for c in (core, 1 - core))
        takes = [pltpu.make_async_copy(x_loc, stage, lsem.at[0]), pltpu.make_async_copy(dy_loc.at[own], dy_own, lsem.at[1])]
        start(takes)
        wait(takes)

        def norm_step(i):
            two = pl.ds(i * 2, 2)
            x_hat, _ = normalize(stage[two].astype(F32).reshape(BLOCK, DIM))
            stage[two] = (gain[...] * x_hat).astype(BF16).reshape(2, ROWS, DIM)

        loop(GROUP, norm_step)
        pl.semaphore_wait(barrier, len(partners))

        mine = rows8(BLOCK * z + ROWS * core, ROWS)
        to = [full.at[:, s, y, x, mine, :] for s in PAIR]
        away = (stage.at[far_half], dy_loc.at[far_half])
        swaps = [remote(away[s], to[s], (sx.at[s], rx.at[s]), sib) for s in PAIR]
        puts = [pltpu.make_async_copy(src, dst, lsem.at[s]) for s, (src, dst) in enumerate(zip((stage.at[own], dy_own), to))]
        start(swaps + puts)
        wait(puts)
        wait_recv(swaps)
        loop(2, gather.tick)

        spots = (
            (w1, wcat.at[:, 0:FFN], wcat.at[:, OWN : OWN + FFN]),
            (w3, wcat.at[:, FFN : 2 * FFN], wcat.at[:, OWN + FFN : OWN + 2 * FFN]),
            (wq, wcat.at[:, 2 * FFN : OWN], wcat.at[:, OWN + 2 * FFN : KEY]),
            (w2, w2o.at[0:FFN], w2o.at[FFN : 2 * FFN]),
            (wo, w2o.at[OCOL[0] : OCOL[1]], w2o.at[OCOL[1] : NZO]),
        )
        shared = ((wk, wcat.at[:, KEY:VAL]), (wv, wcat.at[:, VAL:NCAT]))
        weights = [(w, near) for w, near, _ in spots] + list(shared)
        local = [pltpu.make_async_copy(w, near, wsem.at[k]) for k, (w, near) in enumerate(weights)]
        far = [remote(w, there, (sw.at[k], rw.at[k]), sib) for k, (w, _, there) in enumerate(spots)]
        start(local)
        meet([sib])
        start(far)
        loop((2, DEPTH + 1), gather.tick)

        def load(b, s):
            return pltpu.make_async_copy(full.at[b, s], (hv, dyv)[s], lsem.at[s])

        def sib_copy(b, s):
            return remote(full.at[b, s], full_sib.at[b, s], (ss.at[b, s], rs.at[b, s]), sib)

        def arrived(b, s):
            load(b, s).start()
            sib_copy(b, s).start()

        arrived(0, 0)
        wait(local)
        wait_recv(far)

        def gz_copies(b):
            rows = rows16(b * SEQ, SEQ)
            views = (
                (g.at[:, OWN:KEY], g_sib.at[rows]),
                (zo.at[:, FFN : 2 * FFN], zo_sib.at[rows, 0:FFN]),
                (zo.at[:, OCOL[1] : NZO], zo_sib.at[rows, FFN:OUT]),
            )
            return [remote(src, dst, (sg.at[b, k], rg.at[b, k]), sib) for k, (src, dst) in enumerate(views)]

        def gz_local(b):
            rows = rows16(b * SEQ, SEQ)
            return [pltpu.make_async_copy(g, g_all.at[rows], gsem.at[0]), pltpu.make_async_copy(zo, zo_all.at[rows], gsem.at[1])]

        def out(b, s):
            return pltpu.make_async_copy((yo, dho)[s], parts.at[2 * b + s], osem.at[s])

        def drained(b):
            wait([*gz_local(b), out(b, 1)])
            wait_send(gz_copies(b))

        scale = HEAD ** -0.5

        def rotate(v, back=False):
            turn = pltpu.roll(v, HEAD // 2, 1) * sin_t[...]
            return v * cos_t[...] + (-turn if back else turn)

        def flat(ref):
            return ref[...].reshape(SEQ, DIM)

        def gate_up(t):
            at = t * W + lax.div(t, 2) * (OWN - FFN)
            return lanes(at, W), lanes(at + FFN, W)

        wide = lambda t: step_of(t, FFN)

        def batch_step(b):
            ahead = 2 * b + DEPTH + 1
            load(b, 0).wait()

            def proj_tile(t):
                proj[:, wide(t)] = dot_nn(flat(hv), wcat[:, wide(t)])

            loop(NCAT // FFN, proj_tile)
            pl.when(b > 0)(lambda: drained(b - 1))
            scatter.tick(2 * b - 1)

            def hidden_tile(t):
                gate_at, up_at = gate_up(t)
                gate = proj[:, gate_at]
                zo[:, step_of(t, W)] = (gate * jax.nn.sigmoid(gate) * proj[:, up_at]).astype(BF16)

            loop(2 * FFN // W, hidden_tile)
            keys = rotate(proj[:, KEY:VAL]).astype(BF16)
            vals = proj[:, VAL:NCAT].astype(BF16)
            qs[2] = keys
            qs[3] = vals
            causal = row_position(lax.broadcasted_iota(jnp.int32, (SEQ, SEQ), 0)) >= row_position(lax.broadcasted_iota(jnp.int32, (SEQ, SEQ), 1))
            for hd in PAIR:
                query = rotate(proj[:, QCOL[hd] : QCOL[hd] + HEAD]).astype(BF16)
                qs[hd] = query
                scores = jnp.where(causal, dot_nt(query, keys) * scale, -1e30)
                e = jnp.exp(scores - jnp.max(scores, **KEEP))
                p = e / jnp.sum(e, **KEEP)
                probs[hd] = p
                zo[:, OCOL[hd] : OCOL[hd] + HEAD] = dot_nn(p.astype(BF16), vals).astype(BF16)

            gather.tick(ahead)
            arrived(b, 1)

            def y_tile(t):
                yo[:, :, :, wide(t)] = dot_nn(zo[...], w2o[:, wide(t)]).astype(BF16).reshape(*TALL, FFN)

            loop(DIM // FFN, y_tile)
            out(b, 0).start()
            load(b, 1).wait()

            def dz_tile(t):
                dz = dot_nt(flat(dyv), w2o[rows16(t * W, W), :])
                gate_at, up_at = gate_up(t)
                gate = proj[:, gate_at]
                sig = jax.nn.sigmoid(gate)
                g[:, gate_at] = (dz * proj[:, up_at] * sig * (1.0 + gate * (1.0 - sig))).astype(BF16)
                g[:, up_at] = (dz * (gate * sig)).astype(BF16)

            loop(2 * FFN // W, dz_tile)
            out(b, 0).wait()
            scatter.tick(2 * b)
            d_heads = dot_nt(flat(dyv), w2o[2 * FFN : NZO, :]).astype(BF16)
            d_keys = d_vals = jnp.zeros((SEQ, HEAD), F32)
            for hd in PAIR:
                d_out = d_heads[:, hd * HEAD : (hd + 1) * HEAD]
                p = probs[hd]
                d_probs = dot_nt(d_out, qs[3])
                d_vals = d_vals + dot_tn(p.astype(BF16), d_out)
                row_dot = jnp.sum(p * d_probs, **KEEP)
                d_scores = (p * (d_probs - row_dot) * scale).astype(BF16)
                g[:, QCOL[hd] : QCOL[hd] + HEAD] = rotate(dot_nn(d_scores, qs[2]), True).astype(BF16)
                d_keys = d_keys + dot_tn(d_scores, qs[hd])
            g[:, KEY:VAL] = rotate(d_keys, True).astype(BF16)
            g[:, VAL:NCAT] = d_vals.astype(BF16)
            gather.tick(ahead + 1)
            pl.when(b < GROUP - 1)(lambda: arrived(b + 1, 0))

            def dh_tile(t):
                dho[:, :, :, wide(t)] = dot_nt(g[...], wcat[rows16(t * FFN, FFN), :]).astype(BF16).reshape(*TALL, FFN)

            loop(DIM // FFN, dh_tile)
            out(b, 1).start()
            start(gz_local(b) + gz_copies(b))

        loop(GROUP, batch_step)
        drained(GROUP - 1)

        def finish(b):
            for s in PAIR:
                gather.finish(2 * b + s)
                sib_copy(b, s).wait()
            wait_recv(gz_copies(b))

        loop(GROUP, finish)
        wait_send(swaps + far)


    def gradients(big, tiles, out1, outq, out2, kvo, kvt, xb, kvp, k1, k2, k3, kc, k4, gacc, gpart, ggot, gz):
        x_in = pltpu.make_async_copy(x_loc, xb, gsem.at[0])
        x_in.start()
        near, away = slice(0, NEAR), slice(NEAR, 2 * NEAR)
        views = (
            (g_all.at[:, KEY:NCAT], big.at[near, KCOL:NBIG]),
            (g_all.at[:, 0:OWN], big.at[near, 0:OWN]),
            (g_sib, big.at[away, 0:OWN]),
            (zo_all.at[:, 0:FFN], big.at[near, OWN : OWN + FFN]),
            (zo_all.at[:, OCOL[0] : OCOL[1]], big.at[near, OWN + FFN : KCOL]),
            (zo_sib, big.at[away, OWN:KCOL]),
        )
        loads = [pltpu.make_async_copy(src, dst, lsem.at[k]) for k, (src, dst) in enumerate(views)]
        start(loads)

        def tile_load(u, s):
            slot = lax.rem(u, 2)
            sources = (full, full_sib)
            return [pltpu.make_async_copy(sources[k].at[:, s, :, :, :, step_of(u, TILE)], tiles.at[slot, k], tsem.at[slot, k]) for k in PAIR]

        tile_load(0, 0)[0].start()
        loads[0].wait()

        def kv_tile(u):
            pl.when(u < STEPS - 1)(lambda: tile_load(u + 1, 0)[0].start())
            tile_load(u, 0)[0].wait()
            kvp[:, step_of(u, TILE)] = dot_tn(big[near, KCOL:NBIG], tiles[lax.rem(u, 2), 0].reshape(NEAR, TILE))

        loop(STEPS, kv_tile)
        start(tile_load(0, 0))

        half = core * (DIM // 2)
        quarter = (half, half + QUARTER)
        ring = ((x, y, xn, yn), (y, x, yn, xn))
        first = [quarter[c] + ring[c][0] * EIGHTH for c in PAIR]
        second = [first[c] + ring[c][1] * W for c in PAIR]
        mine = rows16(z * KROWS, KROWS)
        hops = {}

        def hop(step, src, dst, target):
            group = hops.setdefault(step, [])
            group.append(remote(src, dst, (ksend.at[step, len(group)], krecv.at[step, len(group)]), target))

        hop(0, kvp.at[:, lanes(DIM // 2 - half, DIM // 2)], k1, sib)
        for c in PAIR:
            a, b, an, bn = ring[c]
            hop(1, kvp.at[:, lanes(quarter[c] + (1 - a) * EIGHTH, EIGHTH)], k2.at[c], an)
            hop(2, kvp.at[:, lanes(first[c] + (1 - b) * W, W)], k3.at[c], bn)
            same = kvo.at[:, lanes(second[c], W)]
            hop(5, same, same, bn)
            same = kvo.at[:, lanes(first[c], EIGHTH)]
            hop(6, same, same, an)
        for k, there in enumerate(zn):
            hop(3, kc.at[rows16(lax.rem(z + k + 1, 4) * KROWS, KROWS)], k4.at[k], there)
            for c in PAIR:
                same = kvo.at[mine, lanes(second[c], W)]
                hop(4, same, same, there)
        same = kvo.at[:, lanes(half, DIM // 2)]
        hop(7, same, same, sib)

        def kv_add(src, at, width):
            def tile(t):
                cols = lanes(at + t * W, W)
                kvp[:, cols] = kvp[:, cols] + src[:, step_of(t, W)]

            loop(width // W, tile)

        def kv_first():
            kv_add(k1, half, DIM // 2)

        def kv_second():
            for c in PAIR:
                kv_add(k2.at[c], first[c], EIGHTH)

        def kv_third():
            for c in PAIR:
                kc[:, c * W : (c + 1) * W] = kvp[:, lanes(second[c], W)] + k3[c]

        def kv_round():
            total = kc[mine, :] + k4[0] + k4[1] + k4[2]
            for c in PAIR:
                kvo[mine, lanes(second[c], W)] = total[:, c * W : (c + 1) * W].astype(BF16)

        def kv_turn(t):
            rows = step_of(t, TILE)
            for s in PAIR:
                kvt[s] = kvo[s * HEAD : (s + 1) * HEAD, rows].astype(F32).T.astype(BF16)
            copies = [pltpu.make_async_copy(kvt.at[s], (dwk, dwv)[s].at[rows], osem.at[s]) for s in PAIR]
            start(copies)
            wait(copies)

        works = (kv_first, kv_second, kv_third, kv_round)

        def kv_step(j):
            for step in range(len(hops)):

                @pl.when(j == step)
                def _(step=step):
                    wait_recv(hops[step])
                    if step < len(works):
                        works[step]()
                    elif step == len(hops) - 1:
                        loop(STEPS, kv_turn)
                    start(hops.get(step + 1, ()))

        meet(partners)
        start(hops[0])
        ticks = ITEMS - 1
        scatter.tick(ticks)
        wait(loads[1:])

        def out_copies(u):
            slot = lax.rem(u, 2)
            rows = step_of(u, TILE)
            sem = o1sem.at[slot]
            return [
                pltpu.make_async_copy(out1.at[slot, :, 0:FFN], dw1.at[rows], sem.at[0]),
                pltpu.make_async_copy(out1.at[slot, :, FFN : 2 * FFN], dw3.at[rows], sem.at[1]),
                pltpu.make_async_copy(outq.at[slot], dwq.at[rows], sem.at[2]),
            ]

        def out2_copies(u):
            slot, cols = lax.rem(u, 2), step_of(u, TILE)
            sem = o2sem.at[slot]
            return [
                pltpu.make_async_copy(out2.at[slot, 0:FFN], dw2.at[:, cols], sem.at[0]),
                pltpu.make_async_copy(out2.at[slot, FFN:OUT], dwo.at[:, cols], sem.at[1]),
            ]

        def gain_step(i):
            first = i * 2
            two = pl.ds(lax.rem(first, GROUP), 2)
            x_hat, _ = normalize(xb[pl.ds(first, 2)].astype(F32).reshape(BLOCK, DIM))
            gacc[...] = gacc[...] + sums[1, lax.div(first, GROUP), two].astype(F32).reshape(BLOCK, DIM) * x_hat

        near = partners[: len(partners) - len(zn)]
        gain_hops = [remote(gpart.at[k], ggot.at[k], (hsend.at[k], hrecv.at[k]), there) for k, there in enumerate(near)]
        last = len(near)
        gain_last = [remote(gpart.at[last], gz.at[z], (hsend.at[last + k], hrecv.at[last + k]), there) for k, there in enumerate(zn)]
        results = pltpu.make_async_copy(sums, sums_out, osem.at[0])
        gain_out = pltpu.make_async_copy(gpart.at[0], dgain, osem.at[1])

        def gain_start():
            x_in.wait()
            gacc[...] = jnp.zeros_like(gacc)
            loop(GROUP, gain_step)
            gpart[0] = jnp.sum(gacc[...], axis=0, keepdims=True)
            gain_hops[0].start()

        def gain_hop(k):
            gain_hops[k].wait_recv()
            gpart[k + 1] = gpart[k] + ggot[k]
            start(gain_hops[k + 1 : k + 2] or gain_last)

        def gain_finish():
            results.start()
            for k in range(1, len(near)):
                gain_hop(k)
            gz[z] = gpart[last]
            wait(gain_last)
            wait_send(gain_hops)
            gpart[0] = gz[0] + gz[1] + gz[2] + gz[3]
            gain_out.start()
            gain_out.wait()
            results.wait()

        def tokens(u):
            return tiles[lax.rem(u, 2)].reshape(2 * NEAR, TILE)

        def grad_in(u):
            wait(tile_load(u, 0))
            pl.when(u < STEPS - 1)(lambda: start(tile_load(u + 1, 0)))
            pl.when(u == STEPS - 1)(lambda: start(tile_load(0, 1)))
            pl.when(u > 1)(lambda: wait(out_copies(u - 2)))
            slot = lax.rem(u, 2)
            for s in PAIR:
                out1[slot, :, s * FFN : (s + 1) * FFN] = dot_tn(tokens(u), big[:, s * FFN : (s + 1) * FFN]).astype(BF16)
            outq[slot] = dot_tn(big[:, 2 * FFN : OWN], tokens(u)).T.astype(BF16)
            start(out_copies(u))

        def grad_out(u):
            wait(tile_load(u, 1))
            pl.when(u < STEPS - 1)(lambda: start(tile_load(u + 1, 1)))
            pl.when(u > 1)(lambda: wait(out2_copies(u - 2)))
            slot = lax.rem(u, 2)
            out2[slot, 0:FFN] = dot_tn(big[:, OWN : OWN + FFN], tokens(u)).astype(BF16)
            out2[slot, FFN:OUT] = dot_tn(big[:, OWN + FFN : KCOL], tokens(u)).astype(BF16)
            start(out2_copies(u))

        def first_half(j):
            grad_in(2 * j)
            pl.when(lax.rem(j, 2) == 1)(lambda: scatter.tick(ticks + 1 + lax.div(j, 2)))
            grad_in(2 * j + 1)
            kv_step(j)

        def second_half(j):
            grad_out(2 * j)
            scatter.tick(ticks + 3 + j)
            grad_out(2 * j + 1)
            kv_step(STEPS // 2 + j)

        loop(STEPS // 2, first_half)
        loop(STEPS // 2 - 1, second_half)
        scatter.finish()
        gain_start()
        loop((STEPS - 2, STEPS - 1), grad_out)
        gain_hop(0)
        loop((STEPS - 1, STEPS), grad_out)
        kv_step(STEPS - 1)
        gain_finish()
        for u in (STEPS - 2, STEPS - 1):
            wait(out_copies(u) + out2_copies(u))
        for group in hops.values():
            wait_send(group)


    tall = (*TALL, DIM)
    half = DIM // 2
    wide = [(DIM, NCAT), (NZO, DIM), tall, tall, (SEQ, NCAT), (SEQ, NZO), (SEQ, NCAT), tall, tall, (2, SEQ, SEQ), (4, SEQ, HEAD)]
    wide += [(ITEMS, ROWS, DIM), (GROUP, ROWS, DIM)]
    types = [BF16] * 4 + [F32] + [BF16] * 4 + [F32] + [BF16] * 3
    pl.run_scoped(activations, *[pltpu.VMEM(s, t) for s, t in zip(wide, types)])
    narrow = [(2 * NEAR, NBIG), (2, 2, GROUP, *TALL, TILE), (2, TILE, 2 * FFN), (2, TILE, HEAD), (2, OUT, TILE), (KV, DIM), (2, TILE, HEAD), (ITEMS, ROWS, DIM)]
    totals = [(KV, DIM), (KV, half), (2, KV, EIGHTH), (2, KV, W), (KV, 2 * W), (3, KROWS, 2 * W), (BLOCK, DIM), (4, 1, DIM), (3, 1, DIM), (4, 1, DIM)]
    buffers = [pltpu.VMEM(s, BF16) for s in narrow] + [pltpu.VMEM(s, F32) for s in totals]
    pl.run_scoped(gradients, *buffers)


def layer_call(*args):
    any_spec = pl.BlockSpec(memory_space=pl.ANY)
    vmem_spec = pl.BlockSpec(memory_space=pltpu.VMEM)
    dma = pltpu.SemaphoreType.DMA
    tall = (*TALL, DIM)
    kept = [(GROUP, 2, *tall)] * 2 + [(ITEMS, *tall), (NEAR, NCAT), (NEAR, NZO), (NEAR, OWN), (NEAR, OUT)]
    shapes = kept + [(2, 2, GROUP, ROWS, DIM), (1, DIM), (DIM, FFN), (DIM, FFN), (DIM, HEAD), (FFN, DIM), (HEAD, DIM), (DIM, HEAD), (DIM, HEAD)]
    types = [BF16] * len(shapes)
    types[len(kept) + 1] = F32
    pairs = [(ITEMS, COPIES), (2,), (5,), (GROUP, 2), (GROUP, 3), (8, 6)]
    results = pl.pallas_call(
        layer_kernel,
        out_shape=[jax.ShapeDtypeStruct(s, t) for s, t in zip(shapes, types)],
        in_specs=[any_spec] * 2 + [vmem_spec] + [any_spec] * (len(args) - 5) + [vmem_spec] * 2,
        out_specs=[any_spec] * len(shapes),
        scratch_shapes=[
            *[dma(s) for s in pairs for _ in PAIR],
            *[dma(s) for s in ((6,), (7,), (2,), (2,), (2, 2), (2, 3), (2, 2), (6,), (6,))],
            pltpu.SemaphoreType.REGULAR,
            pltpu.VMEM((2, 2, GROUP, ROWS, DIM), BF16),
            *scatter_scratch(),
        ],
        compiler_params=pltpu.CompilerParams(collective_id=0, has_side_effects=True, vmem_limit_bytes=VMEM_BYTES),
        name="layer",
    )(*args)
    return results[len(kept) :]


def finish_kernel(sums, x_loc, dy_loc, gain, *refs):
    *refs, sv, xv, dyv, sem = refs
    count = len(refs) // 3
    sources, (y_out, dx_out, *refs) = refs[:count], refs[count:]
    places, buffers = refs[:count], refs[count:]
    loads = [pltpu.make_async_copy(src, dst, sem.at[k]) for k, (src, dst) in enumerate(zip((sums, x_loc, dy_loc, *sources), (sv, xv, dyv, *buffers)))]
    stores = [pltpu.make_async_copy(src, dst, sem.at[k]) for k, (src, dst) in enumerate(zip((xv, dyv), (y_out, dx_out)))]
    moved = [pltpu.make_async_copy(src, dst, sem.at[3 + k]) for k, (src, dst) in enumerate(zip(buffers, places))]
    start(loads)
    wait(loads[:3])

    def step(i):
        rows = rows16(i * BLOCK, BLOCK)
        res = xv[rows, :].astype(F32)
        x_hat, inv_std = normalize(res)
        d_hat = sv[1, rows, :].astype(F32) * gain[...]
        dx = inv_std * (d_hat - mean(d_hat) - x_hat * mean(d_hat * x_hat)) + dyv[rows, :].astype(F32)
        xv[rows, :] = (res + sv[0, rows, :].astype(F32)).astype(BF16)
        dyv[rows, :] = dx.astype(BF16)

    for k, c in enumerate(moved):
        loop((k, k + 1), step)
        loads[3 + k].wait()
        c.start()
    loop((len(moved), GROUP), step)
    start(stores)
    wait(stores + moved)


def finish_call(sums, x, dy, gain, *grads):
    any_spec = pl.BlockSpec(memory_space=pl.ANY)
    shapes = [x.shape] * 2 + [v.shape for v in grads]
    types = [BF16] * 2 + [v.dtype for v in grads]
    tokens = [sums.shape, x.shape, x.shape]
    return pl.pallas_call(
        finish_kernel,
        out_shape=[jax.ShapeDtypeStruct(s, t) for s, t in zip(shapes, types)],
        in_specs=[any_spec] * 3 + [pl.BlockSpec(memory_space=pltpu.VMEM)] + [any_spec] * len(grads),
        out_specs=[any_spec] * len(shapes),
        scratch_shapes=[
            *[pltpu.VMEM(v.shape, v.dtype) for v in grads],
            *[pltpu.VMEM(s, BF16) for s in tokens],
            pltpu.SemaphoreType.DMA((3 + len(grads),)),
        ],
        compiler_params=pltpu.CompilerParams(vmem_limit_bytes=VMEM_BYTES),
        name="finish",
    )(sums, x, dy, gain, *grads)


def rope_tables():
    inv_freq = np.float32(ROPE_BASE) ** (-np.arange(HEAD // 2, dtype=np.float32) * 2 / HEAD)
    pos = row_position(np.arange(SEQ)).astype(np.float32)
    angles = pos[:, None] * inv_freq.astype(np.float32)
    cos, sin = np.cos(angles), np.sin(angles)
    return np.concatenate([cos, cos], axis=1), np.concatenate([-sin, sin], axis=1)


def solution(mesh):
    def layer_shard(x_loc, dy_loc, ln_gain, w_query, w_key, w_value, w_out, w_gate, w_up, w_down):
        gain = ln_gain.reshape(1, DIM)
        weights = (w_gate, w_up, w_query.reshape(DIM, HEAD), w_key, w_value, w_down, w_out.reshape(HEAD, DIM))
        sums, *grads = layer_call(x_loc, dy_loc, gain, *weights, *rope_tables())
        flat = (ITEMS * ROWS, DIM)
        y_loc, grad_x, dgain, dw1, dw3, dwq, dw2, dwo, dwk, dwv = finish_call(
            sums.reshape(2, *flat), x_loc.reshape(flat), dy_loc.reshape(flat), gain, *grads
        )
        y_loc, grad_x = (v.reshape(x_loc.shape) for v in (y_loc, grad_x))
        return y_loc, grad_x, dgain.reshape(DIM), dwq.reshape(DIM, 1, HEAD), dwk, dwv, dwo.reshape(1, HEAD, DIM), dw1, dw3, dw2

    act = P(None, "tp", None)
    columns, lead, every = P(None, "tp"), P("tp"), P()
    specs = (act, act, every, act, every, every, lead, columns, columns, lead)
    return jax.shard_map(layer_shard, mesh=mesh, in_specs=specs, out_specs=specs, check_vma=False)
```

```python
import jax
import jax.numpy as jnp
import numpy as np
from jax import lax
from jax.experimental import pallas as pl
from jax.experimental.pallas import tpu as pltpu
from jax.sharding import PartitionSpec as P

LN_EPS = 1e-6
ROPE_BASE = 10000.0
MESH = pl.DeviceIdType.MESH
KEEP = dict(axis=-1, keepdims=True)
F32 = jnp.float32
BF16 = jnp.bfloat16
ALL = slice(None)
PAIR = range(2)
LANES = 128
W = 256
VMEM_BYTES = 67043328

GROUP = 8
ITEMS = 2 * GROUP
ROWS = 8
BLOCK = 2 * ROWS
LINE = 4 * BLOCK
SEQ = 4 * LINE
TALL = (2, 2, LINE)
DIM = 4096
HEAD = 128
FFN = 512
OUT = FFN + HEAD
OWN = 2 * FFN + HEAD
KEY = 2 * OWN
VAL = KEY + HEAD
NCAT = VAL + HEAD
NZO = 2 * OUT
QCOL = (2 * FFN, OWN + 2 * FFN)
OCOL = (2 * FFN, 2 * FFN + HEAD)
NEAR = GROUP * SEQ

DEPTH = 5
COPIES = 14


class Columns:
    def __init__(self, a):
        self.a, self.c = a, DIM // 2 - a
        self.left = (slice(0, a), slice(a, 2 * a))
        self.both_left = slice(0, 2 * a)
        self.right = (slice(2 * a, 2 * a + self.c), slice(2 * a + self.c, DIM))
        self.both_right = slice(2 * a, DIM)
        self.halves = (slice(0, self.c), slice(self.c, 2 * self.c))


GCOL = SCOL = Columns(1280)


def place():
    i = lax.axis_index("tp")
    return lax.div(i, 8), lax.rem(lax.div(i, 4), 2), lax.rem(lax.div(i, 2), 2), lax.rem(i, 2)


def index(z, y, x, core):
    return ((z * 2 + y) * 2 + x) * 2 + core


def rows8(start, size):
    return pl.ds(pl.multiple_of(start, ROWS), size)


def rows16(start, size):
    return pl.ds(pl.multiple_of(start, BLOCK), size)


def lanes(start, size):
    return pl.ds(pl.multiple_of(start, LANES), size)


def step_of(t, size):
    return lanes(t * size, size)


def loop(count, body):
    lo, hi = count if isinstance(count, tuple) else (0, count)

    def run(i, carry):
        body(i)
        return carry

    lax.fori_loop(lo, hi, run, 0)


def remote(src, dst, sems, target):
    return pltpu.make_async_remote_copy(src, dst, *sems, device_id=(target,), device_id_type=MESH)


def start(copies):
    for c in copies:
        c.start()


def wait(copies):
    for c in copies:
        c.wait()


def wait_recv(copies):
    for c in copies:
        c.wait_recv()


def wait_send(copies):
    for c in copies:
        c.wait_send()


def partners_of(z, y, x, core):
    chips = [index(lax.rem(z + k, 4), y, x, core) for k in (1, 2, 3)]
    return [index(z, y, x, 1 - core), index(z, y, 1 - x, core), index(z, 1 - y, x, core)] + chips


def greet(semaphore, others):
    for there in others:
        pl.semaphore_signal(semaphore, inc=1, device_id=(there,), device_id_type=MESH)


def dot_nt(a, b):
    return lax.dot_general(a, b, (((1,), (1,)), ((), ())), preferred_element_type=F32)


def dot_tn(a, b):
    return lax.dot_general(a, b, (((0,), (0,)), ((), ())), preferred_element_type=F32)


def dot_nn(a, b):
    return jnp.dot(a, b, preferred_element_type=F32)


def normalize(x):
    centered = x - mean(x)
    inv_std = lax.rsqrt(mean(centered * centered) + LN_EPS)
    return centered * inv_std, inv_std


def mean(v):
    return jnp.mean(v, **KEEP)


def add_into(dst, src, width):
    def tile(t):
        cols = step_of(t, W)
        dst[..., cols] = (dst[..., cols].astype(F32) + src[..., cols].astype(F32)).astype(BF16)

    loop(width // W, tile)


def row_position(r):
    return ((r // BLOCK) % 4) * LINE + (r // (2 * LINE)) * (2 * BLOCK) + ((r // LINE) % 2) * BLOCK + r % BLOCK


class Line:
    def __init__(self, z, y, x, core):
        low = lax.div(z, 2)
        odd = lax.rem(z, 2)
        self.mid = low != odd
        self.end = low == odd
        side = index(z + 1 - 2 * odd, y, x, core)
        across = index(3 - z, y, x, core)
        self.three = rows16(BLOCK - BLOCK * low, 3 * BLOCK)
        self.half = rows16(2 * BLOCK * low, 2 * BLOCK)
        self.other = rows16(2 * BLOCK - 2 * BLOCK * low, 2 * BLOCK)
        self.tip = rows16(3 * BLOCK * low, BLOCK)
        self.own = rows16(BLOCK * z, BLOCK)
        self.spread = ((self.own, side), (self.half, across), (self.three, side))
        self.merge = ((self.three, side), (self.other, across), (self.tip, side))


class Transfer:
    def __init__(self, spot, send, recv):
        self.z, self.y, self.x, self.core = spot
        self.line = Line(*spot)
        self.sib, self.xn, self.yn, *self.zn = partners_of(*spot)
        self.send, self.recv, self.keys = send, recv, {}

    def sems(self, slot, key):
        k = self.keys.setdefault(key, len(self.keys))
        return self.send.at[slot, k], self.recv.at[slot, k]

    def on_end(self, body):
        pl.when(self.line.end)(body)

    def on_mid(self, body):
        pl.when(self.line.mid)(body)

    def tick(self, m):
        for k, stage in reversed(list(enumerate(self.stages))):
            n = m - k
            pl.when((n >= 0) & (n < ITEMS))(lambda stage=stage, n=n: stage(n))


class Gather(Transfer):
    def __init__(self, spot, buf, send, recv):
        super().__init__(spot, send, recv)
        self.buf = buf
        self.stages = (self.stage0, self.stage1, self.stage2, self.stage3, self.stage4, self.stage5)

    def copy(self, n, key, ys, xs, rows, cols, target):
        view = self.buf.at[lax.div(n, 2), lax.rem(n, 2), ys, xs, rows, cols]
        return remote(view, view, self.sems(n, key), target)

    def za(self, n, step):
        rows, target = self.line.spread[step]
        return self.copy(n, ("za", step), self.y, self.x, rows, GCOL.both_left, target)

    def zc(self, n, step):
        rows, target = self.line.spread[step]
        return self.copy(n, ("zc", step), ALL, ALL, rows, GCOL.both_right, target)

    def c1(self, n):
        cols, own = GCOL.right, self.line.own
        return [self.copy(n, "c1x", self.y, self.x, own, cols[0], self.xn), self.copy(n, "c1y", self.y, self.x, own, cols[1], self.yn)]

    def c2(self, n):
        cols, own = GCOL.right, self.line.own
        return [self.copy(n, "c2y", self.y, ALL, own, cols[0], self.yn), self.copy(n, "c2x", ALL, self.x, own, cols[1], self.xn)]

    def a1(self, n):
        cols = GCOL.left
        return [self.copy(n, "a1y", self.y, self.x, ALL, cols[0], self.yn), self.copy(n, "a1x", self.y, self.x, ALL, cols[1], self.xn)]

    def a2(self, n):
        cols = GCOL.left
        return [self.copy(n, "a2x", ALL, self.x, ALL, cols[0], self.xn), self.copy(n, "a2y", self.y, ALL, ALL, cols[1], self.yn)]

    def pass_on(self, chain, n, step):
        def body():
            chain(n, step - 1).wait_recv()
            chain(n, step).start()

        self.on_mid(body)

    def stage0(self, n):
        self.on_end(lambda: self.za(n, 0).start())
        start(self.c1(n))

    def stage1(self, n):
        self.pass_on(self.za, n, 1)
        wait_recv(self.c1(n))
        start(self.c2(n))

    def stage2(self, n):
        self.pass_on(self.za, n, 2)
        wait_recv(self.c2(n))
        self.on_end(lambda: self.zc(n, 0).start())

    def stage3(self, n):
        self.on_end(lambda: self.za(n, 2).wait_recv())
        start(self.a1(n))
        self.pass_on(self.zc, n, 1)

    def stage4(self, n):
        wait_recv(self.a1(n))
        start(self.a2(n))
        self.pass_on(self.zc, n, 2)

    def stage5(self, n):
        wait_recv(self.a2(n))
        self.on_end(lambda: self.zc(n, 2).wait_recv())

    def finish(self, n):
        wait_send(self.c1(n) + self.c2(n) + self.a1(n) + self.a2(n))
        self.on_end(lambda: wait_send([self.za(n, 0), self.zc(n, 0)]))
        self.on_mid(lambda: wait_send([chain(n, step) for chain in (self.za, self.zc) for step in (1, 2)]))


def scatter_shapes():
    a, c = SCOL.a, SCOL.c
    return dict(
        b1=(3, 2, 2, LINE, a), b2=(5, 2, LINE, a), za0=(3, 2, 3 * BLOCK, a), za1=(3, 2, 2 * BLOCK, a), za2=(4, 2, BLOCK, a),
        own_a=(2, 2, 2, LINE, a), own_c=(4, *TALL, 2 * c), zc0=(3, 2, 2, 3 * BLOCK, 2 * c), zc1=(3, 2, 2, 2 * BLOCK, 2 * c),
        zc2=(4, 2, 2, BLOCK, 2 * c), h1=(3, 2, 2, BLOCK, c), h2=(3, 2, BLOCK, c), fin=(3, 2, ROWS, DIM),
    )


SLOTS = 6


def scatter_scratch():
    dma = pltpu.SemaphoreType.DMA
    buffers = [pltpu.VMEM(s, BF16) for s in scatter_shapes().values()]
    return buffers + [dma((SLOTS, COPIES)), dma((SLOTS, COPIES)), dma((SLOTS, 3)), dma((ITEMS,)), dma((ITEMS,))]


class Scatter(Transfer):
    def __init__(self, spot, parts, sums, refs):
        shapes = scatter_shapes()
        self.depth = {name: s[0] for name, s in shapes.items()}
        self.ring = dict(zip(shapes, refs))
        send, recv, self.lsem, *self.store_sems = refs[len(shapes) :]
        super().__init__(spot, send, recv)
        self.parts, self.sums = parts, sums
        self.stages = (self.stage0, self.stage1, self.stage2, self.stage3, self.stage4, self.stage5)

    def slot(self, name, n, *at):
        return self.ring[name].at[(lax.rem(n, self.depth[name]), *at)]

    def copy(self, n, key, src, dst, target):
        return remote(src, dst, self.sems(lax.rem(n, SLOTS), key), target)

    def a1(self, n):
        cols = SCOL.left
        return [
            self.copy(n, "a1x", self.parts.at[n, :, 1 - self.x, :, cols[0]], self.slot("b1", n, 0), self.xn),
            self.copy(n, "a1y", self.parts.at[n, 1 - self.y, :, :, cols[1]], self.slot("b1", n, 1), self.yn),
        ]

    def a2(self, n):
        return [
            self.copy(n, "a2y", self.slot("b1", n, 0, 1 - self.y), self.slot("b2", n, 0), self.yn),
            self.copy(n, "a2x", self.slot("b1", n, 1, 1 - self.x), self.slot("b2", n, 1), self.xn),
        ]

    def za(self, n, step):
        rows, target = self.line.merge[step]
        key = f"za{step}"
        return self.copy(n, key, self.slot("b2", n, ALL, rows, ALL), self.slot(key, n), target)

    def zc(self, n, step):
        rows, target = self.line.merge[step]
        key = f"zc{step}"
        src = self.slot("own_c", n, ALL, ALL, rows, ALL) if step else self.parts.at[n, :, :, rows, SCOL.both_right]
        return self.copy(n, key, src, self.slot(key, n), target)

    def h1(self, n):
        cols = SCOL.halves
        return [
            self.copy(n, "h1y", self.slot("zc2", n, 1 - self.y, ALL, ALL, cols[0]), self.slot("h1", n, 0), self.yn),
            self.copy(n, "h1x", self.slot("zc2", n, ALL, 1 - self.x, ALL, cols[1]), self.slot("h1", n, 1), self.xn),
        ]

    def h2(self, n):
        cols = SCOL.halves
        return [
            self.copy(n, "h2x", self.slot("zc2", n, self.y, 1 - self.x, ALL, cols[0]), self.slot("h2", n, 0), self.xn),
            self.copy(n, "h2y", self.slot("zc2", n, 1 - self.y, self.x, ALL, cols[1]), self.slot("h2", n, 1), self.yn),
        ]

    def loads(self, n):
        sem = self.lsem.at[lax.rem(n, SLOTS)]
        views = (
            (self.parts.at[n, :, self.x, :, SCOL.left[0]], self.slot("own_a", n, 0)),
            (self.parts.at[n, self.y, :, :, SCOL.left[1]], self.slot("own_a", n, 1)),
            (self.parts.at[n, :, :, :, SCOL.both_right], self.slot("own_c", n)),
        )
        return [pltpu.make_async_copy(src, dst, sem.at[k]) for k, (src, dst) in enumerate(views)]

    def kept(self, n):
        return self.sums.at[lax.rem(n, 2), self.core, lax.div(n, 2)]

    def store(self, n):
        send, recv = self.store_sems
        return remote(self.slot("fin", n, 1 - self.core), self.kept(n), (send.at[n], recv.at[n]), self.sib)

    def stage0(self, n):
        start(self.a1(n))
        self.on_end(lambda: self.zc(n, 0).start())
        start(self.loads(n))

    def stage1(self, n):
        wait(self.loads(n))
        wait_recv(self.a1(n))
        for c in PAIR:
            add_into(self.slot("b1", n, c), self.slot("own_a", n, c), SCOL.a)
        start(self.a2(n))

        def middle():
            self.zc(n, 0).wait_recv()
            add_into(self.slot("own_c", n, ALL, ALL, self.line.three), self.slot("zc0", n), 2 * SCOL.c)
            self.zc(n, 1).start()

        self.on_mid(middle)
        wait_send(self.a1(n))
        self.on_end(lambda: self.zc(n, 0).wait_send())

    def stage2(self, n):
        wait_recv(self.a2(n))
        for c, mine in enumerate((self.y, self.x)):
            add_into(self.slot("b2", n, c), self.slot("b1", n, c, mine), SCOL.a)
        self.on_end(lambda: self.za(n, 0).start())

        def middle():
            self.zc(n, 1).wait_recv()
            add_into(self.slot("own_c", n, ALL, ALL, self.line.half), self.slot("zc1", n), 2 * SCOL.c)
            self.zc(n, 2).start()
            self.zc(n, 1).wait_send()

        self.on_mid(middle)
        wait_send(self.a2(n))

    def stage3(self, n):
        own_c = self.slot("own_c", n, ALL, ALL, self.line.own)

        def middle():
            self.za(n, 0).wait_recv()
            add_into(self.slot("b2", n, ALL, self.line.three), self.slot("za0", n), SCOL.a)
            self.za(n, 1).start()
            self.slot("zc2", n)[...] = own_c[...]

        def tip():
            self.zc(n, 2).wait_recv()
            add_into(self.slot("zc2", n), own_c, 2 * SCOL.c)

        self.on_mid(middle)
        self.on_end(tip)
        start(self.h1(n))
        self.on_mid(lambda: self.zc(n, 2).wait_send())
        self.on_end(lambda: self.za(n, 0).wait_send())

    def stage4(self, n):
        def middle():
            self.za(n, 1).wait_recv()
            add_into(self.slot("b2", n, ALL, self.line.half), self.slot("za1", n), SCOL.a)
            self.za(n, 2).start()
            self.za(n, 1).wait_send()

        self.on_mid(middle)
        wait_recv(self.h1(n))
        cols = SCOL.halves
        add_into(self.slot("zc2", n, self.y, ALL, ALL, cols[0]), self.slot("h1", n, 0), SCOL.c)
        add_into(self.slot("zc2", n, ALL, self.x, ALL, cols[1]), self.slot("h1", n, 1), SCOL.c)
        start(self.h2(n))
        wait_send(self.h1(n))

    def stage5(self, n):
        pl.when(n >= self.depth["fin"])(lambda: self.store(n - self.depth["fin"]).wait_send())

        def tip():
            self.za(n, 2).wait_recv()
            add_into(self.slot("b2", n, ALL, self.line.own), self.slot("za2", n), SCOL.a)

        self.on_end(tip)
        self.on_mid(lambda: self.za(n, 2).wait_send())
        wait_recv(self.h2(n))
        fin = self.slot("fin", n)

        def put(total, col):
            for core in PAIR:
                fin[core, :, lanes(col, W)] = total[core * ROWS : (core + 1) * ROWS].astype(BF16)

        def left(t):
            for c in PAIR:
                put(self.slot("b2", n, c, self.line.own)[:, step_of(t, W)].astype(F32), c * SCOL.a + t * W)

        def right(t):
            for c in PAIR:
                mine = self.slot("zc2", n, self.y, self.x)[:, lanes(c * SCOL.c + t * W, W)].astype(F32)
                put(mine + self.slot("h2", n, c)[:, step_of(t, W)].astype(F32), 2 * SCOL.a + c * SCOL.c + t * W)

        loop(SCOL.a // W, left)
        loop(SCOL.c // W, right)
        self.store(n).start()
        self.kept(n)[...] = fin[self.core]
        wait_send(self.h2(n))

    def finish(self):
        loop((ITEMS - self.depth["fin"], ITEMS), lambda n: self.store(n).wait_send())
        loop(ITEMS, lambda n: self.store(n).wait_recv())


TILE = 512
STEPS = DIM // TILE
KV = 2 * HEAD
KCOL = OWN + OUT
NBIG = KCOL + KV
QUARTER = DIM // 4
EIGHTH = DIM // 8
KROWS = KV // 4


def layer_kernel(
    x_loc, dy_loc, gain, w1, w3, wq, wk, wv, w2, wo, cos_t, sin_t,
    full, full_sib, parts, g_all, zo_all, g_sib, zo_sib, sums_out, dgain, dw1, dw3, dwq, dw2, dwo, dwk, dwv,
    gsend, grecv, sx, rx, sw, rw, ss, rs, sg, rg, ksend, krecv, lsem, wsem, osem, gsem,
    tsem, o1sem, o2sem, tosem, hsend, hrecv, ready, sums, *scatter_refs,
):
    spot = place()
    z, y, x, core = spot
    partners = partners_of(*spot)
    sib, xn, yn, *zn = partners
    barrier = pltpu.get_barrier_semaphore()
    greet(barrier, partners)
    gather = Gather(spot, full, gsend, grecv)
    scatter = Scatter(spot, parts, sums, scatter_refs)

    def meet(others):
        greet(ready, others)
        pl.semaphore_wait(ready, len(others))

    def activations(wcat, w2o, hv, dyv, proj, zo, g, yo, dho, probs, qs, stage, dy_own):
        own, far_half = (rows8(GROUP * c, GROUP) for c in (core, 1 - core))
        takes = [pltpu.make_async_copy(x_loc, stage, lsem.at[0]), pltpu.make_async_copy(dy_loc.at[own], dy_own, lsem.at[1])]
        start(takes)
        wait(takes)

        def norm_step(i):
            two = pl.ds(i * 2, 2)
            x_hat, _ = normalize(stage[two].astype(F32).reshape(BLOCK, DIM))
            stage[two] = (gain[...] * x_hat).astype(BF16).reshape(2, ROWS, DIM)

        loop(GROUP, norm_step)
        pl.semaphore_wait(barrier, len(partners))

        mine = rows8(BLOCK * z + ROWS * core, ROWS)
        to = [full.at[:, s, y, x, mine, :] for s in PAIR]
        away = (stage.at[far_half], dy_loc.at[far_half])
        swaps = [remote(away[s], to[s], (sx.at[s], rx.at[s]), sib) for s in PAIR]
        puts = [pltpu.make_async_copy(src, dst, lsem.at[s]) for s, (src, dst) in enumerate(zip((stage.at[own], dy_own), to))]
        start(swaps + puts)
        wait(puts)
        wait_recv(swaps)
        loop(2, gather.tick)

        spots = (
            (w1, wcat.at[:, 0:FFN], wcat.at[:, OWN : OWN + FFN]),
            (w3, wcat.at[:, FFN : 2 * FFN], wcat.at[:, OWN + FFN : OWN + 2 * FFN]),
            (wq, wcat.at[:, 2 * FFN : OWN], wcat.at[:, OWN + 2 * FFN : KEY]),
            (w2, w2o.at[0:FFN], w2o.at[FFN : 2 * FFN]),
            (wo, w2o.at[OCOL[0] : OCOL[1]], w2o.at[OCOL[1] : NZO]),
        )
        shared = ((wk, wcat.at[:, KEY:VAL]), (wv, wcat.at[:, VAL:NCAT]))
        weights = [(w, near) for w, near, _ in spots] + list(shared)
        local = [pltpu.make_async_copy(w, near, wsem.at[k]) for k, (w, near) in enumerate(weights)]
        far = [remote(w, there, (sw.at[k], rw.at[k]), sib) for k, (w, _, there) in enumerate(spots)]
        start(local)
        meet([sib])
        start(far)
        loop((2, DEPTH + 1), gather.tick)

        def load(b, s):
            return pltpu.make_async_copy(full.at[b, s], (hv, dyv)[s], lsem.at[s])

        def sib_copy(b, s):
            return remote(full.at[b, s], full_sib.at[b, s], (ss.at[b, s], rs.at[b, s]), sib)

        def arrived(b, s):
            load(b, s).start()
            sib_copy(b, s).start()

        arrived(0, 0)
        wait(local)
        wait_recv(far)

        def gz_copies(b):
            rows = rows16(b * SEQ, SEQ)
            views = (
                (g.at[:, OWN:KEY], g_sib.at[rows]),
                (zo.at[:, FFN : 2 * FFN], zo_sib.at[rows, 0:FFN]),
                (zo.at[:, OCOL[1] : NZO], zo_sib.at[rows, FFN:OUT]),
            )
            return [remote(src, dst, (sg.at[b, k], rg.at[b, k]), sib) for k, (src, dst) in enumerate(views)]

        def gz_local(b):
            rows = rows16(b * SEQ, SEQ)
            return [pltpu.make_async_copy(g, g_all.at[rows], gsem.at[0]), pltpu.make_async_copy(zo, zo_all.at[rows], gsem.at[1])]

        def out(b, s):
            return pltpu.make_async_copy((yo, dho)[s], parts.at[2 * b + s], osem.at[s])

        def drained(b):
            wait([*gz_local(b), out(b, 1)])
            wait_send(gz_copies(b))

        scale = HEAD ** -0.5

        def rotate(v, back=False):
            turn = pltpu.roll(v, HEAD // 2, 1) * sin_t[...]
            return v * cos_t[...] + (-turn if back else turn)

        def flat(ref):
            return ref[...].reshape(SEQ, DIM)

        def gate_up(t):
            at = t * W + lax.div(t, 2) * (OWN - FFN)
            return lanes(at, W), lanes(at + FFN, W)

        wide = lambda t: step_of(t, FFN)

        def batch_step(b):
            ahead = 2 * b + DEPTH + 1
            load(b, 0).wait()

            def proj_tile(t):
                proj[:, wide(t)] = dot_nn(flat(hv), wcat[:, wide(t)])

            loop(NCAT // FFN, proj_tile)
            pl.when(b > 0)(lambda: drained(b - 1))
            scatter.tick(2 * b - 1)

            def hidden_tile(t):
                gate_at, up_at = gate_up(t)
                gate = proj[:, gate_at]
                zo[:, step_of(t, W)] = (gate * jax.nn.sigmoid(gate) * proj[:, up_at]).astype(BF16)

            loop(2 * FFN // W, hidden_tile)
            keys = rotate(proj[:, KEY:VAL]).astype(BF16)
            vals = proj[:, VAL:NCAT].astype(BF16)
            qs[2] = keys
            qs[3] = vals
            causal = row_position(lax.broadcasted_iota(jnp.int32, (SEQ, SEQ), 0)) >= row_position(lax.broadcasted_iota(jnp.int32, (SEQ, SEQ), 1))
            for hd in PAIR:
                query = rotate(proj[:, QCOL[hd] : QCOL[hd] + HEAD]).astype(BF16)
                qs[hd] = query
                scores = jnp.where(causal, dot_nt(query, keys) * scale, -1e30)
                e = jnp.exp(scores - jnp.max(scores, **KEEP))
                p = e / jnp.sum(e, **KEEP)
                probs[hd] = p
                zo[:, OCOL[hd] : OCOL[hd] + HEAD] = dot_nn(p.astype(BF16), vals).astype(BF16)

            gather.tick(ahead)
            arrived(b, 1)

            def y_tile(t):
                yo[:, :, :, wide(t)] = dot_nn(zo[...], w2o[:, wide(t)]).astype(BF16).reshape(*TALL, FFN)

            loop(DIM // FFN, y_tile)
            out(b, 0).start()
            load(b, 1).wait()

            def dz_tile(t):
                dz = dot_nt(flat(dyv), w2o[rows16(t * W, W), :])
                gate_at, up_at = gate_up(t)
                gate = proj[:, gate_at]
                sig = jax.nn.sigmoid(gate)
                g[:, gate_at] = (dz * proj[:, up_at] * sig * (1.0 + gate * (1.0 - sig))).astype(BF16)
                g[:, up_at] = (dz * (gate * sig)).astype(BF16)

            loop(2 * FFN // W, dz_tile)
            out(b, 0).wait()
            scatter.tick(2 * b)
            d_heads = dot_nt(flat(dyv), w2o[2 * FFN : NZO, :]).astype(BF16)
            d_keys = d_vals = jnp.zeros((SEQ, HEAD), F32)
            for hd in PAIR:
                d_out = d_heads[:, hd * HEAD : (hd + 1) * HEAD]
                p = probs[hd]
                d_probs = dot_nt(d_out, qs[3])
                d_vals = d_vals + dot_tn(p.astype(BF16), d_out)
                row_dot = jnp.sum(p * d_probs, **KEEP)
                d_scores = (p * (d_probs - row_dot) * scale).astype(BF16)
                g[:, QCOL[hd] : QCOL[hd] + HEAD] = rotate(dot_nn(d_scores, qs[2]), True).astype(BF16)
                d_keys = d_keys + dot_tn(d_scores, qs[hd])
            g[:, KEY:VAL] = rotate(d_keys, True).astype(BF16)
            g[:, VAL:NCAT] = d_vals.astype(BF16)
            gather.tick(ahead + 1)
            pl.when(b < GROUP - 1)(lambda: arrived(b + 1, 0))

            def dh_tile(t):
                dho[:, :, :, wide(t)] = dot_nt(g[...], wcat[rows16(t * FFN, FFN), :]).astype(BF16).reshape(*TALL, FFN)

            loop(DIM // FFN, dh_tile)
            out(b, 1).start()
            start(gz_local(b) + gz_copies(b))

        loop(GROUP, batch_step)
        drained(GROUP - 1)

        def finish(b):
            for s in PAIR:
                gather.finish(2 * b + s)
                sib_copy(b, s).wait()
            wait_recv(gz_copies(b))

        loop(GROUP, finish)
        wait_send(swaps + far)


    def gradients(big, tiles, out1, outq, out2, kvo, xb, kvp, k1, k2, k3, kc, k4, gacc, gpart, ggot, gz):
        x_in = pltpu.make_async_copy(x_loc, xb, gsem.at[0])
        x_in.start()
        near, away = slice(0, NEAR), slice(NEAR, 2 * NEAR)
        views = (
            (g_all.at[:, KEY:NCAT], big.at[near, KCOL:NBIG]),
            (g_all.at[:, 0:OWN], big.at[near, 0:OWN]),
            (g_sib, big.at[away, 0:OWN]),
            (zo_all.at[:, 0:FFN], big.at[near, OWN : OWN + FFN]),
            (zo_all.at[:, OCOL[0] : OCOL[1]], big.at[near, OWN + FFN : KCOL]),
            (zo_sib, big.at[away, OWN:KCOL]),
        )
        loads = [pltpu.make_async_copy(src, dst, lsem.at[k]) for k, (src, dst) in enumerate(views)]
        start(loads)

        def tile_load(u, s):
            slot = lax.rem(u, 2)
            sources = (full, full_sib)
            return [pltpu.make_async_copy(sources[k].at[:, s, :, :, :, step_of(u, TILE)], tiles.at[slot, k], tsem.at[slot, k]) for k in PAIR]

        tile_load(0, 0)[0].start()
        loads[0].wait()

        def kv_tile(u):
            pl.when(u < STEPS - 1)(lambda: tile_load(u + 1, 0)[0].start())
            tile_load(u, 0)[0].wait()
            kvp[:, step_of(u, TILE)] = dot_tn(big[near, KCOL:NBIG], tiles[lax.rem(u, 2), 0].reshape(NEAR, TILE))

        loop(STEPS, kv_tile)
        start(tile_load(0, 0))

        half = core * (DIM // 2)
        quarter = (half, half + QUARTER)
        ring = ((x, y, xn, yn), (y, x, yn, xn))
        first = [quarter[c] + ring[c][0] * EIGHTH for c in PAIR]
        second = [first[c] + ring[c][1] * W for c in PAIR]
        mine = rows16(z * KROWS, KROWS)
        hops = {}

        def hop(step, src, dst, target):
            group = hops.setdefault(step, [])
            group.append(remote(src, dst, (ksend.at[step, len(group)], krecv.at[step, len(group)]), target))

        hop(0, kvp.at[:, lanes(DIM // 2 - half, DIM // 2)], k1, sib)
        for c in PAIR:
            a, b, an, bn = ring[c]
            hop(1, kvp.at[:, lanes(quarter[c] + (1 - a) * EIGHTH, EIGHTH)], k2.at[c], an)
            hop(2, kvp.at[:, lanes(first[c] + (1 - b) * W, W)], k3.at[c], bn)
            same = kvo.at[:, lanes(second[c], W)]
            hop(5, same, same, bn)
            same = kvo.at[:, lanes(first[c], EIGHTH)]
            hop(6, same, same, an)
        for k, there in enumerate(zn):
            hop(3, kc.at[rows16(lax.rem(z + k + 1, 4) * KROWS, KROWS)], k4.at[k], there)
            for c in PAIR:
                same = kvo.at[mine, lanes(second[c], W)]
                hop(4, same, same, there)
        same = kvo.at[:, lanes(half, DIM // 2)]
        hop(7, same, same, sib)

        def kv_add(src, at, width):
            def tile(t):
                cols = lanes(at + t * W, W)
                kvp[:, cols] = kvp[:, cols] + src[:, step_of(t, W)]

            loop(width // W, tile)

        def kv_first():
            kv_add(k1, half, DIM // 2)

        def kv_second():
            for c in PAIR:
                kv_add(k2.at[c], first[c], EIGHTH)

        def kv_third():
            for c in PAIR:
                kc[:, c * W : (c + 1) * W] = kvp[:, lanes(second[c], W)] + k3[c]

        def kv_round():
            total = kc[mine, :] + k4[0] + k4[1] + k4[2]
            for c in PAIR:
                kvo[mine, lanes(second[c], W)] = total[:, c * W : (c + 1) * W].astype(BF16)

        def turned(t):
            views = ((out1.at[s, :, lanes(t * HEAD, HEAD)], (dwk, dwv)[s].at[step_of(t, TILE)]) for s in PAIR)
            return [pltpu.make_async_copy(src, dst, tosem.at[s, t]) for s, (src, dst) in enumerate(views)]

        def kv_turn(t):
            for s in PAIR:
                out1[s, :, lanes(t * HEAD, HEAD)] = kvo[s * HEAD : (s + 1) * HEAD, step_of(t, TILE)].astype(F32).T.astype(BF16)
            start(turned(t))

        works = (kv_first, kv_second, kv_third, kv_round)

        def kv_step(j):
            for step in range(len(hops)):

                @pl.when(j == step)
                def _(step=step):
                    wait_recv(hops[step])
                    if step < len(works):
                        works[step]()
                    elif step == len(hops) - 1:
                        loop((STEPS - 2, STEPS), lambda u: wait(out_copies(u)))
                        loop(STEPS, kv_turn)
                    start(hops.get(step + 1, ()))

        meet(partners)
        start(hops[0])
        ticks = ITEMS - 1
        scatter.tick(ticks)
        wait(loads[1:])

        def out_copies(u):
            slot = lax.rem(u, 2)
            rows = step_of(u, TILE)
            sem = o1sem.at[slot]
            return [
                pltpu.make_async_copy(out1.at[slot, :, 0:FFN], dw1.at[rows], sem.at[0]),
                pltpu.make_async_copy(out1.at[slot, :, FFN : 2 * FFN], dw3.at[rows], sem.at[1]),
                pltpu.make_async_copy(outq.at[slot], dwq.at[rows], sem.at[2]),
            ]

        def out2_copies(u):
            slot, cols = lax.rem(u, 2), step_of(u, TILE)
            sem = o2sem.at[slot]
            return [
                pltpu.make_async_copy(out2.at[slot, 0:FFN], dw2.at[:, cols], sem.at[0]),
                pltpu.make_async_copy(out2.at[slot, FFN:OUT], dwo.at[:, cols], sem.at[1]),
            ]

        def gain_step(i):
            first = i * 2
            two = pl.ds(lax.rem(first, GROUP), 2)
            x_hat, _ = normalize(xb[pl.ds(first, 2)].astype(F32).reshape(BLOCK, DIM))
            gacc[...] = gacc[...] + sums[1, lax.div(first, GROUP), two].astype(F32).reshape(BLOCK, DIM) * x_hat

        near = partners[: len(partners) - len(zn)]
        gain_hops = [remote(gpart.at[k], ggot.at[k], (hsend.at[k], hrecv.at[k]), there) for k, there in enumerate(near)]
        last = len(near)
        gain_last = [remote(gpart.at[last], gz.at[z], (hsend.at[last + k], hrecv.at[last + k]), there) for k, there in enumerate(zn)]
        results = pltpu.make_async_copy(sums, sums_out, osem.at[0])
        gain_out = pltpu.make_async_copy(gpart.at[0], dgain, osem.at[1])

        def gain_start():
            results.start()
            x_in.wait()
            gacc[...] = jnp.zeros_like(gacc)
            loop(GROUP, gain_step)
            gpart[0] = jnp.sum(gacc[...], axis=0, keepdims=True)
            gain_hops[0].start()

        def gain_hop(k):
            gain_hops[k].wait_recv()
            gpart[k + 1] = gpart[k] + ggot[k]
            start(gain_hops[k + 1 : k + 2] or gain_last)

        def gain_finish():
            gain_hop(last - 1)
            gz[z] = gpart[last]
            wait(gain_last)
            wait_send(gain_hops)
            gpart[0] = gz[0] + gz[1] + gz[2] + gz[3]
            gain_out.start()
            gain_out.wait()
            results.wait()

        def tokens(u):
            return tiles[lax.rem(u, 2)].reshape(2 * NEAR, TILE)

        def grad_in(u):
            wait(tile_load(u, 0))
            pl.when(u < STEPS - 1)(lambda: start(tile_load(u + 1, 0)))
            pl.when(u == STEPS - 1)(lambda: start(tile_load(0, 1)))
            pl.when(u > 1)(lambda: wait(out_copies(u - 2)))
            slot = lax.rem(u, 2)
            for s in PAIR:
                out1[slot, :, s * FFN : (s + 1) * FFN] = dot_tn(tokens(u), big[:, s * FFN : (s + 1) * FFN]).astype(BF16)
            outq[slot] = dot_tn(big[:, 2 * FFN : OWN], tokens(u)).T.astype(BF16)
            start(out_copies(u))

        def grad_out(u):
            wait(tile_load(u, 1))
            pl.when(u < STEPS - 1)(lambda: start(tile_load(u + 1, 1)))
            pl.when(u > 1)(lambda: wait(out2_copies(u - 2)))
            slot = lax.rem(u, 2)
            out2[slot, 0:FFN] = dot_tn(big[:, OWN : OWN + FFN], tokens(u)).astype(BF16)
            out2[slot, FFN:OUT] = dot_tn(big[:, OWN + FFN : KCOL], tokens(u)).astype(BF16)
            start(out2_copies(u))

        def first_half(j):
            grad_in(2 * j)
            pl.when(lax.rem(j, 2) == 1)(lambda: scatter.tick(ticks + 1 + lax.div(j, 2)))
            grad_in(2 * j + 1)
            kv_step(j)

        def second_half(j):
            grad_out(2 * j)
            scatter.tick(ticks + 3 + j)
            grad_out(2 * j + 1)
            kv_step(STEPS // 2 + j)

        loop(STEPS // 2, first_half)
        loop(STEPS // 2 - 1, second_half)
        scatter.finish()
        gain_start()
        loop((STEPS - 2, STEPS - 1), grad_out)
        gain_hop(0)
        kv_step(STEPS - 1)
        gain_hop(1)
        loop((STEPS - 1, STEPS), grad_out)
        gain_finish()
        loop(STEPS, lambda t: wait(turned(t)))
        for u in (STEPS - 2, STEPS - 1):
            wait(out2_copies(u))
        for group in hops.values():
            wait_send(group)


    tall = (*TALL, DIM)
    half = DIM // 2
    wide = [(DIM, NCAT), (NZO, DIM), tall, tall, (SEQ, NCAT), (SEQ, NZO), (SEQ, NCAT), tall, tall, (2, SEQ, SEQ), (4, SEQ, HEAD)]
    wide += [(ITEMS, ROWS, DIM), (GROUP, ROWS, DIM)]
    types = [BF16] * 4 + [F32] + [BF16] * 4 + [F32] + [BF16] * 3
    pl.run_scoped(activations, *[pltpu.VMEM(s, t) for s, t in zip(wide, types)])
    narrow = [(2 * NEAR, NBIG), (2, 2, GROUP, *TALL, TILE), (2, TILE, 2 * FFN), (2, TILE, HEAD), (2, OUT, TILE), (KV, DIM), (ITEMS, ROWS, DIM)]
    totals = [(KV, DIM), (KV, half), (2, KV, EIGHTH), (2, KV, W), (KV, 2 * W), (3, KROWS, 2 * W), (BLOCK, DIM), (4, 1, DIM), (3, 1, DIM), (4, 1, DIM)]
    buffers = [pltpu.VMEM(s, BF16) for s in narrow] + [pltpu.VMEM(s, F32) for s in totals]
    pl.run_scoped(gradients, *buffers)


def layer_call(*args):
    any_spec = pl.BlockSpec(memory_space=pl.ANY)
    vmem_spec = pl.BlockSpec(memory_space=pltpu.VMEM)
    dma = pltpu.SemaphoreType.DMA
    tall = (*TALL, DIM)
    kept = [(GROUP, 2, *tall)] * 2 + [(ITEMS, *tall), (NEAR, NCAT), (NEAR, NZO), (NEAR, OWN), (NEAR, OUT)]
    shapes = kept + [(2, 2, GROUP, ROWS, DIM), (1, DIM), (DIM, FFN), (DIM, FFN), (DIM, HEAD), (FFN, DIM), (HEAD, DIM), (DIM, HEAD), (DIM, HEAD)]
    types = [BF16] * len(shapes)
    types[len(kept) + 1] = F32
    pairs = [(ITEMS, COPIES), (2,), (5,), (GROUP, 2), (GROUP, 3), (8, 6)]
    results = pl.pallas_call(
        layer_kernel,
        out_shape=[jax.ShapeDtypeStruct(s, t) for s, t in zip(shapes, types)],
        in_specs=[any_spec] * 2 + [vmem_spec] + [any_spec] * (len(args) - 5) + [vmem_spec] * 2,
        out_specs=[any_spec] * len(shapes),
        scratch_shapes=[
            *[dma(s) for s in pairs for _ in PAIR],
            *[dma(s) for s in ((6,), (7,), (2,), (2,), (2, 2), (2, 3), (2, 2), (2, STEPS), (6,), (6,))],
            pltpu.SemaphoreType.REGULAR,
            pltpu.VMEM((2, 2, GROUP, ROWS, DIM), BF16),
            *scatter_scratch(),
        ],
        compiler_params=pltpu.CompilerParams(collective_id=0, has_side_effects=True, vmem_limit_bytes=VMEM_BYTES),
        name="layer",
    )(*args)
    return results[len(kept) :]


def finish_kernel(sums, x_loc, dy_loc, gain, *refs):
    *refs, sv, xv, dyv, sem = refs
    count = len(refs) // 3
    sources, (y_out, dx_out, *refs) = refs[:count], refs[count:]
    places, buffers = refs[:count], refs[count:]
    loads = [pltpu.make_async_copy(src, dst, sem.at[k]) for k, (src, dst) in enumerate(zip((sums, x_loc, dy_loc, *sources), (sv, xv, dyv, *buffers)))]
    stores = [pltpu.make_async_copy(src, dst, sem.at[k]) for k, (src, dst) in enumerate(zip((xv, dyv), (y_out, dx_out)))]
    moved = [pltpu.make_async_copy(src, dst, sem.at[3 + k]) for k, (src, dst) in enumerate(zip(buffers, places))]
    start(loads)
    wait(loads[:3])

    def step(i):
        rows = rows16(i * BLOCK, BLOCK)
        res = xv[rows, :].astype(F32)
        x_hat, inv_std = normalize(res)
        d_hat = sv[1, rows, :].astype(F32) * gain[...]
        dx = inv_std * (d_hat - mean(d_hat) - x_hat * mean(d_hat * x_hat)) + dyv[rows, :].astype(F32)
        xv[rows, :] = (res + sv[0, rows, :].astype(F32)).astype(BF16)
        dyv[rows, :] = dx.astype(BF16)

    for k, c in enumerate(moved):
        loop((k, k + 1), step)
        loads[3 + k].wait()
        c.start()
    loop((len(moved), GROUP), step)
    start(stores)
    wait(stores + moved)


def finish_call(sums, x, dy, gain, *grads):
    any_spec = pl.BlockSpec(memory_space=pl.ANY)
    shapes = [x.shape] * 2 + [v.shape for v in grads]
    types = [BF16] * 2 + [v.dtype for v in grads]
    tokens = [sums.shape, x.shape, x.shape]
    return pl.pallas_call(
        finish_kernel,
        out_shape=[jax.ShapeDtypeStruct(s, t) for s, t in zip(shapes, types)],
        in_specs=[any_spec] * 3 + [pl.BlockSpec(memory_space=pltpu.VMEM)] + [any_spec] * len(grads),
        out_specs=[any_spec] * len(shapes),
        scratch_shapes=[
            *[pltpu.VMEM(v.shape, v.dtype) for v in grads],
            *[pltpu.VMEM(s, BF16) for s in tokens],
            pltpu.SemaphoreType.DMA((3 + len(grads),)),
        ],
        compiler_params=pltpu.CompilerParams(vmem_limit_bytes=VMEM_BYTES),
        name="finish",
    )(sums, x, dy, gain, *grads)


def rope_tables():
    inv_freq = np.float32(ROPE_BASE) ** (-np.arange(HEAD // 2, dtype=np.float32) * 2 / HEAD)
    pos = row_position(np.arange(SEQ)).astype(np.float32)
    angles = pos[:, None] * inv_freq.astype(np.float32)
    cos, sin = np.cos(angles), np.sin(angles)
    return np.concatenate([cos, cos], axis=1), np.concatenate([-sin, sin], axis=1)


def solution(mesh):
    def layer_shard(x_loc, dy_loc, ln_gain, w_query, w_key, w_value, w_out, w_gate, w_up, w_down):
        gain = ln_gain.reshape(1, DIM)
        weights = (w_gate, w_up, w_query.reshape(DIM, HEAD), w_key, w_value, w_down, w_out.reshape(HEAD, DIM))
        sums, *grads = layer_call(x_loc, dy_loc, gain, *weights, *rope_tables())
        flat = (ITEMS * ROWS, DIM)
        y_loc, grad_x, dgain, dw1, dw3, dwq, dw2, dwo, dwk, dwv = finish_call(
            sums.reshape(2, *flat), x_loc.reshape(flat), dy_loc.reshape(flat), gain, *grads
        )
        y_loc, grad_x = (v.reshape(x_loc.shape) for v in (y_loc, grad_x))
        return y_loc, grad_x, dgain.reshape(DIM), dwq.reshape(DIM, 1, HEAD), dwk, dwv, dwo.reshape(1, HEAD, DIM), dw1, dw3, dw2

    act = P(None, "tp", None)
    columns, lead, every = P(None, "tp"), P("tp"), P()
    specs = (act, act, every, act, every, every, lead, columns, columns, lead)
    return jax.shard_map(layer_shard, mesh=mesh, in_specs=specs, out_specs=specs, check_vma=False)
```

```python
import jax
import jax.numpy as jnp
import numpy as np
from jax import lax
from jax.experimental import pallas as pl
from jax.experimental.pallas import tpu as pltpu
from jax.sharding import PartitionSpec as P

LN_EPS = 1e-6
ROPE_BASE = 10000.0
MESH = pl.DeviceIdType.MESH
KEEP = dict(axis=-1, keepdims=True)
F32 = jnp.float32
BF16 = jnp.bfloat16
ALL = slice(None)
PAIR = range(2)
LANES = 128
W = 256
VMEM_BYTES = 67043328

GROUP = 8
ITEMS = 2 * GROUP
ROWS = 8
BLOCK = 2 * ROWS
LINE = 4 * BLOCK
SEQ = 4 * LINE
TALL = (2, 2, LINE)
DIM = 4096
HEAD = 128
FFN = 512
OUT = FFN + HEAD
OWN = 2 * FFN + HEAD
KEY = 2 * OWN
VAL = KEY + HEAD
NCAT = VAL + HEAD
NZO = 2 * OUT
QCOL = (2 * FFN, OWN + 2 * FFN)
OCOL = (2 * FFN, 2 * FFN + HEAD)
NEAR = GROUP * SEQ

DEPTH = 5
COPIES = 14


class Columns:
    def __init__(self, a):
        self.a, self.c = a, DIM // 2 - a
        self.left = (slice(0, a), slice(a, 2 * a))
        self.both_left = slice(0, 2 * a)
        self.right = (slice(2 * a, 2 * a + self.c), slice(2 * a + self.c, DIM))
        self.both_right = slice(2 * a, DIM)
        self.halves = (slice(0, self.c), slice(self.c, 2 * self.c))


GCOL = SCOL = Columns(1280)


def place():
    i = lax.axis_index("tp")
    return lax.div(i, 8), lax.rem(lax.div(i, 4), 2), lax.rem(lax.div(i, 2), 2), lax.rem(i, 2)


def index(z, y, x, core):
    return ((z * 2 + y) * 2 + x) * 2 + core


def rows8(start, size):
    return pl.ds(pl.multiple_of(start, ROWS), size)


def rows16(start, size):
    return pl.ds(pl.multiple_of(start, BLOCK), size)


def lanes(start, size):
    return pl.ds(pl.multiple_of(start, LANES), size)


def step_of(t, size):
    return lanes(t * size, size)


def loop(count, body):
    lo, hi = count if isinstance(count, tuple) else (0, count)

    def run(i, carry):
        body(i)
        return carry

    lax.fori_loop(lo, hi, run, 0)


def remote(src, dst, sems, target):
    return pltpu.make_async_remote_copy(src, dst, *sems, device_id=(target,), device_id_type=MESH)


def start(copies):
    for c in copies:
        c.start()


def wait(copies):
    for c in copies:
        c.wait()


def wait_recv(copies):
    for c in copies:
        c.wait_recv()


def wait_send(copies):
    for c in copies:
        c.wait_send()


def partners_of(z, y, x, core):
    chips = [index(lax.rem(z + k, 4), y, x, core) for k in (1, 2, 3)]
    return [index(z, y, x, 1 - core), index(z, y, 1 - x, core), index(z, 1 - y, x, core)] + chips


def greet(semaphore, others):
    for there in others:
        pl.semaphore_signal(semaphore, inc=1, device_id=(there,), device_id_type=MESH)


def dot_nt(a, b):
    return lax.dot_general(a, b, (((1,), (1,)), ((), ())), preferred_element_type=F32)


def dot_tn(a, b):
    return lax.dot_general(a, b, (((0,), (0,)), ((), ())), preferred_element_type=F32)


def dot_nn(a, b):
    return jnp.dot(a, b, preferred_element_type=F32)


def normalize(x):
    centered = x - mean(x)
    inv_std = lax.rsqrt(mean(centered * centered) + LN_EPS)
    return centered * inv_std, inv_std


def mean(v):
    return jnp.mean(v, **KEEP)


def add_into(dst, src, width):
    def tile(t):
        cols = step_of(t, W)
        dst[..., cols] = (dst[..., cols].astype(F32) + src[..., cols].astype(F32)).astype(BF16)

    loop(width // W, tile)


def row_position(r):
    return ((r // BLOCK) % 4) * LINE + (r // (2 * LINE)) * (2 * BLOCK) + ((r // LINE) % 2) * BLOCK + r % BLOCK


class Line:
    def __init__(self, z, y, x, core):
        low = lax.div(z, 2)
        odd = lax.rem(z, 2)
        self.mid = low != odd
        self.end = low == odd
        side = index(z + 1 - 2 * odd, y, x, core)
        across = index(3 - z, y, x, core)
        self.three = rows16(BLOCK - BLOCK * low, 3 * BLOCK)
        self.half = rows16(2 * BLOCK * low, 2 * BLOCK)
        self.other = rows16(2 * BLOCK - 2 * BLOCK * low, 2 * BLOCK)
        self.tip = rows16(3 * BLOCK * low, BLOCK)
        self.own = rows16(BLOCK * z, BLOCK)
        self.spread = ((self.own, side), (self.half, across), (self.three, side))
        self.merge = ((self.three, side), (self.other, across), (self.tip, side))


class Transfer:
    def __init__(self, spot, send, recv):
        self.z, self.y, self.x, self.core = spot
        self.line = Line(*spot)
        self.sib, self.xn, self.yn, *self.zn = partners_of(*spot)
        self.send, self.recv, self.keys = send, recv, {}

    def sems(self, slot, key):
        k = self.keys.setdefault(key, len(self.keys))
        return self.send.at[slot, k], self.recv.at[slot, k]

    def on_end(self, body):
        pl.when(self.line.end)(body)

    def on_mid(self, body):
        pl.when(self.line.mid)(body)

    def tick(self, m):
        for k, stage in reversed(list(enumerate(self.stages))):
            n = m - k
            pl.when((n >= 0) & (n < ITEMS))(lambda stage=stage, n=n: stage(n))


class Gather(Transfer):
    def __init__(self, spot, buf, send, recv):
        super().__init__(spot, send, recv)
        self.buf = buf
        self.stages = (self.stage0, self.stage1, self.stage2, self.stage3, self.stage4, self.stage5)

    def copy(self, n, key, ys, xs, rows, cols, target):
        view = self.buf.at[lax.div(n, 2), lax.rem(n, 2), ys, xs, rows, cols]
        return remote(view, view, self.sems(n, key), target)

    def za(self, n, step):
        rows, target = self.line.spread[step]
        return self.copy(n, ("za", step), self.y, self.x, rows, GCOL.both_left, target)

    def zc(self, n, step):
        rows, target = self.line.spread[step]
        return self.copy(n, ("zc", step), ALL, ALL, rows, GCOL.both_right, target)

    def c1(self, n):
        cols, own = GCOL.right, self.line.own
        return [self.copy(n, "c1x", self.y, self.x, own, cols[0], self.xn), self.copy(n, "c1y", self.y, self.x, own, cols[1], self.yn)]

    def c2(self, n):
        cols, own = GCOL.right, self.line.own
        return [self.copy(n, "c2y", self.y, ALL, own, cols[0], self.yn), self.copy(n, "c2x", ALL, self.x, own, cols[1], self.xn)]

    def a1(self, n):
        cols = GCOL.left
        return [self.copy(n, "a1y", self.y, self.x, ALL, cols[0], self.yn), self.copy(n, "a1x", self.y, self.x, ALL, cols[1], self.xn)]

    def a2(self, n):
        cols = GCOL.left
        return [self.copy(n, "a2x", ALL, self.x, ALL, cols[0], self.xn), self.copy(n, "a2y", self.y, ALL, ALL, cols[1], self.yn)]

    def pass_on(self, chain, n, step):
        def body():
            chain(n, step - 1).wait_recv()
            chain(n, step).start()

        self.on_mid(body)

    def stage0(self, n):
        self.on_end(lambda: self.za(n, 0).start())
        start(self.c1(n))

    def stage1(self, n):
        self.pass_on(self.za, n, 1)
        wait_recv(self.c1(n))
        start(self.c2(n))

    def stage2(self, n):
        self.pass_on(self.za, n, 2)
        wait_recv(self.c2(n))
        self.on_end(lambda: self.zc(n, 0).start())

    def stage3(self, n):
        self.on_end(lambda: self.za(n, 2).wait_recv())
        start(self.a1(n))
        self.pass_on(self.zc, n, 1)

    def stage4(self, n):
        wait_recv(self.a1(n))
        start(self.a2(n))
        self.pass_on(self.zc, n, 2)

    def stage5(self, n):
        wait_recv(self.a2(n))
        self.on_end(lambda: self.zc(n, 2).wait_recv())

    def finish(self, n):
        wait_send(self.c1(n) + self.c2(n) + self.a1(n) + self.a2(n))
        self.on_end(lambda: wait_send([self.za(n, 0), self.zc(n, 0)]))
        self.on_mid(lambda: wait_send([chain(n, step) for chain in (self.za, self.zc) for step in (1, 2)]))


def scatter_shapes():
    a, c = SCOL.a, SCOL.c
    return dict(
        b1=(3, 2, 2, LINE, a), b2=(5, 2, LINE, a), za0=(3, 2, 3 * BLOCK, a), za1=(3, 2, 2 * BLOCK, a), za2=(4, 2, BLOCK, a),
        own_a=(2, 2, 2, LINE, a), own_c=(4, *TALL, 2 * c), zc0=(3, 2, 2, 3 * BLOCK, 2 * c), zc1=(3, 2, 2, 2 * BLOCK, 2 * c),
        zc2=(4, 2, 2, BLOCK, 2 * c), h1=(3, 2, 2, BLOCK, c), h2=(3, 2, BLOCK, c), fin=(3, 2, ROWS, DIM),
    )


SLOTS = 6


def scatter_scratch():
    dma = pltpu.SemaphoreType.DMA
    buffers = [pltpu.VMEM(s, BF16) for s in scatter_shapes().values()]
    return buffers + [dma((SLOTS, COPIES)), dma((SLOTS, COPIES)), dma((SLOTS, 3)), dma((ITEMS,)), dma((ITEMS,))]


class Scatter(Transfer):
    def __init__(self, spot, parts, sums, refs):
        shapes = scatter_shapes()
        self.depth = {name: s[0] for name, s in shapes.items()}
        self.ring = dict(zip(shapes, refs))
        send, recv, self.lsem, *self.store_sems = refs[len(shapes) :]
        super().__init__(spot, send, recv)
        self.parts, self.sums = parts, sums
        self.stages = (self.stage0, self.stage1, self.stage2, self.stage3, self.stage4, self.stage5)

    def slot(self, name, n, *at):
        return self.ring[name].at[(lax.rem(n, self.depth[name]), *at)]

    def copy(self, n, key, src, dst, target):
        return remote(src, dst, self.sems(lax.rem(n, SLOTS), key), target)

    def a1(self, n):
        cols = SCOL.left
        return [
            self.copy(n, "a1x", self.parts.at[n, :, 1 - self.x, :, cols[0]], self.slot("b1", n, 0), self.xn),
            self.copy(n, "a1y", self.parts.at[n, 1 - self.y, :, :, cols[1]], self.slot("b1", n, 1), self.yn),
        ]

    def a2(self, n):
        return [
            self.copy(n, "a2y", self.slot("b1", n, 0, 1 - self.y), self.slot("b2", n, 0), self.yn),
            self.copy(n, "a2x", self.slot("b1", n, 1, 1 - self.x), self.slot("b2", n, 1), self.xn),
        ]

    def za(self, n, step):
        rows, target = self.line.merge[step]
        key = f"za{step}"
        return self.copy(n, key, self.slot("b2", n, ALL, rows, ALL), self.slot(key, n), target)

    def zc(self, n, step):
        rows, target = self.line.merge[step]
        key = f"zc{step}"
        src = self.slot("own_c", n, ALL, ALL, rows, ALL) if step else self.parts.at[n, :, :, rows, SCOL.both_right]
        return self.copy(n, key, src, self.slot(key, n), target)

    def h1(self, n):
        cols = SCOL.halves
        return [
            self.copy(n, "h1y", self.slot("zc2", n, 1 - self.y, ALL, ALL, cols[0]), self.slot("h1", n, 0), self.yn),
            self.copy(n, "h1x", self.slot("zc2", n, ALL, 1 - self.x, ALL, cols[1]), self.slot("h1", n, 1), self.xn),
        ]

    def h2(self, n):
        cols = SCOL.halves
        return [
            self.copy(n, "h2x", self.slot("zc2", n, self.y, 1 - self.x, ALL, cols[0]), self.slot("h2", n, 0), self.xn),
            self.copy(n, "h2y", self.slot("zc2", n, 1 - self.y, self.x, ALL, cols[1]), self.slot("h2", n, 1), self.yn),
        ]

    def loads(self, n):
        sem = self.lsem.at[lax.rem(n, SLOTS)]
        views = (
            (self.parts.at[n, :, self.x, :, SCOL.left[0]], self.slot("own_a", n, 0)),
            (self.parts.at[n, self.y, :, :, SCOL.left[1]], self.slot("own_a", n, 1)),
            (self.parts.at[n, :, :, :, SCOL.both_right], self.slot("own_c", n)),
        )
        return [pltpu.make_async_copy(src, dst, sem.at[k]) for k, (src, dst) in enumerate(views)]

    def kept(self, n):
        return self.sums.at[lax.rem(n, 2), self.core, lax.div(n, 2)]

    def store(self, n):
        send, recv = self.store_sems
        return remote(self.slot("fin", n, 1 - self.core), self.kept(n), (send.at[n], recv.at[n]), self.sib)

    def stage0(self, n):
        start(self.a1(n))
        self.on_end(lambda: self.zc(n, 0).start())
        start(self.loads(n))

    def stage1(self, n):
        wait(self.loads(n))
        wait_recv(self.a1(n))
        for c in PAIR:
            add_into(self.slot("b1", n, c), self.slot("own_a", n, c), SCOL.a)
        start(self.a2(n))

        def middle():
            self.zc(n, 0).wait_recv()
            add_into(self.slot("own_c", n, ALL, ALL, self.line.three), self.slot("zc0", n), 2 * SCOL.c)
            self.zc(n, 1).start()

        self.on_mid(middle)
        wait_send(self.a1(n))
        self.on_end(lambda: self.zc(n, 0).wait_send())

    def stage2(self, n):
        wait_recv(self.a2(n))
        for c, mine in enumerate((self.y, self.x)):
            add_into(self.slot("b2", n, c), self.slot("b1", n, c, mine), SCOL.a)
        self.on_end(lambda: self.za(n, 0).start())

        def middle():
            self.zc(n, 1).wait_recv()
            add_into(self.slot("own_c", n, ALL, ALL, self.line.half), self.slot("zc1", n), 2 * SCOL.c)
            self.zc(n, 2).start()
            self.zc(n, 1).wait_send()

        self.on_mid(middle)
        wait_send(self.a2(n))

    def stage3(self, n):
        own_c = self.slot("own_c", n, ALL, ALL, self.line.own)

        def middle():
            self.za(n, 0).wait_recv()
            add_into(self.slot("b2", n, ALL, self.line.three), self.slot("za0", n), SCOL.a)
            self.za(n, 1).start()
            self.slot("zc2", n)[...] = own_c[...]

        def tip():
            self.zc(n, 2).wait_recv()
            add_into(self.slot("zc2", n), own_c, 2 * SCOL.c)

        self.on_mid(middle)
        self.on_end(tip)
        start(self.h1(n))
        self.on_mid(lambda: self.zc(n, 2).wait_send())
        self.on_end(lambda: self.za(n, 0).wait_send())

    def stage4(self, n):
        def middle():
            self.za(n, 1).wait_recv()
            add_into(self.slot("b2", n, ALL, self.line.half), self.slot("za1", n), SCOL.a)
            self.za(n, 2).start()
            self.za(n, 1).wait_send()

        self.on_mid(middle)
        wait_recv(self.h1(n))
        cols = SCOL.halves
        add_into(self.slot("zc2", n, self.y, ALL, ALL, cols[0]), self.slot("h1", n, 0), SCOL.c)
        add_into(self.slot("zc2", n, ALL, self.x, ALL, cols[1]), self.slot("h1", n, 1), SCOL.c)
        start(self.h2(n))
        wait_send(self.h1(n))

    def stage5(self, n):
        pl.when(n >= self.depth["fin"])(lambda: self.store(n - self.depth["fin"]).wait_send())

        def tip():
            self.za(n, 2).wait_recv()
            add_into(self.slot("b2", n, ALL, self.line.own), self.slot("za2", n), SCOL.a)

        self.on_end(tip)
        self.on_mid(lambda: self.za(n, 2).wait_send())
        wait_recv(self.h2(n))
        fin = self.slot("fin", n)

        def put(total, col):
            for core in PAIR:
                fin[core, :, lanes(col, W)] = total[core * ROWS : (core + 1) * ROWS].astype(BF16)

        def left(t):
            for c in PAIR:
                put(self.slot("b2", n, c, self.line.own)[:, step_of(t, W)].astype(F32), c * SCOL.a + t * W)

        def right(t):
            for c in PAIR:
                mine = self.slot("zc2", n, self.y, self.x)[:, lanes(c * SCOL.c + t * W, W)].astype(F32)
                put(mine + self.slot("h2", n, c)[:, step_of(t, W)].astype(F32), 2 * SCOL.a + c * SCOL.c + t * W)

        loop(SCOL.a // W, left)
        loop(SCOL.c // W, right)
        self.store(n).start()
        self.kept(n)[...] = fin[self.core]
        wait_send(self.h2(n))

    def finish(self):
        loop((ITEMS - self.depth["fin"], ITEMS), lambda n: self.store(n).wait_send())
        loop(ITEMS, lambda n: self.store(n).wait_recv())


TILE = 512
STEPS = DIM // TILE
KV = 2 * HEAD
KCOL = OWN + OUT
NBIG = KCOL + KV
QUARTER = DIM // 4
EIGHTH = DIM // 8
KROWS = KV // 4


def layer_kernel(
    x_loc, dy_loc, gain, w1, w3, wq, wk, wv, w2, wo, cos_t, sin_t,
    full, full_sib, parts, g_all, zo_all, g_sib, zo_sib, sums_out, dgain, dw1, dw3, dwq, dw2, dwo, dwk, dwv,
    gsend, grecv, sx, rx, sw, rw, ss, rs, sg, rg, ksend, krecv, lsem, wsem, osem, gsem,
    tsem, o1sem, o2sem, tosem, hsend, hrecv, ready, sums, *scatter_refs,
):
    spot = place()
    z, y, x, core = spot
    partners = partners_of(*spot)
    sib, xn, yn, *zn = partners
    barrier = pltpu.get_barrier_semaphore()
    greet(barrier, partners)
    gather = Gather(spot, full, gsend, grecv)
    scatter = Scatter(spot, parts, sums, scatter_refs)

    def meet(others):
        greet(ready, others)
        pl.semaphore_wait(ready, len(others))

    def activations(wcat, w2o, hv, dyv, proj, zo, g, yo, dho, probs, qs, stage, dy_own):
        own, far_half = (rows8(GROUP * c, GROUP) for c in (core, 1 - core))
        takes = [pltpu.make_async_copy(x_loc, stage, lsem.at[0]), pltpu.make_async_copy(dy_loc.at[own], dy_own, lsem.at[1])]
        start(takes)
        wait(takes)

        def norm_step(i):
            two = pl.ds(i * 2, 2)
            x_hat, _ = normalize(stage[two].astype(F32).reshape(BLOCK, DIM))
            stage[two] = (gain[...] * x_hat).astype(BF16).reshape(2, ROWS, DIM)

        loop(GROUP, norm_step)
        pl.semaphore_wait(barrier, len(partners))

        mine = rows8(BLOCK * z + ROWS * core, ROWS)
        to = [full.at[:, s, y, x, mine, :] for s in PAIR]
        away = (stage.at[far_half], dy_loc.at[far_half])
        swaps = [remote(away[s], to[s], (sx.at[s], rx.at[s]), sib) for s in PAIR]
        puts = [pltpu.make_async_copy(src, dst, lsem.at[s]) for s, (src, dst) in enumerate(zip((stage.at[own], dy_own), to))]
        start(swaps + puts)
        for s in PAIR:
            puts[s].wait()
            swaps[s].wait_recv()
            loop((s, s + 1), gather.tick)

        spots = (
            (w1, wcat.at[:, 0:FFN], wcat.at[:, OWN : OWN + FFN]),
            (w3, wcat.at[:, FFN : 2 * FFN], wcat.at[:, OWN + FFN : OWN + 2 * FFN]),
            (wq, wcat.at[:, 2 * FFN : OWN], wcat.at[:, OWN + 2 * FFN : KEY]),
            (w2, w2o.at[0:FFN], w2o.at[FFN : 2 * FFN]),
            (wo, w2o.at[OCOL[0] : OCOL[1]], w2o.at[OCOL[1] : NZO]),
        )
        shared = ((wk, wcat.at[:, KEY:VAL]), (wv, wcat.at[:, VAL:NCAT]))
        weights = [(w, near) for w, near, _ in spots] + list(shared)
        local = [pltpu.make_async_copy(w, near, wsem.at[k]) for k, (w, near) in enumerate(weights)]
        far = [remote(w, there, (sw.at[k], rw.at[k]), sib) for k, (w, _, there) in enumerate(spots)]
        start(local)
        meet([sib])
        start(far)
        loop((2, DEPTH + 1), gather.tick)

        def load(b, s):
            return pltpu.make_async_copy(full.at[b, s], (hv, dyv)[s], lsem.at[s])

        def sib_copy(b, s):
            return remote(full.at[b, s], full_sib.at[b, s], (ss.at[b, s], rs.at[b, s]), sib)

        def arrived(b, s):
            load(b, s).start()
            sib_copy(b, s).start()

        arrived(0, 0)
        wait(local)
        wait_recv(far)

        def gz_copies(b):
            rows = rows16(b * SEQ, SEQ)
            views = (
                (g.at[:, OWN:KEY], g_sib.at[rows]),
                (zo.at[:, FFN : 2 * FFN], zo_sib.at[rows, 0:FFN]),
                (zo.at[:, OCOL[1] : NZO], zo_sib.at[rows, FFN:OUT]),
            )
            return [remote(src, dst, (sg.at[b, k], rg.at[b, k]), sib) for k, (src, dst) in enumerate(views)]

        def gz_local(b):
            rows = rows16(b * SEQ, SEQ)
            return [pltpu.make_async_copy(g, g_all.at[rows], gsem.at[0]), pltpu.make_async_copy(zo, zo_all.at[rows], gsem.at[1])]

        def out(b, s):
            return pltpu.make_async_copy((yo, dho)[s], parts.at[2 * b + s], osem.at[s])

        def drained(b):
            wait([*gz_local(b), out(b, 1)])
            wait_send(gz_copies(b))

        scale = HEAD ** -0.5

        def rotate(v, back=False):
            turn = pltpu.roll(v, HEAD // 2, 1) * sin_t[...]
            return v * cos_t[...] + (-turn if back else turn)

        def flat(ref):
            return ref[...].reshape(SEQ, DIM)

        def gate_up(t):
            at = t * W + lax.div(t, 2) * (OWN - FFN)
            return lanes(at, W), lanes(at + FFN, W)

        wide = lambda t: step_of(t, FFN)

        def batch_step(b):
            ahead = 2 * b + DEPTH + 1
            load(b, 0).wait()

            def proj_tile(t):
                proj[:, wide(t)] = dot_nn(flat(hv), wcat[:, wide(t)])

            loop(NCAT // FFN, proj_tile)
            pl.when(b > 0)(lambda: drained(b - 1))
            scatter.tick(2 * b - 1)

            def hidden_tile(t):
                gate_at, up_at = gate_up(t)
                gate = proj[:, gate_at]
                zo[:, step_of(t, W)] = (gate * jax.nn.sigmoid(gate) * proj[:, up_at]).astype(BF16)

            loop(2 * FFN // W, hidden_tile)
            keys = rotate(proj[:, KEY:VAL]).astype(BF16)
            vals = proj[:, VAL:NCAT].astype(BF16)
            qs[2] = keys
            qs[3] = vals
            causal = row_position(lax.broadcasted_iota(jnp.int32, (SEQ, SEQ), 0)) >= row_position(lax.broadcasted_iota(jnp.int32, (SEQ, SEQ), 1))
            for hd in PAIR:
                query = rotate(proj[:, QCOL[hd] : QCOL[hd] + HEAD]).astype(BF16)
                qs[hd] = query
                scores = jnp.where(causal, dot_nt(query, keys) * scale, -1e30)
                e = jnp.exp(scores - jnp.max(scores, **KEEP))
                p = e / jnp.sum(e, **KEEP)
                probs[hd] = p
                zo[:, OCOL[hd] : OCOL[hd] + HEAD] = dot_nn(p.astype(BF16), vals).astype(BF16)

            gather.tick(ahead)
            arrived(b, 1)

            def y_tile(t):
                yo[:, :, :, wide(t)] = dot_nn(zo[...], w2o[:, wide(t)]).astype(BF16).reshape(*TALL, FFN)

            loop(DIM // FFN, y_tile)
            out(b, 0).start()
            load(b, 1).wait()

            def dz_tile(t):
                dz = dot_nt(flat(dyv), w2o[rows16(t * W, W), :])
                gate_at, up_at = gate_up(t)
                gate = proj[:, gate_at]
                sig = jax.nn.sigmoid(gate)
                g[:, gate_at] = (dz * proj[:, up_at] * sig * (1.0 + gate * (1.0 - sig))).astype(BF16)
                g[:, up_at] = (dz * (gate * sig)).astype(BF16)

            loop(2 * FFN // W, dz_tile)
            out(b, 0).wait()
            scatter.tick(2 * b)
            d_heads = dot_nt(flat(dyv), w2o[2 * FFN : NZO, :]).astype(BF16)
            d_keys = d_vals = jnp.zeros((SEQ, HEAD), F32)
            for hd in PAIR:
                d_out = d_heads[:, hd * HEAD : (hd + 1) * HEAD]
                p = probs[hd]
                d_probs = dot_nt(d_out, qs[3])
                d_vals = d_vals + dot_tn(p.astype(BF16), d_out)
                row_dot = jnp.sum(p * d_probs, **KEEP)
                d_scores = (p * (d_probs - row_dot) * scale).astype(BF16)
                g[:, QCOL[hd] : QCOL[hd] + HEAD] = rotate(dot_nn(d_scores, qs[2]), True).astype(BF16)
                d_keys = d_keys + dot_tn(d_scores, qs[hd])
            g[:, KEY:VAL] = rotate(d_keys, True).astype(BF16)
            g[:, VAL:NCAT] = d_vals.astype(BF16)
            gather.tick(ahead + 1)
            pl.when(b < GROUP - 1)(lambda: arrived(b + 1, 0))

            def dh_tile(t):
                dho[:, :, :, wide(t)] = dot_nt(g[...], wcat[rows16(t * FFN, FFN), :]).astype(BF16).reshape(*TALL, FFN)

            loop(DIM // FFN, dh_tile)
            out(b, 1).start()
            start(gz_local(b) + gz_copies(b))

        loop(GROUP, batch_step)
        drained(GROUP - 1)

        def finish(b):
            for s in PAIR:
                gather.finish(2 * b + s)
                sib_copy(b, s).wait()
            wait_recv(gz_copies(b))

        loop(GROUP, finish)
        wait_send(swaps + far)


    def gradients(big, tiles, out1, outq, out2, kvo, xb, kvp, k1, k2, k3, kc, k4, gacc, gpart, ggot, gz):
        x_in = pltpu.make_async_copy(x_loc, xb, gsem.at[0])
        x_in.start()
        near, away = slice(0, NEAR), slice(NEAR, 2 * NEAR)
        views = (
            (g_all.at[:, KEY:NCAT], big.at[near, KCOL:NBIG]),
            (g_all.at[:, 0:OWN], big.at[near, 0:OWN]),
            (g_sib, big.at[away, 0:OWN]),
            (zo_all.at[:, 0:FFN], big.at[near, OWN : OWN + FFN]),
            (zo_all.at[:, OCOL[0] : OCOL[1]], big.at[near, OWN + FFN : KCOL]),
            (zo_sib, big.at[away, OWN:KCOL]),
        )
        loads = [pltpu.make_async_copy(src, dst, lsem.at[k]) for k, (src, dst) in enumerate(views)]
        start(loads)

        def tile_load(u, s):
            slot = lax.rem(u, 2)
            sources = (full, full_sib)
            return [pltpu.make_async_copy(sources[k].at[:, s, :, :, :, step_of(u, TILE)], tiles.at[slot, k], tsem.at[slot, k]) for k in PAIR]

        tile_load(0, 0)[0].start()
        loads[0].wait()

        def kv_tile(u):
            pl.when(u < STEPS - 1)(lambda: tile_load(u + 1, 0)[0].start())
            tile_load(u, 0)[0].wait()
            kvp[:, step_of(u, TILE)] = dot_tn(big[near, KCOL:NBIG], tiles[lax.rem(u, 2), 0].reshape(NEAR, TILE))

        loop(STEPS, kv_tile)
        start(tile_load(0, 0))

        half = core * (DIM // 2)
        quarter = (half, half + QUARTER)
        ring = ((x, y, xn, yn), (y, x, yn, xn))
        first = [quarter[c] + ring[c][0] * EIGHTH for c in PAIR]
        second = [first[c] + ring[c][1] * W for c in PAIR]
        mine = rows16(z * KROWS, KROWS)
        hops = {}

        def hop(step, src, dst, target):
            group = hops.setdefault(step, [])
            group.append(remote(src, dst, (ksend.at[step, len(group)], krecv.at[step, len(group)]), target))

        hop(0, kvp.at[:, lanes(DIM // 2 - half, DIM // 2)], k1, sib)
        for c in PAIR:
            a, b, an, bn = ring[c]
            hop(1, kvp.at[:, lanes(quarter[c] + (1 - a) * EIGHTH, EIGHTH)], k2.at[c], an)
            hop(2, kvp.at[:, lanes(first[c] + (1 - b) * W, W)], k3.at[c], bn)
            same = kvo.at[:, lanes(second[c], W)]
            hop(5, same, same, bn)
            same = kvo.at[:, lanes(first[c], EIGHTH)]
            hop(6, same, same, an)
        for k, there in enumerate(zn):
            hop(3, kc.at[rows16(lax.rem(z + k + 1, 4) * KROWS, KROWS)], k4.at[k], there)
            for c in PAIR:
                same = kvo.at[mine, lanes(second[c], W)]
                hop(4, same, same, there)
        same = kvo.at[:, lanes(half, DIM // 2)]
        hop(7, same, same, sib)

        def kv_add(src, at, width):
            def tile(t):
                cols = lanes(at + t * W, W)
                kvp[:, cols] = kvp[:, cols] + src[:, step_of(t, W)]

            loop(width // W, tile)

        def kv_first():
            kv_add(k1, half, DIM // 2)

        def kv_second():
            for c in PAIR:
                kv_add(k2.at[c], first[c], EIGHTH)

        def kv_third():
            for c in PAIR:
                kc[:, c * W : (c + 1) * W] = kvp[:, lanes(second[c], W)] + k3[c]

        def kv_round():
            total = kc[mine, :] + k4[0] + k4[1] + k4[2]
            for c in PAIR:
                kvo[mine, lanes(second[c], W)] = total[:, c * W : (c + 1) * W].astype(BF16)

        def turned(t):
            views = ((out1.at[s, :, lanes(t * HEAD, HEAD)], (dwk, dwv)[s].at[step_of(t, TILE)]) for s in PAIR)
            return [pltpu.make_async_copy(src, dst, tosem.at[s, t]) for s, (src, dst) in enumerate(views)]

        def kv_turn(t):
            for s in PAIR:
                out1[s, :, lanes(t * HEAD, HEAD)] = kvo[s * HEAD : (s + 1) * HEAD, step_of(t, TILE)].astype(F32).T.astype(BF16)
            start(turned(t))

        works = (kv_first, kv_second, kv_third, kv_round)

        def kv_step(j):
            for step in range(len(hops)):

                @pl.when(j == step)
                def _(step=step):
                    wait_recv(hops[step])
                    if step < len(works):
                        works[step]()
                    elif step == len(hops) - 1:
                        loop((STEPS - 2, STEPS), lambda u: wait(out_copies(u)))
                        loop(STEPS, kv_turn)
                    start(hops.get(step + 1, ()))

        meet(partners)
        start(hops[0])
        ticks = ITEMS - 1
        scatter.tick(ticks)
        wait(loads[1:])

        def out_copies(u):
            slot = lax.rem(u, 2)
            rows = step_of(u, TILE)
            sem = o1sem.at[slot]
            return [
                pltpu.make_async_copy(out1.at[slot, :, 0:FFN], dw1.at[rows], sem.at[0]),
                pltpu.make_async_copy(out1.at[slot, :, FFN : 2 * FFN], dw3.at[rows], sem.at[1]),
                pltpu.make_async_copy(outq.at[slot], dwq.at[rows], sem.at[2]),
            ]

        def out2_copies(u):
            slot, cols = lax.rem(u, 2), step_of(u, TILE)
            sem = o2sem.at[slot]
            return [
                pltpu.make_async_copy(out2.at[slot, 0:FFN], dw2.at[:, cols], sem.at[0]),
                pltpu.make_async_copy(out2.at[slot, FFN:OUT], dwo.at[:, cols], sem.at[1]),
            ]

        def gain_step(i):
            first = i * 2
            two = pl.ds(lax.rem(first, GROUP), 2)
            x_hat, _ = normalize(xb[pl.ds(first, 2)].astype(F32).reshape(BLOCK, DIM))
            gacc[...] = gacc[...] + sums[1, lax.div(first, GROUP), two].astype(F32).reshape(BLOCK, DIM) * x_hat

        near = partners[: len(partners) - len(zn)]
        gain_hops = [remote(gpart.at[k], ggot.at[k], (hsend.at[k], hrecv.at[k]), there) for k, there in enumerate(near)]
        last = len(near)
        gain_last = [remote(gpart.at[last], gz.at[z], (hsend.at[last + k], hrecv.at[last + k]), there) for k, there in enumerate(zn)]
        results = pltpu.make_async_copy(sums, sums_out, osem.at[0])
        gain_out = pltpu.make_async_copy(gpart.at[0], dgain, osem.at[1])

        def gain_start():
            results.start()
            x_in.wait()
            gacc[...] = jnp.zeros_like(gacc)
            loop(GROUP, gain_step)
            gpart[0] = jnp.sum(gacc[...], axis=0, keepdims=True)
            gain_hops[0].start()

        def gain_hop(k):
            gain_hops[k].wait_recv()
            gpart[k + 1] = gpart[k] + ggot[k]
            start(gain_hops[k + 1 : k + 2] or gain_last)

        def gain_finish():
            gain_hop(last - 1)
            gz[z] = gpart[last]
            wait(gain_last)
            wait_send(gain_hops)
            gpart[0] = gz[0] + gz[1] + gz[2] + gz[3]
            gain_out.start()
            gain_out.wait()
            results.wait()

        def tokens(u):
            return tiles[lax.rem(u, 2)].reshape(2 * NEAR, TILE)

        def grad_in(u):
            wait(tile_load(u, 0))
            pl.when(u < STEPS - 1)(lambda: start(tile_load(u + 1, 0)))
            pl.when(u == STEPS - 1)(lambda: start(tile_load(0, 1)))
            pl.when(u > 1)(lambda: wait(out_copies(u - 2)))
            slot = lax.rem(u, 2)
            for s in PAIR:
                out1[slot, :, s * FFN : (s + 1) * FFN] = dot_tn(tokens(u), big[:, s * FFN : (s + 1) * FFN]).astype(BF16)
            outq[slot] = dot_tn(big[:, 2 * FFN : OWN], tokens(u)).T.astype(BF16)
            start(out_copies(u))

        def grad_out(u):
            wait(tile_load(u, 1))
            pl.when(u < STEPS - 1)(lambda: start(tile_load(u + 1, 1)))
            pl.when(u > 1)(lambda: wait(out2_copies(u - 2)))
            slot = lax.rem(u, 2)
            out2[slot, 0:FFN] = dot_tn(big[:, OWN : OWN + FFN], tokens(u)).astype(BF16)
            out2[slot, FFN:OUT] = dot_tn(big[:, OWN + FFN : KCOL], tokens(u)).astype(BF16)
            start(out2_copies(u))

        def first_half(j):
            grad_in(2 * j)
            pl.when(lax.rem(j, 2) == 1)(lambda: scatter.tick(ticks + 1 + lax.div(j, 2)))
            grad_in(2 * j + 1)
            kv_step(j)

        def second_half(j):
            grad_out(2 * j)
            scatter.tick(ticks + 3 + j)
            grad_out(2 * j + 1)
            kv_step(STEPS // 2 + j)

        loop(STEPS // 2, first_half)
        loop(STEPS // 2 - 1, second_half)
        scatter.finish()
        gain_start()
        loop((STEPS - 2, STEPS - 1), grad_out)
        gain_hop(0)
        kv_step(STEPS - 1)
        gain_hop(1)
        loop((STEPS - 1, STEPS), grad_out)
        gain_finish()
        loop(STEPS, lambda t: wait(turned(t)))
        for u in (STEPS - 2, STEPS - 1):
            wait(out2_copies(u))
        for group in hops.values():
            wait_send(group)


    tall = (*TALL, DIM)
    half = DIM // 2
    wide = [(DIM, NCAT), (NZO, DIM), tall, tall, (SEQ, NCAT), (SEQ, NZO), (SEQ, NCAT), tall, tall, (2, SEQ, SEQ), (4, SEQ, HEAD)]
    wide += [(ITEMS, ROWS, DIM), (GROUP, ROWS, DIM)]
    types = [BF16] * 4 + [F32] + [BF16] * 4 + [F32] + [BF16] * 3
    pl.run_scoped(activations, *[pltpu.VMEM(s, t) for s, t in zip(wide, types)])
    narrow = [(2 * NEAR, NBIG), (2, 2, GROUP, *TALL, TILE), (2, TILE, 2 * FFN), (2, TILE, HEAD), (2, OUT, TILE), (KV, DIM), (ITEMS, ROWS, DIM)]
    totals = [(KV, DIM), (KV, half), (2, KV, EIGHTH), (2, KV, W), (KV, 2 * W), (3, KROWS, 2 * W), (BLOCK, DIM), (4, 1, DIM), (3, 1, DIM), (4, 1, DIM)]
    buffers = [pltpu.VMEM(s, BF16) for s in narrow] + [pltpu.VMEM(s, F32) for s in totals]
    pl.run_scoped(gradients, *buffers)


def layer_call(*args):
    any_spec = pl.BlockSpec(memory_space=pl.ANY)
    vmem_spec = pl.BlockSpec(memory_space=pltpu.VMEM)
    dma = pltpu.SemaphoreType.DMA
    tall = (*TALL, DIM)
    kept = [(GROUP, 2, *tall)] * 2 + [(ITEMS, *tall), (NEAR, NCAT), (NEAR, NZO), (NEAR, OWN), (NEAR, OUT)]
    shapes = kept + [(2, 2, GROUP, ROWS, DIM), (1, DIM), (DIM, FFN), (DIM, FFN), (DIM, HEAD), (FFN, DIM), (HEAD, DIM), (DIM, HEAD), (DIM, HEAD)]
    types = [BF16] * len(shapes)
    types[len(kept) + 1] = F32
    pairs = [(ITEMS, COPIES), (2,), (5,), (GROUP, 2), (GROUP, 3), (8, 6)]
    results = pl.pallas_call(
        layer_kernel,
        out_shape=[jax.ShapeDtypeStruct(s, t) for s, t in zip(shapes, types)],
        in_specs=[any_spec] * 2 + [vmem_spec] + [any_spec] * (len(args) - 5) + [vmem_spec] * 2,
        out_specs=[any_spec] * len(shapes),
        scratch_shapes=[
            *[dma(s) for s in pairs for _ in PAIR],
            *[dma(s) for s in ((6,), (7,), (2,), (2,), (2, 2), (2, 3), (2, 2), (2, STEPS), (6,), (6,))],
            pltpu.SemaphoreType.REGULAR,
            pltpu.VMEM((2, 2, GROUP, ROWS, DIM), BF16),
            *scatter_scratch(),
        ],
        compiler_params=pltpu.CompilerParams(collective_id=0, has_side_effects=True, vmem_limit_bytes=VMEM_BYTES),
        name="layer",
    )(*args)
    return results[len(kept) :]


def finish_kernel(sums, x_loc, dy_loc, gain, *refs):
    *refs, sv, xv, dyv, sem = refs
    count = len(refs) // 3
    sources, (y_out, dx_out, *refs) = refs[:count], refs[count:]
    places, buffers = refs[:count], refs[count:]
    loads = [pltpu.make_async_copy(src, dst, sem.at[k]) for k, (src, dst) in enumerate(zip((sums, x_loc, dy_loc, *sources), (sv, xv, dyv, *buffers)))]
    stores = [pltpu.make_async_copy(src, dst, sem.at[k]) for k, (src, dst) in enumerate(zip((xv, dyv), (y_out, dx_out)))]
    moved = [pltpu.make_async_copy(src, dst, sem.at[3 + k]) for k, (src, dst) in enumerate(zip(buffers, places))]
    start(loads)
    wait(loads[:3])

    def step(i):
        rows = rows16(i * BLOCK, BLOCK)
        res = xv[rows, :].astype(F32)
        x_hat, inv_std = normalize(res)
        d_hat = sv[1, rows, :].astype(F32) * gain[...]
        dx = inv_std * (d_hat - mean(d_hat) - x_hat * mean(d_hat * x_hat)) + dyv[rows, :].astype(F32)
        xv[rows, :] = (res + sv[0, rows, :].astype(F32)).astype(BF16)
        dyv[rows, :] = dx.astype(BF16)

    for k, c in enumerate(moved):
        loop((k, k + 1), step)
        loads[3 + k].wait()
        c.start()
    loop((len(moved), GROUP), step)
    start(stores)
    wait(stores + moved)


def finish_call(sums, x, dy, gain, *grads):
    any_spec = pl.BlockSpec(memory_space=pl.ANY)
    shapes = [x.shape] * 2 + [v.shape for v in grads]
    types = [BF16] * 2 + [v.dtype for v in grads]
    tokens = [sums.shape, x.shape, x.shape]
    return pl.pallas_call(
        finish_kernel,
        out_shape=[jax.ShapeDtypeStruct(s, t) for s, t in zip(shapes, types)],
        in_specs=[any_spec] * 3 + [pl.BlockSpec(memory_space=pltpu.VMEM)] + [any_spec] * len(grads),
        out_specs=[any_spec] * len(shapes),
        scratch_shapes=[
            *[pltpu.VMEM(v.shape, v.dtype) for v in grads],
            *[pltpu.VMEM(s, BF16) for s in tokens],
            pltpu.SemaphoreType.DMA((3 + len(grads),)),
        ],
        compiler_params=pltpu.CompilerParams(vmem_limit_bytes=VMEM_BYTES),
        name="finish",
    )(sums, x, dy, gain, *grads)


def rope_tables():
    inv_freq = np.float32(ROPE_BASE) ** (-np.arange(HEAD // 2, dtype=np.float32) * 2 / HEAD)
    pos = row_position(np.arange(SEQ)).astype(np.float32)
    angles = pos[:, None] * inv_freq.astype(np.float32)
    cos, sin = np.cos(angles), np.sin(angles)
    return np.concatenate([cos, cos], axis=1), np.concatenate([-sin, sin], axis=1)


def solution(mesh):
    def layer_shard(x_loc, dy_loc, ln_gain, w_query, w_key, w_value, w_out, w_gate, w_up, w_down):
        gain = ln_gain.reshape(1, DIM)
        weights = (w_gate, w_up, w_query.reshape(DIM, HEAD), w_key, w_value, w_down, w_out.reshape(HEAD, DIM))
        sums, *grads = layer_call(x_loc, dy_loc, gain, *weights, *rope_tables())
        flat = (ITEMS * ROWS, DIM)
        y_loc, grad_x, dgain, dw1, dw3, dwq, dw2, dwo, dwk, dwv = finish_call(
            sums.reshape(2, *flat), x_loc.reshape(flat), dy_loc.reshape(flat), gain, *grads
        )
        y_loc, grad_x = (v.reshape(x_loc.shape) for v in (y_loc, grad_x))
        return y_loc, grad_x, dgain.reshape(DIM), dwq.reshape(DIM, 1, HEAD), dwk, dwv, dwo.reshape(1, HEAD, DIM), dw1, dw3, dw2

    act = P(None, "tp", None)
    columns, lead, every = P(None, "tp"), P("tp"), P()
    specs = (act, act, every, act, every, every, lead, columns, columns, lead)
    return jax.shard_map(layer_shard, mesh=mesh, in_specs=specs, out_specs=specs, check_vma=False)
```
